32 devices in a mesh: gx: 8 (over z, y), gy: 4 (over x, core).
Axes of the slice: x: 2, y: 2, z: 4, core: 2. Of those that a mesh axis runs over, the one named last changes fastest.
Arguments:
- charge_density: float32 [256, 256, 256], P('gx', 'gy'), may hold values from -5080 to 5140
Outputs:
- potential: float32 [256, 256, 256], P('gx', 'gy')
- energies: float32 [2], replicated
The draws below stay inside these ranges and needn't reach their ends.
All inputs are finite; a program needn't handle non-finite values.
Results may differ from the reference program's by a relative error of at most 0.0003.
Values sent between devices are 32-bit elements.
A program may use at most 192 MiB of HBM per device.

```python
import math
import jax
import jax.numpy as jnp
import numpy as np
from jax import lax

N = 256
ORDER = 16


def draw_charge_density(key, part):
    level_key, noise_key = jax.random.split(jax.random.fold_in(key, 11))
    bound = float((N + 1) * (N + 1) // 13)
    levels = jax.random.uniform(level_key, (8, 8, 8), jnp.float32, minval=0.0, maxval=60.0)
    noise = jax.random.uniform(noise_key, (N, N, N), jnp.float32, minval=-bound, maxval=bound)
    block = N // 8
    coarse = jnp.repeat(jnp.repeat(jnp.repeat(levels, block, 0), block, 1), block, 2)
    return (coarse + noise).astype(jnp.float32)


def setup_inputs(seed: int = 0) -> dict:
    key_of = jax.random.split(jax.random.key(seed), 2)
    return {
        "charge_density": draw_charge_density(jax.random.fold_in(key_of[1], 71), 0),
    }


exact_mode = lax.Precision.HIGHEST
outer_ratio = 1.1
radius_scale = math.sqrt(3.0) / 2.0

def sine_table(length):
    counter = jnp.arange(length, dtype=jnp.int32) + 1
    product = counter[:, None] * counter[None, :] % (2 * (length + 1))
    return jnp.sin(math.pi * product.astype(jnp.float32) / (length + 1))

def eigen_line(counter, length):
    half_angle = math.pi * (counter + 1).astype(jnp.float32) / (2.0 * (length + 1))
    return 4.0 * float((length + 1) * (length + 1)) * jnp.sin(half_angle) ** 2

def recurrence_tables():
    degree_count = ORDER + 1
    near_coeff = np.zeros((degree_count, degree_count, 1), np.float32)
    far_coeff = np.zeros((degree_count, degree_count, 1), np.float32)
    sector = np.ones(degree_count, np.float32)
    for degree in range(1, degree_count):
        for azimuth in range(degree):
            divisor = math.sqrt(degree * degree - azimuth * azimuth)
            near_coeff[degree, azimuth, 0] = (2 * degree - 1) / divisor
            far_coeff[degree, azimuth, 0] = math.sqrt((degree - 1) * (degree - 1) - azimuth * azimuth) / divisor
        if degree >= 2:
            sector[degree] = math.sqrt((2 * degree - 1) / (2.0 * degree))
    return (near_coeff, far_coeff, sector)

def expansion_weights():
    degree_count = ORDER + 1
    weights = np.zeros((degree_count, degree_count), np.float32)
    for degree in range(degree_count):
        for azimuth in range(degree + 1):
            factor = 1.0 if azimuth == 0 else 2.0
            weights[degree, azimuth] = factor / (4.0 * math.pi * radius_scale * outer_ratio ** (degree + 1))
    return weights

def harmonic_sweep(unit_x, unit_y, unit_z, visitor, running):
    near_coeff, far_coeff, sector = recurrence_tables()
    degree_count = ORDER + 1
    selector = np.eye(degree_count, dtype=np.float32)[:, :, None]
    empty_rows = jnp.zeros((degree_count,) + unit_x.shape, unit_x.dtype)
    sector_cosine = jnp.ones_like(unit_x)
    sector_sine = jnp.zeros_like(unit_x)
    cosine_prev, sine_prev, cosine_old, sine_old = (empty_rows, empty_rows, empty_rows, empty_rows)
    for degree in range(degree_count):
        if degree > 0:
            sector_cosine, sector_sine = (sector[degree] * (unit_x * sector_cosine - unit_y * sector_sine), sector[degree] * (unit_x * sector_sine + unit_y * sector_cosine))
        cosine_now = near_coeff[degree] * unit_z * cosine_prev - far_coeff[degree] * cosine_old + selector[degree] * sector_cosine
        sine_now = near_coeff[degree] * unit_z * sine_prev - far_coeff[degree] * sine_old + selector[degree] * sector_sine
        running = visitor(running, degree, cosine_now, sine_now)
        cosine_old, sine_old = (cosine_prev, sine_prev)
        cosine_prev, sine_prev = (cosine_now, sine_now)
    return running

def face_moments(point_x, point_y, point_z, charge):
    radius = jnp.sqrt(point_x * point_x + point_y * point_y + point_z * point_z)
    scaled_radius = radius / radius_scale

    def visitor(running, degree, cosine_now, sine_now):
        weight, moment_cosine, moment_sine, facing_cosine, facing_sine = running
        moment_cosine = moment_cosine + [jnp.dot(cosine_now, weight, precision=exact_mode)]
        moment_sine = moment_sine + [jnp.dot(sine_now, weight, precision=exact_mode)]
        facing_cosine = facing_cosine + [jnp.dot(cosine_now, charge, precision=exact_mode)]
        facing_sine = facing_sine + [jnp.dot(sine_now, charge, precision=exact_mode)]
        return (weight * scaled_radius, moment_cosine, moment_sine, facing_cosine, facing_sine)
    result = harmonic_sweep(point_x / radius, point_y / radius, point_z / radius, visitor, (charge, [], [], [], []))
    return tuple((jnp.stack(listing) for listing in result[1:]))

def face_potential(point_x, point_y, point_z, weight_cosine, weight_sine):
    radius = jnp.sqrt(point_x * point_x + point_y * point_y + point_z * point_z)

    def visitor(accum, degree, cosine_now, sine_now):
        accum = accum + jnp.dot(weight_cosine[degree], cosine_now, precision=exact_mode)
        return accum + jnp.dot(weight_sine[degree], sine_now, precision=exact_mode)
    return harmonic_sweep(point_x / radius, point_y / radius, point_z / radius, visitor, jnp.zeros_like(point_x))

def transform(volume, sine_rows):
    volume = jnp.einsum('abc,ck->abk', volume, sine_rows, precision=exact_mode)
    volume = jnp.einsum('abk,bj->ajk', volume, sine_rows, precision=exact_mode)
    return jnp.einsum('ajk,ai->ijk', volume, sine_rows, precision=exact_mode)

def poisson_solve(volume, sine_rows, denominator):
    return transform(transform(volume, sine_rows) / denominator, sine_rows)

def reference(charge_density):
    length = N
    spacing = 1.0 / (length + 1)
    sine_rows = sine_table(length)
    eigen_rows = eigen_line(jnp.arange(length, dtype=jnp.int32), length)
    denominator = (eigen_rows[:, None, None] + eigen_rows[None, :, None] + eigen_rows[None, None, :]) * ((length + 1) / 2.0) ** 3
    first_field = poisson_solve(charge_density, sine_rows, denominator)
    coords = (jnp.arange(length, dtype=jnp.float32) - (length - 1) / 2.0) * spacing
    grid_rows = jnp.broadcast_to(coords[:, None], (length, length)).reshape(-1)
    grid_columns = jnp.broadcast_to(coords[None, :], (length, length)).reshape(-1)
    plane_half = jnp.full((length * length,), 0.5, jnp.float32)
    boundary_faces = [(grid_rows, grid_columns, -plane_half, first_field[:, :, 0]), (grid_rows, grid_columns, plane_half, first_field[:, :, -1]), (-plane_half, grid_rows, grid_columns, first_field[0]), (plane_half, grid_rows, grid_columns, first_field[-1]), (grid_rows, -plane_half, grid_columns, first_field[:, 0]), (grid_rows, plane_half, grid_columns, first_field[:, -1])]
    totals = None
    for point_x, point_y, point_z, near_cells in boundary_faces:
        face_terms = face_moments(point_x, point_y, point_z, spacing * near_cells.reshape(-1))
        if totals is None:
            totals = face_terms
        else:
            totals = tuple((earlier + later for earlier, later in zip(totals, face_terms)))
    weights = expansion_weights()
    weight_cosine = weights * totals[0]
    weight_sine = weights * totals[1]
    potentials = []
    for point_x, point_y, point_z, near_cells in boundary_faces:
        potentials.append(face_potential(point_x, point_y, point_z, weight_cosine, weight_sine).reshape(length, length) / spacing ** 2)
    source = charge_density
    source = source.at[:, :, 0].add(potentials[0])
    source = source.at[:, :, -1].add(potentials[1])
    source = source.at[0].add(potentials[2])
    source = source.at[-1].add(potentials[3])
    source = source.at[:, 0].add(potentials[4])
    source = source.at[:, -1].add(potentials[5])
    potential = poisson_solve(source, sine_rows, denominator)
    energies = spacing ** 3 * jnp.stack([jnp.sum(charge_density * first_field), jnp.sum(charge_density * potential)])
    return (potential, energies)
```

```python
import functools
import math

import jax
import jax.numpy as jnp
import numpy as np
from jax import lax
from jax.experimental import pallas as pl
from jax.experimental.pallas import tpu as pltpu
from jax.sharding import PartitionSpec as P

ORDER = 16
DEG = ORDER + 1
RATIO = 1.1
RADIUS = math.sqrt(3.0) / 2.0
HIGH = lax.Precision.HIGH
BEST = lax.Precision.HIGHEST
LANES = 128
MESH = pl.DeviceIdType.MESH


def solid_harmonics(x, y, z):
    rr = x * x + y * y + z * z
    out = np.zeros((DEG, 2 * DEG - 1) + x.shape)
    cos = np.zeros((DEG, DEG) + x.shape)
    sin = np.zeros((DEG, DEG) + x.shape)
    cos[0, 0] = 1.0
    for l in range(1, DEG):
        s = 1.0 if l == 1 else math.sqrt((2 * l - 1) / (2.0 * l))
        cos[l, l] = s * (x * cos[l - 1, l - 1] - y * sin[l - 1, l - 1])
        sin[l, l] = s * (x * sin[l - 1, l - 1] + y * cos[l - 1, l - 1])
        for m in range(l):
            div = math.sqrt(l * l - m * m)
            far = math.sqrt((l - 1) * (l - 1) - m * m) if l - 1 > m else 0.0
            for f in (cos, sin):
                f[l, m] = (2 * l - 1) * z * f[l - 1, m] / div
                if l >= 2 and far:
                    f[l, m] = f[l, m] - far * rr * f[l - 2, m] / div
    out[:, :DEG] = cos
    out[:, DEG:] = sin[:, 1:]
    return out


def face_tensors():
    t = np.cos(np.pi * (np.arange(DEG) + 0.5) / DEG)
    fwd = np.cos(np.arange(DEG)[:, None] * np.arccos(t)[None, :]) * (2.0 / DEG)
    fwd[0] *= 0.5
    u, v = np.meshgrid(t / 2, t / 2, indexing="ij")
    half = np.full_like(u, 0.5)
    tensors = []
    for pts in ((half, u, v), (u, half, v), (u, v, half)):
        vals = solid_harmonics(*pts)
        tensors.append(np.einsum("pu,lfuv,qv->lfpq", fwd, vals, fwd))
    par = np.ones((3, DEG, 2 * DEG - 1))
    for l in range(DEG):
        for f in range(2 * DEG - 1):
            m, odd = (f, 0) if f < DEG else (f - ORDER, 1)
            par[0, l, f] = (-1.0) ** (m + odd)
            par[1, l, f] = (-1.0) ** odd
            par[2, l, f] = (-1.0) ** (l + m)
    return np.stack(tensors).astype(np.float32).reshape(3, DEG, 2 * DEG - 1, DEG * DEG), par.astype(np.float32)


def expansion_weights():
    w = np.zeros((DEG, 2 * DEG - 1))
    for l in range(DEG):
        for f in range(2 * DEG - 1):
            m = f if f < DEG else f - ORDER
            w[l, f] = (1.0 if m == 0 else 2.0) / (4.0 * math.pi * RADIUS * RATIO ** (l + 1))
    return w.astype(np.float32)


def split(x):
    hi = x.astype(jnp.bfloat16)
    return hi, (x - hi.astype(jnp.float32)).astype(jnp.bfloat16)


def dot(a, b):
    return jnp.dot(a, b, preferred_element_type=jnp.float32)


def left_mul(mat, x):
    hi, lo = split(x)
    return dot(mat[0], hi) + dot(mat[0], lo) + dot(mat[1], hi)


def right_mul(x, mat):
    hi, lo = split(x)
    return dot(hi, mat[0]) + dot(lo, mat[0]) + dot(hi, mat[1])


def split_table(table):
    t = jnp.asarray(np.asarray(table, np.float32))
    return jnp.stack(split(t))


def turn(x, shift):
    width = x.shape[-1]
    shift %= width
    return pltpu.roll(x, shift, x.ndim - 1) if shift else x


class Plan:
    def __init__(self, ca, cb, n, gx, gy):
        self.ca, self.cb, self.n, self.gx, self.gy = ca, cb, n, gx, gy
        self.kb = n // gy
        self.jb = n // gx
        self.width = LANES
        self.pack = LANES // self.kb
        self.sub = ca // self.pack
        self.step = max(1, self.sub // 8)
        self.pair = 2 if self.step % 2 == 0 else 1
        self.chunks = self.sub // self.step
        self.tile = min(n, 64)

    def lanes(self, rows):
        return lax.broadcasted_iota(jnp.int32, (rows, LANES), 1) // self.kb


def greet(p):
    ix, iy = lax.axis_index("gx"), lax.axis_index("gy")
    barrier = pltpu.get_barrier_semaphore()
    for d in range(1, p.gx):
        pl.semaphore_signal(barrier, inc=1, device_id={"gx": lax.rem(ix + d, p.gx)}, device_id_type=MESH)
    for d in range(1, p.gy):
        pl.semaphore_signal(barrier, inc=1, device_id={"gy": lax.rem(iy + d, p.gy)}, device_id_type=MESH)
    pl.semaphore_wait(barrier, p.gx + p.gy - 2)


def remote(src, dst, send, recv, where):
    return pltpu.make_async_remote_copy(
        src_ref=src, dst_ref=dst, send_sem=send, recv_sem=recv, device_id=where, device_id_type=MESH
    )


def mode_tables(p, epsj_ref, epsk_ref, tab_ref):
    iy = lax.axis_index("gy")
    sigma = epsj_ref[...] + epsk_ref[iy][0:1]
    s = 0.5 * jnp.sqrt(sigma)
    t = jnp.sqrt(1.0 + s * s)
    theta = 2.0 * jnp.log1p(s + s * s / (1.0 + t))
    lam = jnp.exp(-theta)
    tab_ref[0] = lam
    tab_ref[1] = 1.0 / (4.0 * s * t)
    tab_ref[2] = jnp.exp(-theta * float(p.sub))
    tab_ref[3] = jnp.exp(-theta * float(p.ca))
    tab_ref[4] = lam / (1.0 - jnp.exp(-theta * (2.0 * (p.n + 1))))
    tab_ref[5] = jnp.exp(-theta * float(p.n + 1))


def edge_sums(p, v_ref, tab_ref, left_ref, right_ref, edge_ref):
    for t in range(p.n // p.tile):
        rows = pl.ds(t * p.tile, p.tile)
        lam, lsub = tab_ref[0, rows], tab_ref[2, rows]
        left, right = v_ref[0, rows], v_ref[p.sub - 1, rows]
        for i in range(1, p.sub):
            left = left * lam + v_ref[i, rows]
            right = right * lam + v_ref[p.sub - 1 - i, rows]
        left_ref[rows] = left
        right_ref[rows] = right
        dev_l, dev_r = left, right
        for g in range(1, p.pack):
            dev_l = dev_l * lsub + turn(left, -g * p.kb)
            dev_r = dev_r * lsub + turn(right, g * p.kb)
        edge_ref[rows] = jnp.where(p.lanes(p.tile) == 0, dev_l, dev_r)


def line_exchange(p, tab_ref, edge_ref, got_ref, back_ref, ends_ref, sems, between):
    ix = lax.axis_index("gx")
    mine = pl.ds(ix * p.jb, p.jb)

    def copies(src, dst, base):
        out = []
        for d in range(1, p.gx):
            r = lax.rem(ix + d, p.gx)
            out.append(remote(src(r), dst, sems.at[base, d], sems.at[base + 1, d], {"gx": r}))
        return out

    first = copies(lambda r: edge_ref.at[pl.ds(r * p.jb, p.jb)], got_ref.at[ix], 0)
    for c in first:
        c.start()
    got_ref[ix] = edge_ref[mine]
    between(0)
    for c in first:
        c.wait_recv()
    lower = p.lanes(p.jb) == 0
    blk, det, lnp = tab_ref[3, mine], tab_ref[4, mine], tab_ref[5, mine]
    state = jnp.zeros((p.jb, LANES), jnp.float32)
    states = []
    for t in range(p.gx):
        states.append(state)
        state = state * blk + jnp.where(lower, got_ref[t], got_ref[p.gx - 1 - t])
    other = jnp.where(lower, turn(state, p.kb), turn(state, -p.kb))
    image = (other - state * lnp) * det
    for t in range(p.gx):
        states[t] = states[t] - image
        image = image * blk
    for t in range(p.gx):
        back_ref[t] = jnp.where(lower, states[t], states[p.gx - 1 - t])
    second = copies(lambda r: back_ref.at[r], ends_ref.at[mine], 2)
    for c in second:
        c.start()
    ends_ref[mine] = back_ref[ix]
    between(1)
    for c in second:
        c.wait_recv()
    for c in first + second:
        c.wait_send()


def carries(p, rows, tab_ref, left_ref, right_ref, ends_ref):
    lsub = tab_ref[2, rows]
    left, right = left_ref[rows], right_ref[rows]
    a = b = ends_ref[rows]
    place = p.lanes(p.tile)
    for g in range(p.pack - 1):
        a = jnp.where(place == g + 1, turn(a * lsub + left, p.kb), a)
        h = p.pack - 1 - g
        b = jnp.where(place == h - 1, turn(b * lsub + right, -p.kb), b)
    return a, b


def forward_kernel(p, rho_ref, sz_ref, sy_ref, epsj_ref, epsk_ref, rhs_ref, first_ref, tab_ref,
                   x_ref, send_ref, spec_ref, left_ref, right_ref, edge_ref, got_ref, back_ref, ends_ref,
                   in_sems, out_sems, land_sems, line_sems):
    iy = lax.axis_index("gy")

    def load(c, g):
        rows = pl.ds(g * p.sub + c * p.step, p.step)
        return pltpu.make_async_copy(rho_ref.at[rows], x_ref.at[rows], in_sems.at[c, g])

    for c in range(p.chunks):
        for g in range(p.pack):
            load(c, g).start()
    greet(p)

    def swap(c, d):
        q = lax.rem(iy + d, p.gy)
        planes = pl.ds(c * p.step, p.step)
        return remote(send_ref.at[q, planes], spec_ref.at[planes, pl.ds(iy * p.cb, p.cb)],
                      out_sems.at[c, d], land_sems.at[c, d], {"gy": q})

    block = p.step * p.cb
    order = list(range(p.gy // 2, p.gy)) + list(range(1, p.gy // 2))

    def transform(c, carry):
        for g in range(p.pack):
            load(c, g).wait()
        x = jnp.concatenate(
            [x_ref[pl.ds(g * p.sub + c * p.step, p.step)].reshape(block, p.n) for g in range(p.pack)], axis=0
        )
        y = right_mul(x, sz_ref)
        place = p.lanes(block)
        planes = pl.ds(c * p.step, p.step)
        for q in range(p.gy):
            col, off = divmod(q * p.kb, LANES)
            piece = None
            for g in range(p.pack):
                part = turn(y[g * block:(g + 1) * block, col * LANES:(col + 1) * LANES], g * p.kb - off)
                piece = part if piece is None else jnp.where(place == g, part, piece)
            send_ref[q, planes] = piece.reshape(p.step, p.cb, LANES)

        @pl.when(c > 0)
        def _():
            for d in order:
                swap(c - 1, d).start()

        spec_ref[planes, pl.ds(iy * p.cb, p.cb)] = send_ref[iy, planes]
        return carry

    lax.fori_loop(0, p.chunks, transform, 0)
    mode_tables(p, epsj_ref, epsk_ref, tab_ref)
    for d in order:
        swap(p.chunks - 1, d).start()

    def across(c, carry):
        for d in order:
            swap(c, d).wait_recv()
        for i in range(0, p.step, p.pair):
            s = c * p.step + i
            x = jnp.concatenate([spec_ref[s + e] for e in range(p.pair)], axis=1)
            y = left_mul(sy_ref, x)
            for e in range(p.pair):
                rhs_ref[s + e] = y[:, e * LANES:(e + 1) * LANES]
        return carry

    lax.fori_loop(0, p.chunks, across, 0)
    edge_sums(p, rhs_ref, tab_ref, left_ref, right_ref, edge_ref)
    line_exchange(p, tab_ref, edge_ref, got_ref, back_ref, ends_ref, line_sems, lambda stage: None)

    for t in range(p.n // p.tile):
        rows = pl.ds(t * p.tile, p.tile)
        lam, inv = tab_ref[0, rows], tab_ref[1, rows]
        a, b = carries(p, rows, tab_ref, left_ref, right_ref, ends_ref)
        for i in range(p.sub - 1, -1, -1):
            b = b * lam
            first_ref[i, rows] = b
            b = b + rhs_ref[i, rows]
        for i in range(p.sub):
            a = a * lam + rhs_ref[i, rows]
            first_ref[i, rows] = (a + first_ref[i, rows]) * inv

    def drain(c, carry):
        for d in order:
            swap(c, d).wait_send()
        return carry

    lax.fori_loop(0, p.chunks, drain, 0)


def forward(p, rho, sz, sy, epsj, epsk):
    f32 = jnp.float32
    cube = (p.sub, p.n, LANES)
    vmem = pl.BlockSpec(memory_space=pltpu.VMEM)
    dma = pltpu.SemaphoreType.DMA
    return pl.pallas_call(
        functools.partial(forward_kernel, p),
        in_specs=[pl.BlockSpec(memory_space=pl.ANY)] + [vmem] * 4,
        out_specs=[vmem] * 3,
        out_shape=[
            jax.ShapeDtypeStruct(cube, f32),
            jax.ShapeDtypeStruct(cube, f32),
            jax.ShapeDtypeStruct((6, p.n, LANES), f32),
        ],
        scratch_shapes=[
            pltpu.VMEM((p.ca, p.cb, p.n), f32),
            pltpu.VMEM((p.gy, p.sub, p.cb, LANES), f32),
            pltpu.VMEM(cube, f32),
            pltpu.VMEM((p.n, LANES), f32),
            pltpu.VMEM((p.n, LANES), f32),
            pltpu.VMEM((p.n, LANES), f32),
            pltpu.VMEM((p.gx, p.jb, LANES), f32),
            pltpu.VMEM((p.gx, p.jb, LANES), f32),
            pltpu.VMEM((p.n, LANES), f32),
            dma((p.chunks, p.pack)),
            dma((p.chunks, p.gy)),
            dma((p.chunks, p.gy)),
            dma((4, p.gx)),
        ],
        compiler_params=pltpu.CompilerParams(
            collective_id=0, has_side_effects=True, vmem_limit_bytes=40 * 2**20
        ),
        name="forward",
    )(rho, sz, sy, epsj, epsk)


def total_copies(p, src_ref, slots_ref, sems, axis, base):
    size = p.gx if axis == "gx" else p.gy
    me = lax.axis_index(axis)
    out = []
    for d in range(1, size):
        r = lax.rem(me + d, size)
        out.append(remote(src_ref, slots_ref.at[me], sems.at[base, d], sems.at[base + 1, d], {axis: r}))
    return out


def reduce_kernel(p, x_ref, out_ref, stage_ref, sum_ref, xs_ref, ys_ref, sems):
    ix, iy = lax.axis_index("gx"), lax.axis_index("gy")
    stage_ref[...] = x_ref[...]
    xs_ref[ix] = x_ref[...]
    greet(p)
    a = total_copies(p, stage_ref, xs_ref, sems, "gx", 0)
    for c in a:
        c.start()
    for c in a:
        c.wait_recv()
    total = xs_ref[0]
    for i in range(1, p.gx):
        total = total + xs_ref[i]
    sum_ref[...] = total
    ys_ref[iy] = total
    b = total_copies(p, sum_ref, ys_ref, sems, "gy", 2)
    for c in b:
        c.start()
    for c in b:
        c.wait_recv()
    total = ys_ref[0]
    for i in range(1, p.gy):
        total = total + ys_ref[i]
    out_ref[...] = total
    for c in a + b:
        c.wait_send()


def all_sum(p, x):
    f32 = jnp.float32
    vmem = pl.BlockSpec(memory_space=pltpu.VMEM)
    return pl.pallas_call(
        functools.partial(reduce_kernel, p),
        in_specs=[vmem],
        out_specs=vmem,
        out_shape=jax.ShapeDtypeStruct(x.shape, f32),
        scratch_shapes=[
            pltpu.VMEM(x.shape, f32),
            pltpu.VMEM(x.shape, f32),
            pltpu.VMEM((p.gx,) + x.shape, f32),
            pltpu.VMEM((p.gy,) + x.shape, f32),
            pltpu.SemaphoreType.DMA((4, max(p.gx, p.gy))),
        ],
        compiler_params=pltpu.CompilerParams(collective_id=1, has_side_effects=True, vmem_limit_bytes=8 * 2**20),
        name="all_sum",
    )(x)


def backward_kernel(p, rhs_ref, first_ref, tab_ref, sy_ref, sz_ref, out_ref, energy_ref,
                    w_ref, u_ref, carry_ref, left_ref, right_ref, edge_ref, got_ref, back_ref, ends_ref,
                    part_ref, xs_ref, sum_ref, ys_ref, res_ref,
                    write_sems, out_sems, land_sems, line_sems, sum_sems):
    ix, iy = lax.axis_index("gx"), lax.axis_index("gy")
    greet(p)
    edge_sums(p, rhs_ref, tab_ref, left_ref, right_ref, edge_ref)

    ea = total_copies(p, part_ref, xs_ref, sum_sems, "gx", 0)
    eb = total_copies(p, sum_ref, ys_ref, sum_sems, "gy", 2)

    def between(stage):
        if stage == 0:
            energy = jnp.zeros((8, LANES), jnp.float32)
            for i in range(p.sub):
                prod = first_ref[i] * rhs_ref[i]
                for r in range(p.n // 8):
                    energy = energy + prod[r * 8:(r + 1) * 8]
            part_ref[...] = energy
            xs_ref[ix] = energy
            return
        for c in ea:
            c.start()

    line_exchange(p, tab_ref, edge_ref, got_ref, back_ref, ends_ref, line_sems, between)
    for t in range(p.n // p.tile):
        rows = pl.ds(t * p.tile, p.tile)
        lam = tab_ref[0, rows]
        a, b = carries(p, rows, tab_ref, left_ref, right_ref, ends_ref)
        carry_ref[rows] = a
        for i in range(p.sub - 1, -1, -1):
            b = b * lam
            w_ref[i, rows] = b
            b = b + rhs_ref[i, rows]
    for c in ea:
        c.wait_recv()
    total = xs_ref[0]
    for i in range(1, p.gx):
        total = total + xs_ref[i]
    sum_ref[...] = total
    ys_ref[iy] = total

    order = list(range(p.gy // 2, p.gy)) + list(range(1, p.gy // 2))

    def swap(c, d):
        q = lax.rem(iy + d, p.gy)
        planes = pl.ds(c * p.step, p.step)
        return remote(u_ref.at[planes, pl.ds(q * p.cb, p.cb)], res_ref.at[iy, planes],
                      out_sems.at[c, d], land_sems.at[c, d], {"gy": q})

    def across(c, carry):
        for t in range(p.n // p.tile):
            rows = pl.ds(t * p.tile, p.tile)
            lam, inv = tab_ref[0, rows], tab_ref[1, rows]
            a = carry_ref[rows]
            for i in range(p.step):
                s = c * p.step + i
                a = a * lam + rhs_ref[s, rows]
                w_ref[s, rows] = (a + w_ref[s, rows]) * inv
            carry_ref[rows] = a
        for i in range(0, p.step, p.pair):
            s = c * p.step + i
            x = jnp.concatenate([w_ref[s + e] for e in range(p.pair)], axis=1)
            y = left_mul(sy_ref, x)
            for e in range(p.pair):
                u_ref[s + e] = y[:, e * LANES:(e + 1) * LANES]
        planes = pl.ds(c * p.step, p.step)

        @pl.when(c > 0)
        def _():
            for d in order:
                swap(c - 1, d).start()

        res_ref[iy, planes] = u_ref[planes, pl.ds(iy * p.cb, p.cb)]
        return carry

    lax.fori_loop(0, p.chunks, across, 0)
    for c in eb:
        c.start()
    for d in order:
        swap(p.chunks - 1, d).start()

    block = p.step * p.cb

    def write(c, g):
        rows = pl.ds(g * p.sub + c * p.step, p.step)
        return pltpu.make_async_copy(x_view(rows), out_ref.at[rows], write_sems.at[c, g])

    def x_view(rows):
        return fin_ref.at[rows]

    fin_ref = energy_ref[1]

    def finish(c, carry):
        for d in order:
            swap(c, d).wait_recv()
        planes = pl.ds(c * p.step, p.step)
        place = p.lanes(block)
        parts = [res_ref[q, planes].reshape(block, LANES) for q in range(p.gy)]
        per = LANES // p.kb
        rows = []
        for g in range(p.pack):
            cols = []
            for col in range(p.n // LANES):
                acc = None
                for e in range(per):
                    part = turn(parts[col * per + e], (e - g) * p.kb)
                    acc = part if acc is None else jnp.where(place == e, part, acc)
                cols.append(acc)
            rows.append(jnp.concatenate(cols, axis=1))
        y = right_mul(jnp.concatenate(rows, axis=0), sz_ref)
        for g in range(p.pack):
            at = pl.ds(g * p.sub + c * p.step, p.step)
            fin_ref[at] = y[g * block:(g + 1) * block].reshape(p.step, p.cb, p.n)

        @pl.when(c > 0)
        def _():
            for g in range(p.pack):
                write(c - 1, g).start()

        return carry

    lax.fori_loop(0, p.chunks, finish, 0)
    for c in eb:
        c.wait_recv()
    total = ys_ref[0]
    for i in range(1, p.gy):
        total = total + ys_ref[i]
    energy_ref[0][...] = total
    for g in range(p.pack):
        write(p.chunks - 1, g).start()
    for c in range(p.chunks):
        for g in range(p.pack):
            write(c, g).wait()
    for c in ea + eb:
        c.wait_send()

    def drain(c, carry):
        for d in order:
            swap(c, d).wait_send()
        return carry

    lax.fori_loop(0, p.chunks, drain, 0)


def backward_entry(p, rhs_ref, first_ref, tab_ref, sy_ref, sz_ref, out_ref, energy_ref, fin_ref, *rest):
    backward_kernel(p, rhs_ref, first_ref, tab_ref, sy_ref, sz_ref, out_ref, (energy_ref, fin_ref), *rest)


def backward(p, rhs, first, tab, sy, sz):
    f32 = jnp.float32
    cube = (p.sub, p.n, LANES)
    plane = (p.n, LANES)
    vmem = pl.BlockSpec(memory_space=pltpu.VMEM)
    dma = pltpu.SemaphoreType.DMA
    return pl.pallas_call(
        functools.partial(backward_entry, p),
        in_specs=[vmem] * 5,
        out_specs=[pl.BlockSpec(memory_space=pl.ANY), vmem],
        out_shape=[jax.ShapeDtypeStruct((p.ca, p.cb, p.n), f32), jax.ShapeDtypeStruct((8, LANES), f32)],
        scratch_shapes=[
            pltpu.VMEM((p.ca, p.cb, p.n), f32),
            pltpu.VMEM(cube, f32),
            pltpu.VMEM(cube, f32),
            pltpu.VMEM(plane, f32),
            pltpu.VMEM(plane, f32),
            pltpu.VMEM(plane, f32),
            pltpu.VMEM(plane, f32),
            pltpu.VMEM((p.gx, p.jb, LANES), f32),
            pltpu.VMEM((p.gx, p.jb, LANES), f32),
            pltpu.VMEM(plane, f32),
            pltpu.VMEM((8, LANES), f32),
            pltpu.VMEM((p.gx, 8, LANES), f32),
            pltpu.VMEM((8, LANES), f32),
            pltpu.VMEM((p.gy, 8, LANES), f32),
            pltpu.VMEM((p.gy, p.sub, p.cb, LANES), f32),
            dma((p.chunks, p.pack)),
            dma((p.chunks, p.gy)),
            dma((p.chunks, p.gy)),
            dma((4, p.gx)),
            dma((4, max(p.gx, p.gy))),
        ],
        compiler_params=pltpu.CompilerParams(
            collective_id=2, has_side_effects=True, vmem_limit_bytes=40 * 2**20
        ),
        name="backward",
    )(rhs, first, tab, sy, sz)


def shards(charge_density):
    ca, cb, n = charge_density.shape
    gx, gy = lax.axis_size("gx"), lax.axis_size("gy")
    ix, iy = lax.axis_index("gx"), lax.axis_index("gy")
    kb = n // gy
    pack = LANES // kb
    sub = ca // pack
    width = pack * kb
    h = 1.0 / (n + 1)
    norm = (2.0 * h) ** 2

    num = np.arange(n) + 1
    sine64 = np.sin(np.pi * ((num[:, None] * num[None, :]) % (2 * (n + 1))) / (n + 1))
    sine = jnp.asarray(sine64.astype(np.float32))
    eps64 = 4.0 * np.sin(np.pi * num / (2.0 * (n + 1))) ** 2
    cheb64 = np.cos(np.arange(DEG)[None, :] * np.arccos((2.0 * np.arange(n) - (n - 1)) * h)[:, None])
    cheb = jnp.asarray(cheb64.astype(np.float32))
    chebhat = jnp.asarray((sine64 @ cheb64).astype(np.float32))
    tensors, parity = face_tensors()

    epsj = jnp.asarray(np.repeat(eps64.astype(np.float32)[:, None], LANES, axis=1))
    epsk = np.tile(eps64.astype(np.float32).reshape(gy, 1, kb), (1, 8, pack))
    plan = Plan(ca, cb, n, gx, gy)
    sz = split_table(sine64)
    rhs, first, tab = forward(plan, charge_density, sz, split_table(sine64 * h * h), epsj, jnp.asarray(epsk))

    edge_rows = jnp.stack([sine[0], sine[n - 1]])
    edge_k = lax.dynamic_slice_in_dim(edge_rows, iy * kb, kb, 1)
    hat_k = lax.dynamic_slice_in_dim(chebhat, iy * kb, kb, 0)
    cheb_a = lax.dynamic_slice_in_dim(cheb, ix * ca, ca, 0)
    wall_x = jnp.stack([first[0, :, :kb], first[sub - 1, :, width - kb :]])
    own_x = jnp.stack([ix == 0, ix == gx - 1]).astype(jnp.float32)
    wall_x = wall_x * own_x[:, None, None]
    mom_x = jnp.einsum("fjk,jp->fpk", wall_x, chebhat, precision=BEST)
    mom_x = jnp.einsum("fpk,kq->fpq", mom_x, hat_k, precision=BEST)
    wall_y = jnp.sum(first[None] * edge_rows[:, None, :, None], axis=2)
    wall_y = wall_y.reshape(2, sub, pack, kb).transpose(0, 2, 1, 3).reshape(2, ca, kb)
    mom_y = jnp.einsum("fak,ap->fpk", wall_y, cheb_a, precision=BEST)
    mom_y = jnp.einsum("fpk,kq->fpq", mom_y, hat_k, precision=BEST)
    edge_lane = jnp.einsum("fk,gh->gkfh", edge_k, jnp.eye(pack, dtype=jnp.float32)).reshape(width, 2 * pack)
    wall_z = jnp.einsum("sjl,lc->csj", first, edge_lane, precision=HIGH)
    wall_z = wall_z.reshape(2, ca, n)
    mom_z = jnp.einsum("faj,jq->faq", wall_z, chebhat, precision=BEST)
    mom_z = jnp.einsum("faq,ap->fpq", mom_z, cheb_a, precision=BEST)
    moments = jnp.stack([mom_x, mom_y, mom_z]).reshape(-1) * (h * norm)
    energy_one = h * norm * jnp.sum(first * rhs)
    packed = jnp.concatenate([moments, energy_one[None]])
    fill = -packed.shape[0] % (8 * LANES)
    packed = all_sum(plan, jnp.pad(packed, (0, fill)).reshape(-1, LANES)).reshape(-1)[: packed.shape[0]]
    moments = packed[:-1].reshape(3, 2, 1, 1, DEG * DEG)
    energy_one = packed[-1]

    tens = jnp.asarray(tensors)
    par = jnp.asarray(parity)
    gain = jnp.asarray(expansion_weights() * (RADIUS ** -np.arange(DEG, dtype=np.float64))[:, None].astype(np.float32))
    lm = jnp.sum(tens * moments[:, 1], axis=3) + par * jnp.sum(tens * moments[:, 0], axis=3)
    lm = jnp.sum(lm, axis=0) * gain
    coef_hi = jnp.sum(tens * lm[None, :, :, None], axis=2).reshape(3, DEG, DEG, DEG)
    coef_lo = jnp.sum(tens * (par * lm[None])[..., None], axis=2).reshape(3, DEG, DEG, DEG)

    coord = jnp.asarray(((np.arange(n) - (n - 1) / 2.0) * h).astype(np.float32))
    coord_a = lax.dynamic_slice_in_dim(coord, ix * ca, ca)

    def face(coefs, cheb_u, cheb_v, u, v):
        part = jnp.einsum("flpq,up->fluq", coefs, cheb_u, precision=BEST)
        part = jnp.einsum("fluq,vq->fluv", part, cheb_v, precision=HIGH)
        rinv = lax.rsqrt(0.25 + u[:, None] * u[:, None] + v[None, :] * v[None, :])
        acc = part[:, ORDER]
        for l in range(ORDER - 1, -1, -1):
            acc = acc * rinv + part[:, l]
        return acc

    coef_x = jnp.where(ix == 0, coef_lo[0], coef_hi[0])[None]
    phi_x = face(coef_x, cheb, cheb, coord, coord)[0]
    phi_y = face(jnp.stack([coef_lo[1], coef_hi[1]]), cheb_a, cheb, coord_a, coord)
    phi_z = face(jnp.stack([coef_lo[2], coef_hi[2]]), cheb_a, cheb, coord_a, coord)

    sine_k = lax.dynamic_slice_in_dim(sine, iy * kb, kb, 1)
    hat_x = jnp.einsum("yz,zk->yk", phi_x, sine_k, precision=HIGH)
    hat_x = jnp.einsum("jy,yk->jk", sine, hat_x, precision=HIGH)
    hat_y = jnp.einsum("faz,zk->fak", phi_y, sine_k, precision=HIGH)
    hat_z = jnp.einsum("fay,yj->faj", phi_z, sine, precision=HIGH)
    hat_y = hat_y.reshape(2, pack, sub, kb).transpose(0, 2, 1, 3).reshape(2, sub, 1, width)
    add = hat_y[0] * edge_rows[0][None, :, None] + hat_y[1] * edge_rows[1][None, :, None]
    add = add + jnp.einsum(
        "csj,lc->sjl", hat_z.reshape(2 * pack, sub, n), edge_lane, precision=HIGH
    )
    rhs2 = rhs + add
    blank = jnp.zeros((n, width - kb), jnp.float32)
    rhs2 = rhs2.at[0].add(own_x[0] * jnp.concatenate([hat_x, blank], axis=1))
    rhs2 = rhs2.at[sub - 1].add(own_x[1] * jnp.concatenate([blank, hat_x], axis=1))
    potential, energy_two = backward(plan, rhs2, first, tab, split_table(sine64 * norm), sz)
    energy_two = h * norm * jnp.sum(energy_two)
    return potential, jnp.stack([energy_one, energy_two])


def solution(mesh):
    return jax.shard_map(
        shards,
        mesh=mesh,
        in_specs=(P("gx", "gy", None),),
        out_specs=(P("gx", "gy", None), P()),
        check_vma=False,
    )
```

```python
import functools
import math

import jax
import jax.numpy as jnp
import numpy as np
from jax import lax
from jax.experimental import pallas as pl
from jax.experimental.pallas import tpu as pltpu
from jax.sharding import PartitionSpec as P

ORDER = 16
DEG = ORDER + 1
RATIO = 1.1
RADIUS = math.sqrt(3.0) / 2.0
LANES = 128
MESH = pl.DeviceIdType.MESH
BF16 = jnp.bfloat16
EVEN = -(-((DEG + 1) // 2) // 8) * 8
ROWS = EVEN + -(-(DEG // 2) // 8) * 8
BLOCK = 32
PER = LANES // BLOCK
NBLK = -(-DEG // PER)
MI = (DEG + 1) // 2


def solid_harmonics(x, y, z):
    rr = x * x + y * y + z * z
    out = np.zeros((DEG, 2 * DEG - 1) + x.shape)
    cos = np.zeros((DEG, DEG) + x.shape)
    sin = np.zeros((DEG, DEG) + x.shape)
    cos[0, 0] = 1.0
    for l in range(1, DEG):
        s = 1.0 if l == 1 else math.sqrt((2 * l - 1) / (2.0 * l))
        cos[l, l] = s * (x * cos[l - 1, l - 1] - y * sin[l - 1, l - 1])
        sin[l, l] = s * (x * sin[l - 1, l - 1] + y * cos[l - 1, l - 1])
        for m in range(l):
            div = math.sqrt(l * l - m * m)
            far = math.sqrt((l - 1) * (l - 1) - m * m) if l - 1 > m else 0.0
            for f in (cos, sin):
                f[l, m] = (2 * l - 1) * z * f[l - 1, m] / div
                if l >= 2 and far:
                    f[l, m] = f[l, m] - far * rr * f[l - 2, m] / div
    out[:, :DEG] = cos
    out[:, DEG:] = sin[:, 1:]
    return out


def face_tensors():
    t = np.cos(np.pi * (np.arange(DEG) + 0.5) / DEG)
    fwd = np.cos(np.arange(DEG)[:, None] * np.arccos(t)[None, :]) * (2.0 / DEG)
    fwd[0] *= 0.5
    u, v = np.meshgrid(t / 2, t / 2, indexing="ij")
    half = np.full_like(u, 0.5)
    tensors = []
    for pts in ((half, u, v), (u, half, v), (u, v, half)):
        vals = solid_harmonics(*pts)
        tensors.append(np.einsum("pu,lfuv,qv->lfpq", fwd, vals, fwd))
    return np.stack(tensors)


def expansion_weights():
    w = np.zeros((DEG, 2 * DEG - 1))
    for l in range(DEG):
        for f in range(2 * DEG - 1):
            m = f if f < DEG else f - ORDER
            w[l, f] = (1.0 if m == 0 else 2.0) / (4.0 * math.pi * RADIUS * RATIO ** (l + 1))
    return w.astype(np.float32)


def split(x):
    hi = x.astype(jnp.bfloat16)
    return hi, (x - hi.astype(jnp.float32)).astype(jnp.bfloat16)


def dot(a, b):
    return jnp.dot(a, b, preferred_element_type=jnp.float32)


def left_mul(mat, x):
    hi, lo = split(x)
    return dot(mat[0], hi) + dot(mat[0], lo) + dot(mat[1], hi)


def right_mul(x, mat):
    hi, lo = split(x)
    return dot(hi, mat[0]) + dot(lo, mat[0]) + dot(hi, mat[1])


def dot_t(a, b):
    return lax.dot_general(a, b, (((1,), (1,)), ((), ())), preferred_element_type=jnp.float32)


def split_table(table):
    t = np.asarray(table, np.float32)
    hi = t.astype(BF16)
    return hi, (t - hi.astype(np.float32)).astype(BF16)


def turn(x, shift):
    width = x.shape[-1]
    shift %= width
    return pltpu.roll(x, shift, x.ndim - 1) if shift else x


class Plan:
    def __init__(self, ca, cb, n, gx, gy):
        self.ca, self.cb, self.n, self.gx, self.gy = ca, cb, n, gx, gy
        self.kb = n // gy
        self.h = 1.0 / (n + 1)
        self.norm = (2.0 * self.h) ** 2
        self.jb = n // gx
        self.width = LANES
        self.pack = LANES // self.kb
        self.sub = ca // self.pack
        self.step = max(1, self.sub // 8)
        self.pair = 2 if self.step % 2 == 0 else 1
        self.chunks = self.sub // self.step
        self.tile = min(n, 64)

    def lanes(self, rows):
        return lax.broadcasted_iota(jnp.int32, (rows, LANES), 1) // self.kb


def greet(p):
    ix, iy = lax.axis_index("gx"), lax.axis_index("gy")
    barrier = pltpu.get_barrier_semaphore()
    for d in range(1, p.gx):
        pl.semaphore_signal(barrier, inc=1, device_id={"gx": lax.rem(ix + d, p.gx)}, device_id_type=MESH)
    for d in range(1, p.gy):
        pl.semaphore_signal(barrier, inc=1, device_id={"gy": lax.rem(iy + d, p.gy)}, device_id_type=MESH)
    pl.semaphore_wait(barrier, p.gx + p.gy - 2)


def remote(src, dst, send, recv, where):
    return pltpu.make_async_remote_copy(
        src_ref=src, dst_ref=dst, send_sem=send, recv_sem=recv, device_id=where, device_id_type=MESH
    )


def mode_tables(p, epsj_ref, epsk_ref, tab_ref):
    iy = lax.axis_index("gy")
    sigma = epsj_ref[0] + epsk_ref[iy][0:1]
    s = 0.5 * jnp.sqrt(sigma)
    t = jnp.sqrt(1.0 + s * s)
    theta = 2.0 * jnp.log1p(s + s * s / (1.0 + t))
    lam = jnp.exp(-theta)
    tab_ref[0] = lam
    tab_ref[1] = p.h * p.h / (4.0 * s * t)
    tab_ref[2] = jnp.exp(-theta * float(p.sub))
    tab_ref[3] = jnp.exp(-theta * float(p.ca))
    tab_ref[4] = lam / (1.0 - jnp.exp(-theta * (2.0 * (p.n + 1))))
    tab_ref[5] = jnp.exp(-theta * float(p.n + 1))


def edge_sums(p, v_ref, tab_ref, left_ref, right_ref, edge_ref):
    for t in range(p.n // p.tile):
        rows = pl.ds(t * p.tile, p.tile)
        lam, lsub = tab_ref[0, rows], tab_ref[2, rows]
        left, right = v_ref[0, rows], v_ref[p.sub - 1, rows]
        for i in range(1, p.sub):
            left = left * lam + v_ref[i, rows]
            right = right * lam + v_ref[p.sub - 1 - i, rows]
        left_ref[rows] = left
        right_ref[rows] = right
        dev_l, dev_r = left, right
        for g in range(1, p.pack):
            dev_l = dev_l * lsub + turn(left, -g * p.kb)
            dev_r = dev_r * lsub + turn(right, g * p.kb)
        edge_ref[rows] = jnp.where(p.lanes(p.tile) == 0, dev_l, dev_r)


def line_exchange(p, tab_ref, edge_ref, got_ref, back_ref, ends_ref, sems, between):
    ix = lax.axis_index("gx")
    mine = pl.ds(ix * p.jb, p.jb)

    def copies(src, dst, base):
        out = []
        for d in range(1, p.gx):
            r = lax.rem(ix + d, p.gx)
            out.append(remote(src(r), dst, sems.at[base, d], sems.at[base + 1, d], {"gx": r}))
        return out

    first = copies(lambda r: edge_ref.at[pl.ds(r * p.jb, p.jb)], got_ref.at[ix], 0)
    for c in first:
        c.start()
    got_ref[ix] = edge_ref[mine]
    between(0)
    for c in first:
        c.wait_recv()
    lower = p.lanes(p.jb) == 0
    blk, det, lnp = tab_ref[3, mine], tab_ref[4, mine], tab_ref[5, mine]
    state = jnp.zeros((p.jb, LANES), jnp.float32)
    states = []
    for t in range(p.gx):
        states.append(state)
        state = state * blk + jnp.where(lower, got_ref[t], got_ref[p.gx - 1 - t])
    other = jnp.where(lower, turn(state, p.kb), turn(state, -p.kb))
    image = (other - state * lnp) * det
    for t in range(p.gx):
        states[t] = states[t] - image
        image = image * blk
    for t in range(p.gx):
        back_ref[t] = jnp.where(lower, states[t], states[p.gx - 1 - t])
    second = copies(lambda r: back_ref.at[r], ends_ref.at[mine], 2)
    for c in second:
        c.start()
    ends_ref[mine] = back_ref[ix]
    between(1)
    for c in second:
        c.wait_recv()
    for c in first + second:
        c.wait_send()


def carries(p, rows, tab_ref, left_ref, right_ref, ends_ref):
    lsub = tab_ref[2, rows]
    left, right = left_ref[rows], right_ref[rows]
    a = b = ends_ref[rows]
    place = p.lanes(p.tile)
    for g in range(p.pack - 1):
        a = jnp.where(place == g + 1, turn(a * lsub + left, p.kb), a)
        h = p.pack - 1 - g
        b = jnp.where(place == h - 1, turn(b * lsub + right, -p.kb), b)
    return a, b


def row_degrees():
    deg = np.full(ROWS, -1)
    deg[: (DEG + 1) // 2] = np.arange(0, DEG, 2)
    deg[EVEN : EVEN + DEG // 2] = np.arange(1, DEG, 2)
    return deg


def harmonic_tables(p):
    tens = face_tensors()
    deg = row_degrees()
    weights = expansion_weights() * (RADIUS ** -np.arange(DEG, dtype=np.float64))[:, None] * (p.norm / p.h)
    big = np.zeros((3, MI, ROWS, NBLK * LANES))
    sign = np.ones((3, ROWS, NBLK * LANES))
    gain = np.zeros((2, NBLK, 16, LANES))
    for l in range(DEG):
        for face in range(3):
            for i in range(ROWS):
                r = deg[i]
                if r < 0:
                    continue
                for q in range(DEG):
                    if face == 0:
                        odd, mpar = r % 2, (l - q) % 2
                    elif face == 1:
                        mpar = (l - q) % 2
                        odd = (r + mpar) % 2
                    else:
                        odd = q % 2
                        mpar = (r + odd) % 2
                    at = l * BLOCK + q
                    sign[face, i, at] = (-1.0) ** (mpar + odd, odd, l + mpar)[face]
                    for mi in range(MI):
                        m = mpar + 2 * mi
                        if m <= l and not (odd and m == 0):
                            big[face, mi, i, at] = tens[face, l, ORDER + m if odd else m][r, q]
        for c in range(2):
            for odd in range(2):
                for mi in range(MI):
                    m = (l - c) % 2 + 2 * mi
                    if m <= l:
                        at = (l % PER) * BLOCK + c
                        gain[odd, l // PER, mi, at : (l % PER + 1) * BLOCK : 2] = weights[l, m]
    return big.astype(np.float32), sign.astype(np.float32), gain.astype(np.float32)


def tables(p):
    n = p.n
    num = np.arange(n) + 1
    sine = np.sin(np.pi * ((num[:, None] * num[None, :]) % (2 * (n + 1))) / (n + 1))
    eps = 4.0 * np.sin(np.pi * num / (2.0 * (n + 1))) ** 2
    cheb = np.cos(np.arange(DEG)[None, :] * np.arccos((2.0 * np.arange(n) - (n - 1)) * p.h)[:, None])
    hat = sine @ cheb
    deg = row_degrees()
    used = deg >= 0
    jtab = np.stack([np.repeat(v[:, None], LANES, axis=1) for v in (eps, sine[0])])
    ktab = np.zeros((p.gy, 8, LANES))
    for r, v in enumerate((eps, sine[0], sine[n - 1])):
        ktab[:, r] = np.tile(v.reshape(p.gy, p.kb), (1, p.pack))
    wide = np.zeros((ROWS + 8, n))
    wide[:ROWS][used] = hat[:, deg[used]].T
    wide[ROWS], wide[ROWS + 1] = sine[0], sine[n - 1]
    lanes = np.zeros((n, LANES))
    for i in range(PER):
        lanes[:, i * BLOCK : i * BLOCK + DEG] = hat
    rows = np.zeros((n, BLOCK))
    rows[:, :ROWS][:, used] = cheb[:, deg[used]]
    rh, rl = split_table(rows)
    cols = np.zeros((BLOCK, n))
    cols[:DEG] = cheb.T
    ch, cl = split_table(cols)
    same = np.arange(LANES)
    same = (same[:, None] // BLOCK == same[None, :] // BLOCK) & ((same[:, None] - same[None, :]) % 2 == 0)
    big, sign, gain = harmonic_tables(p)
    f32 = np.float32
    return [
        np.stack(split_table(sine)),
        jtab.astype(f32),
        ktab.astype(f32),
        np.stack(split_table(wide)),
        lanes.astype(f32),
        np.concatenate([rh, rl, rh, np.zeros_like(rh)], axis=1),
        np.concatenate([ch, ch, cl, np.zeros_like(ch)], axis=0),
        big,
        sign,
        gain,
        same.astype(BF16),
    ]


def iota(shape, dim):
    return lax.broadcasted_iota(jnp.int32, shape, dim)


def face_prep(p, dmat_ref, rx_ref, ra_ref):
    ix = lax.axis_index("gx")
    shape = (p.sub, LANES)
    cell = ix * p.ca + (iota(shape, 1) // p.kb) * p.sub + iota(shape, 0)
    t = (2 * cell - (p.n - 1)).astype(jnp.float32) * p.h
    prev, cur = jnp.ones(shape, jnp.float32), t
    dmat_ref[0] = prev
    for d in range(1, DEG):
        dmat_ref[d] = cur
        prev, cur = cur, 2.0 * t * cur - prev
    def inverse_radius(rows, start):
        u = (2 * (start + iota((rows, p.n), 0)) - (p.n - 1)).astype(jnp.float32) * (0.5 * p.h)
        v = (2 * iota((rows, p.n), 1) - (p.n - 1)).astype(jnp.float32) * (0.5 * p.h)
        return lax.rsqrt(0.25 + u * u + v * v)
    rx_ref[...] = inverse_radius(p.n, 0)
    ra_ref[...] = inverse_radius(p.ca, ix * p.ca)


def moments(p, first_ref, rhs_ref, w_ref, v_ref, ktab_ref, dmat_ref, g_ref, y_ref, pay_ref):
    ix, iy = lax.axis_index("gx"), lax.axis_index("gy")
    pair = 2 if p.sub % 2 == 0 else 1
    energy = jnp.zeros((8, LANES), jnp.float32)
    for s in range(0, p.sub, pair):
        x = jnp.concatenate([first_ref[s + e] for e in range(pair)], axis=1)
        y = left_mul(w_ref, x)
        for e in range(pair):
            g_ref[s + e] = y[:, e * LANES:(e + 1) * LANES]
    for s in range(p.sub):
        prod = first_ref[s] * rhs_ref[s]
        for r in range(p.n // 8):
            energy = energy + prod[r * 8:(r + 1) * 8]
    y_ref[...] = jnp.zeros_like(y_ref)
    row_of = {d: i for i, d in enumerate(row_degrees()) if d >= 0}
    lane = iota((ROWS, LANES), 1)
    edge = [ktab_ref[iy][1:2], ktab_ref[iy][2:3]]
    mz = jnp.zeros((ROWS, LANES), jnp.float32)
    for d in range(DEG):
        acc = g_ref[0] * dmat_ref[d, 0:1]
        for s in range(1, p.sub):
            acc = acc + g_ref[s] * dmat_ref[d, s:s + 1]
        for f in range(2):
            at = f * ROWS + row_of[d]
            y_ref[at:at + 1] = acc[ROWS + f:ROWS + f + 1]
            total = jnp.sum(acc[:ROWS] * edge[f], axis=1, keepdims=True)
            mz = jnp.where(lane == f * BLOCK + d, total, mz)
    place = lane // p.kb
    lo = jnp.where((place == 0) & (ix == 0), g_ref[0][:ROWS], 0.0)
    hi = jnp.where((place == p.pack - 1) & (ix == p.gx - 1), g_ref[p.sub - 1][:ROWS], 0.0)
    x = jnp.concatenate([lo, hi, y_ref[...]], axis=0)
    table = v_ref[pl.ds(pl.multiple_of(iy * p.kb, 16), p.kb)]
    y = right_mul(x, split(jnp.concatenate([table] * p.pack, axis=0)))
    which = lane // BLOCK
    packed = y[0:ROWS]
    for i in range(1, 4):
        packed = jnp.where(which == i, y[i * ROWS:(i + 1) * ROWS], packed)
    pay_ref[0:ROWS] = packed
    pay_ref[ROWS:2 * ROWS] = mz
    pay_ref[2 * ROWS:2 * ROWS + 8] = energy


def sum_slots(ref, count):
    total = ref[0]
    for i in range(1, count):
        total = total + ref[i]
    return total


def total_copies(p, src_ref, slots_ref, sems, axis, base):
    size = p.gx if axis == "gx" else p.gy
    me = lax.axis_index(axis)
    out = []
    for d in range(1, size):
        r = lax.rem(me + d, size)
        out.append(remote(src_ref, slots_ref.at[me], sems.at[base, d], sems.at[base + 1, d], {axis: r}))
    return out


def all_sum(p, pay_ref, xs_ref, sum_ref, ys_ref, sems):
    ix, iy = lax.axis_index("gx"), lax.axis_index("gy")
    a = total_copies(p, pay_ref, xs_ref, sems, "gx", 0)
    for c in a:
        c.start()
    xs_ref[ix] = pay_ref[...]
    for c in a:
        c.wait_recv()
    total = sum_slots(xs_ref, p.gx)
    sum_ref[...] = total
    b = total_copies(p, sum_ref, ys_ref, sems, "gy", 2)
    for c in b:
        c.start()
    ys_ref[iy] = total
    for c in b:
        c.wait_recv()
    for c in a + b:
        c.wait_send()
    return sum_slots(ys_ref, p.gy)


def trade(x):
    odd = iota(x.shape, 1) % 2 == 1
    return jnp.where(odd, turn(x, 1), turn(x, -1))


def coefficients(p, packed, mz, big_ref, sign_ref, gain_ref, same_ref, s_ref, coef_ref):
    which = iota((ROWS, LANES), 1) // BLOCK

    def spread(x, i):
        x = turn(jnp.where(which == i, x, 0.0), -i * BLOCK)
        x = x + turn(x, BLOCK)
        return x + turn(x, 2 * BLOCK)

    tall = (BLOCK, LANES)
    row, col = iota(tall, 0), iota(tall, 1)
    degree = jnp.where(row < EVEN, 2 * row, 2 * (row - EVEN) + 1)
    place = (col % BLOCK == degree).astype(jnp.float32).astype(BF16)
    mz = split(jnp.concatenate([mz, jnp.zeros((BLOCK - ROWS, LANES), jnp.float32)], axis=0))

    def flip(f):
        pick = (col == f * BLOCK + degree).astype(jnp.float32).astype(BF16)
        hi, lo = split(dot_t(pick, mz[0]) + dot_t(pick, mz[1]))
        return (dot(hi, place) + dot(lo, place))[:ROWS]

    pairs = [(spread(packed, 0), spread(packed, 1)), (spread(packed, 2), spread(packed, 3)), (flip(0), flip(1))]
    s_ref[...] = jnp.zeros_like(s_ref)
    for face in range(3):
        lo, hi = pairs[face]
        for blk in range(NBLK):
            cols = slice(blk * LANES, (blk + 1) * LANES)
            both = hi + sign_ref[face][:, cols] * lo
            for mi in range(MI):
                prod = big_ref[face, mi][:, cols] * both
                s_ref[face, 0, blk, mi:mi + 1] = jnp.sum(prod[:EVEN], axis=0, keepdims=True)
                s_ref[face, 1, blk, mi:mi + 1] = jnp.sum(prod[EVEN:], axis=0, keepdims=True)
    hi, lo = split(s_ref[...].reshape(6 * NBLK * 16, LANES))
    spread_sum = (dot(hi, same_ref[...]) + dot(lo, same_ref[...])).reshape(3, 2, NBLK, 16, LANES)
    lane = iota((16, LANES), 1)
    for blk in range(NBLK):
        l = blk * PER + lane // BLOCK
        right = lane % 2 == 1
        cross = (l - lane) % 2 == 1
        sx, sy, sz = spread_sum[0], spread_sum[1], spread_sum[2]
        lm = []
        for b in range(2):
            wide = [jnp.where((lane + b) % 2 == 0, sz[a, blk], trade(sz[a, blk])) for a in range(2)]
            other = jnp.where((l + lane + b) % 2 == 1, wide[1], wide[0])
            lm.append((sx[b, blk] + jnp.where(cross, sy[1 - b, blk], sy[b, blk]) + other) * gain_ref[b, blk])
        rows = [lm, [jnp.where(cross, lm[1 - b], lm[b]) for b in range(2)],
                [jnp.where(right, *[jnp.where((l + a) % 2 == 1, trade(lm[b]), lm[b]) for b in (1, 0)]) for a in range(2)]]
        cols = slice(blk * LANES, (blk + 1) * LANES)
        for face in range(3):
            even = jnp.zeros((EVEN, LANES), jnp.float32)
            odd = jnp.zeros((ROWS - EVEN, LANES), jnp.float32)
            for mi in range(MI):
                t = big_ref[face, mi][:, cols]
                even = even + t[:EVEN] * rows[face][0][mi:mi + 1]
                odd = odd + t[EVEN:] * rows[face][1][mi:mi + 1]
            coef_ref[face, blk] = jnp.concatenate([even, odd], axis=0)


def face_coefs(p, coef_ref, sign_ref, c3_ref):
    ix = lax.axis_index("gx")
    which = iota((ROWS, LANES), 1) // BLOCK
    gap = jnp.zeros((BLOCK - ROWS, LANES), jnp.float32)
    rest = jnp.zeros((LANES - 3 * BLOCK, LANES), jnp.float32)
    for l in range(DEG):
        blk, i = divmod(l, PER)
        cols = slice(blk * LANES, (blk + 1) * LANES)
        for face in range(3):
            hi = coef_ref[face, blk]
            lo = hi * sign_ref[face][:, cols]
            for k, c in enumerate([jnp.where(ix == 0, lo, hi)] if face == 0 else [lo, hi]):
                c = turn(jnp.where(which == i, c, 0.0), -i * BLOCK)
                c = c + turn(c, BLOCK) + turn(c, 2 * BLOCK)
                top = c.astype(BF16).astype(jnp.float32)
                full = jnp.concatenate([top, gap, top, gap, c - top, gap, rest], axis=0)
                c3_ref[l, max(0, 2 * face - 1) + k] = full.astype(BF16)


def triple(e):
    top = e.astype(BF16).astype(jnp.float32)
    return jnp.where(iota(e.shape, 1) // BLOCK == 1, e - top, top).astype(BF16)


def faces(p, c3_ref, cu_ref, vt_ref, rx_ref, ra_ref, fx_ref, fa_ref):
    ix = lax.axis_index("gx")
    edge = (ix == 0) | (ix == p.gx - 1)
    fa_ref[...] = jnp.zeros_like(fa_ref)
    near = pl.ds(pl.multiple_of(ix * p.ca, 16), p.ca)

    @pl.when(edge)
    def _():
        fx_ref[...] = jnp.zeros_like(fx_ref)

        def step(i, carry):
            e = dot(cu_ref[...], c3_ref[DEG - 1 - i, 0])
            fx_ref[...] = fx_ref[...] * rx_ref[...] + dot(triple(e), vt_ref[...])
            return carry

        lax.fori_loop(0, DEG, step, 0)

    def step(i, carry):
        e = dot(cu_ref[near], jnp.concatenate([c3_ref[DEG - 1 - i, k] for k in range(1, 5)], axis=1))
        e = jnp.concatenate([e[:, k * LANES:(k + 1) * LANES] for k in range(4)], axis=0)
        ra = jnp.concatenate([ra_ref[...]] * 4, axis=0)
        fa_ref[...] = fa_ref[...] * ra + dot(triple(e), vt_ref[...])
        return carry

    lax.fori_loop(0, DEG, step, 0)


def add_faces(p, rhs_ref, sine_ref, jtab_ref, ktab_ref, fx_ref, fa_ref):
    ix, iy = lax.axis_index("gx"), lax.axis_index("gy")
    ca = p.ca
    chunk = pl.ds(pl.multiple_of(iy * p.kb, 16), p.kb)
    near = [jnp.concatenate([sine_ref[i, chunk]] * p.pack, axis=0) for i in range(2)]

    def to_lanes(x):
        hi, lo = split(x)
        return dot_t(hi, near[0]) + dot_t(lo, near[0]) + dot_t(hi, near[1])

    @pl.when((ix == 0) | (ix == p.gx - 1))
    def _():
        hat = left_mul(sine_ref, to_lanes(fx_ref[...]))
        place = p.lanes(p.n)
        rhs_ref[0] += jnp.where((place == 0) & (ix == 0), hat, 0.0)
        rhs_ref[p.sub - 1] += jnp.where((place == p.pack - 1) & (ix == p.gx - 1), hat, 0.0)

    hy = to_lanes(fa_ref[0:2 * ca])
    place = p.lanes(p.sub)
    planes = []
    for f in range(2):
        acc = hy[f * ca:f * ca + p.sub]
        for g in range(1, p.pack):
            acc = jnp.where(place == g, hy[f * ca + g * p.sub:f * ca + (g + 1) * p.sub], acc)
        planes.append(acc)
    plus, minus = planes[0] + planes[1], planes[0] - planes[1]

    hi, lo = split(jnp.concatenate([fa_ref[2 * ca:4 * ca]] * (LANES // (2 * ca)), axis=0))
    hz = dot_t(sine_ref[0], hi) + dot_t(sine_ref[1], hi) + dot_t(sine_ref[0], lo)
    top = hz.astype(BF16).astype(jnp.float32)
    both = jnp.where(iota(hz.shape, 1) // (2 * ca) == 1, hz - top, top).astype(BF16)
    top = top.astype(BF16)
    square = (LANES, LANES)
    row, col = iota(square, 0), iota(square, 1)
    edge = jnp.where(row % (2 * ca) < ca, ktab_ref[iy][1:2], ktab_ref[iy][2:3])
    head = edge.astype(BF16).astype(jnp.float32)
    fits = (row % ca) // p.sub == col // p.kb
    first = jnp.where(fits & (row // (2 * ca) < 2), head, 0.0)
    second = jnp.where(fits & (row < 2 * ca), edge - head, 0.0)
    pair = 2 if p.sub % 2 == 0 else 1
    even = iota((p.n, LANES), 0) % 2 == 0
    for s in range(0, p.sub, pair):
        pick = [row % p.sub == s + e for e in range(pair)]
        one = jnp.concatenate([jnp.where(k, first, 0.0).astype(BF16) for k in pick], axis=1)
        two = jnp.concatenate([jnp.where(k, second, 0.0).astype(BF16) for k in pick], axis=1)
        add = dot(both, one) + dot(top, two)
        for e in range(pair):
            at = s + e
            wave = jnp.where(even, plus[at:at + 1], minus[at:at + 1])
            rhs_ref[at] += add[:, e * LANES:(e + 1) * LANES] + jtab_ref[1] * wave


def kernel(p, rho_ref, *refs):
    names = ("sine", "jtab", "ktab", "wide", "lanes", "cu", "vt", "big", "sign", "gain", "same")
    hbm = refs[:len(names)]
    out_ref, energy_ref = refs[len(names):len(names) + 2]
    rest = refs[len(names) + 2:]
    local = rest[:len(names)]
    (x_ref, send_ref, spec_ref, rhs_ref, first_ref, tab_ref, left_ref, right_ref, edge_ref, carry_ref,
     got_ref, back_ref, ends_ref, got2_ref, back2_ref, ends2_ref,
     dmat_ref, rx_ref, ra_ref, g_ref, y_ref, pay_ref, pxs_ref, psum_ref, pys_ref,
     s_ref, coef_ref, c3_ref, fx_ref, fa_ref,
     part_ref, xs_ref, sum_ref, ys_ref, u_ref, res_ref, fin_ref,
     table_sems, in_sems, out_sems, land_sems, back_out_sems, back_land_sems,
     line_sems, line2_sems, pay_sems, sum_sems, write_sems) = rest[len(names):]
    sine_ref, jtab_ref, ktab_ref, wide_ref, lanes_ref, cu_ref, vt_ref, big_ref, sign_ref, gain_ref, same_ref = local
    w_ref = spec_ref
    ix, iy = lax.axis_index("gx"), lax.axis_index("gy")
    order = list(range(p.gy // 2, p.gy)) + list(range(1, p.gy // 2))
    block = p.step * p.cb
    staged = [pltpu.make_async_copy(hbm[i], local[i], table_sems.at[i]) for i in range(len(names))]

    def load(c, g):
        rows = pl.ds(g * p.sub + c * p.step, p.step)
        return pltpu.make_async_copy(rho_ref.at[rows], x_ref.at[rows], in_sems.at[c, g])

    staged[0].start()
    for c in range(p.chunks):
        for g in range(p.pack):
            load(c, g).start()
    for copy in staged[1:]:
        copy.start()
    greet(p)
    staged[0].wait()

    def swap(c, d):
        q = lax.rem(iy + d, p.gy)
        planes = pl.ds(c * p.step, p.step)
        return remote(send_ref.at[q, planes], spec_ref.at[planes, pl.ds(iy * p.cb, p.cb)],
                      out_sems.at[c, d], land_sems.at[c, d], {"gy": q})

    def transform(c, carry):
        for g in range(p.pack):
            load(c, g).wait()
        x = jnp.concatenate(
            [x_ref[pl.ds(g * p.sub + c * p.step, p.step)].reshape(block, p.n) for g in range(p.pack)], axis=0
        )
        y = right_mul(x, sine_ref)
        place = p.lanes(block)
        planes = pl.ds(c * p.step, p.step)
        for q in range(p.gy):
            col, off = divmod(q * p.kb, LANES)
            piece = None
            for g in range(p.pack):
                part = turn(y[g * block:(g + 1) * block, col * LANES:(col + 1) * LANES], g * p.kb - off)
                piece = part if piece is None else jnp.where(place == g, part, piece)
            send_ref[q, planes] = piece.reshape(p.step, p.cb, LANES)

        @pl.when(c > 0)
        def _():
            for d in order:
                swap(c - 1, d).start()

        spec_ref[planes, pl.ds(iy * p.cb, p.cb)] = send_ref[iy, planes]
        return carry

    lax.fori_loop(0, p.chunks, transform, 0)
    staged[1].wait()
    staged[2].wait()
    mode_tables(p, jtab_ref, ktab_ref, tab_ref)
    for d in order:
        swap(p.chunks - 1, d).start()
    face_prep(p, dmat_ref, rx_ref, ra_ref)

    def across(c, carry):
        for d in order:
            swap(c, d).wait_recv()
        for i in range(0, p.step, p.pair):
            s = c * p.step + i
            x = jnp.concatenate([spec_ref[s + e] for e in range(p.pair)], axis=1)
            y = left_mul(sine_ref, x)
            for e in range(p.pair):
                rhs_ref[s + e] = y[:, e * LANES:(e + 1) * LANES]
        return carry

    lax.fori_loop(0, p.chunks, across, 0)
    edge_sums(p, rhs_ref, tab_ref, left_ref, right_ref, edge_ref)
    line_exchange(p, tab_ref, edge_ref, got_ref, back_ref, ends_ref, line_sems, lambda stage: None)

    for t in range(p.n // p.tile):
        rows = pl.ds(t * p.tile, p.tile)
        lam, inv = tab_ref[0, rows], tab_ref[1, rows]
        a, b = carries(p, rows, tab_ref, left_ref, right_ref, ends_ref)
        for i in range(p.sub - 1, -1, -1):
            b = b * lam
            first_ref[i, rows] = b
            b = b + rhs_ref[i, rows]
        for i in range(p.sub):
            a = a * lam + rhs_ref[i, rows]
            first_ref[i, rows] = (a + first_ref[i, rows]) * inv

    def drain(c, carry):
        for d in order:
            swap(c, d).wait_send()
        return carry

    lax.fori_loop(0, p.chunks, drain, 0)
    for copy in staged[3:]:
        copy.wait()

    moments(p, first_ref, rhs_ref, wide_ref, lanes_ref, ktab_ref, dmat_ref, g_ref, y_ref, pay_ref)
    total = all_sum(p, pay_ref, pxs_ref, psum_ref, pys_ref, pay_sems)
    energy_one = jnp.sum(total[2 * ROWS:2 * ROWS + 8])
    coefficients(p, total[:ROWS], total[ROWS:2 * ROWS], big_ref, sign_ref, gain_ref, same_ref, s_ref, coef_ref)
    face_coefs(p, coef_ref, sign_ref, c3_ref)
    faces(p, c3_ref, cu_ref, vt_ref, rx_ref, ra_ref, fx_ref, fa_ref)
    add_faces(p, rhs_ref, sine_ref, jtab_ref, ktab_ref, fx_ref, fa_ref)

    edge_sums(p, rhs_ref, tab_ref, left_ref, right_ref, edge_ref)
    ea = total_copies(p, part_ref, xs_ref, sum_sems, "gx", 0)
    eb = total_copies(p, sum_ref, ys_ref, sum_sems, "gy", 2)

    def between(stage):
        if stage == 0:
            energy = jnp.zeros((8, LANES), jnp.float32)
            for i in range(p.sub):
                prod = first_ref[i] * rhs_ref[i]
                for r in range(p.n // 8):
                    energy = energy + prod[r * 8:(r + 1) * 8]
            part_ref[...] = energy
            xs_ref[ix] = energy
            return
        for c in ea:
            c.start()

    line_exchange(p, tab_ref, edge_ref, got2_ref, back2_ref, ends2_ref, line2_sems, between)
    for t in range(p.n // p.tile):
        rows = pl.ds(t * p.tile, p.tile)
        lam = tab_ref[0, rows]
        a, b = carries(p, rows, tab_ref, left_ref, right_ref, ends2_ref)
        carry_ref[rows] = a
        for i in range(p.sub - 1, -1, -1):
            b = b * lam
            first_ref[i, rows] = b
            b = b + rhs_ref[i, rows]
    for c in ea:
        c.wait_recv()
    total = sum_slots(xs_ref, p.gx)
    sum_ref[...] = total
    ys_ref[iy] = total

    def swap_back(c, d):
        q = lax.rem(iy + d, p.gy)
        planes = pl.ds(c * p.step, p.step)
        return remote(u_ref.at[planes, pl.ds(q * p.cb, p.cb)], res_ref.at[iy, planes],
                      back_out_sems.at[c, d], back_land_sems.at[c, d], {"gy": q})

    def back_across(c, carry):
        for t in range(p.n // p.tile):
            rows = pl.ds(t * p.tile, p.tile)
            lam, inv = tab_ref[0, rows], tab_ref[1, rows] * p.norm
            a = carry_ref[rows]
            for i in range(p.step):
                s = c * p.step + i
                a = a * lam + rhs_ref[s, rows]
                first_ref[s, rows] = (a + first_ref[s, rows]) * inv
            carry_ref[rows] = a
        for i in range(0, p.step, p.pair):
            s = c * p.step + i
            x = jnp.concatenate([first_ref[s + e] for e in range(p.pair)], axis=1)
            y = left_mul(sine_ref, x)
            for e in range(p.pair):
                u_ref[s + e] = y[:, e * LANES:(e + 1) * LANES]
        planes = pl.ds(c * p.step, p.step)

        @pl.when(c > 0)
        def _():
            for d in order:
                swap_back(c - 1, d).start()

        res_ref[iy, planes] = u_ref[planes, pl.ds(iy * p.cb, p.cb)]
        return carry

    lax.fori_loop(0, p.chunks, back_across, 0)
    for c in eb:
        c.start()
    for d in order:
        swap_back(p.chunks - 1, d).start()

    def write(c, g):
        rows = pl.ds(g * p.sub + c * p.step, p.step)
        return pltpu.make_async_copy(fin_ref.at[rows], out_ref.at[rows], write_sems.at[c, g])

    def finish(c, carry):
        for d in order:
            swap_back(c, d).wait_recv()
        planes = pl.ds(c * p.step, p.step)
        place = p.lanes(block)
        parts = [res_ref[q, planes].reshape(block, LANES) for q in range(p.gy)]
        per = LANES // p.kb
        rows = []
        for g in range(p.pack):
            cols = []
            for col in range(p.n // LANES):
                acc = None
                for e in range(per):
                    part = turn(parts[col * per + e], (e - g) * p.kb)
                    acc = part if acc is None else jnp.where(place == e, part, acc)
                cols.append(acc)
            rows.append(jnp.concatenate(cols, axis=1))
        y = right_mul(jnp.concatenate(rows, axis=0), sine_ref)
        for g in range(p.pack):
            at = pl.ds(g * p.sub + c * p.step, p.step)
            fin_ref[at] = y[g * block:(g + 1) * block].reshape(p.step, p.cb, p.n)

        @pl.when(c > 0)
        def _():
            for g in range(p.pack):
                write(c - 1, g).start()

        return carry

    lax.fori_loop(0, p.chunks, finish, 0)
    for c in eb:
        c.wait_recv()
    energy_two = jnp.sum(sum_slots(ys_ref, p.gy))
    for g in range(p.pack):
        write(p.chunks - 1, g).start()
    scale = p.h**3 * p.norm
    energy_ref[...] = jnp.where(iota((8, LANES), 1) == 0, energy_one, energy_two) * scale
    for c in range(p.chunks):
        for g in range(p.pack):
            write(c, g).wait()
    for c in ea + eb:
        c.wait_send()

    def back_drain(c, carry):
        for d in order:
            swap_back(c, d).wait_send()
        return carry

    lax.fori_loop(0, p.chunks, back_drain, 0)


def shards(charge_density):
    ca, cb, n = charge_density.shape
    p = Plan(ca, cb, n, lax.axis_size("gx"), lax.axis_size("gy"))
    f32 = jnp.float32
    data = tables(p)
    cube = (p.sub, p.n, LANES)
    plane = (p.n, LANES)
    slots = (p.gx, p.jb, LANES)
    pay = (2 * ROWS + 8, LANES)
    box = (p.gy, p.sub, p.cb, LANES)
    vmem = lambda shape, dtype=f32: pltpu.VMEM(shape, dtype)
    dma = pltpu.SemaphoreType.DMA
    anywhere = pl.BlockSpec(memory_space=pl.ANY)
    whole = (p.ca, p.cb, p.n)
    scratch = [vmem(t.shape, t.dtype) for t in data]
    scratch += [vmem(whole), vmem(box), vmem(cube), vmem(cube), vmem(cube), vmem((6,) + plane)]
    scratch += [vmem(plane)] * 4
    scratch += [vmem(slots), vmem(slots), vmem(plane)] * 2
    scratch += [vmem((DEG, p.sub, LANES)), vmem((p.n, p.n)), vmem((p.ca, p.n)), vmem((p.sub, ROWS + 8, LANES)),
                vmem((2 * ROWS, LANES)), vmem(pay), vmem((p.gx,) + pay), vmem(pay), vmem((p.gy,) + pay)]
    scratch += [vmem((3, 2, NBLK, 16, LANES)), vmem((3, NBLK, ROWS, LANES)), vmem((DEG, 5, LANES, LANES), BF16),
                vmem((p.n, p.n)), vmem((4 * p.ca, p.n))]
    scratch += [vmem((8, LANES)), vmem((p.gx, 8, LANES)), vmem((8, LANES)), vmem((p.gy, 8, LANES)),
                vmem(cube), vmem(box), vmem(whole)]
    most = max(p.gx, p.gy)
    scratch += [dma((len(data),)), dma((p.chunks, p.pack))] + [dma((p.chunks, p.gy))] * 4
    scratch += [dma((4, p.gx))] * 2 + [dma((4, most))] * 2 + [dma((p.chunks, p.pack))]
    potential, energies = pl.pallas_call(
        functools.partial(kernel, p),
        in_specs=[anywhere] * (1 + len(data)),
        out_specs=[anywhere, pl.BlockSpec(memory_space=pltpu.VMEM)],
        out_shape=[jax.ShapeDtypeStruct(whole, f32), jax.ShapeDtypeStruct((8, LANES), f32)],
        scratch_shapes=scratch,
        compiler_params=pltpu.CompilerParams(
            collective_id=0, has_side_effects=True, vmem_limit_bytes=56 * 2**20
        ),
        name="james",
    )(charge_density, *[jnp.asarray(t) for t in data])
    return potential, energies[0, :2]


def solution(mesh):
    return jax.shard_map(
        shards,
        mesh=mesh,
        in_specs=(P("gx", "gy", None),),
        out_specs=(P("gx", "gy", None), P()),
        check_vma=False,
    )
```

```python
import functools
import math

import jax
import jax.numpy as jnp
import numpy as np
from jax import lax
from jax.experimental import pallas as pl
from jax.experimental.pallas import tpu as pltpu
from jax.sharding import PartitionSpec as P

ORDER = 16
DEG = ORDER + 1
RATIO = 1.1
RADIUS = math.sqrt(3.0) / 2.0
LANES = 128
MESH = pl.DeviceIdType.MESH
BF16 = jnp.bfloat16
EVEN = -(-((DEG + 1) // 2) // 8) * 8
ROWS = EVEN + -(-(DEG // 2) // 8) * 8
BLOCK = 32
PER = LANES // BLOCK
NBLK = -(-DEG // PER)
MI = (DEG + 1) // 2
LOT = 2 * PER * NBLK


def solid_harmonics(x, y, z):
    rr = x * x + y * y + z * z
    out = np.zeros((DEG, 2 * DEG - 1) + x.shape)
    cos = np.zeros((DEG, DEG) + x.shape)
    sin = np.zeros((DEG, DEG) + x.shape)
    cos[0, 0] = 1.0
    for l in range(1, DEG):
        s = 1.0 if l == 1 else math.sqrt((2 * l - 1) / (2.0 * l))
        cos[l, l] = s * (x * cos[l - 1, l - 1] - y * sin[l - 1, l - 1])
        sin[l, l] = s * (x * sin[l - 1, l - 1] + y * cos[l - 1, l - 1])
        for m in range(l):
            div = math.sqrt(l * l - m * m)
            far = math.sqrt((l - 1) * (l - 1) - m * m) if l - 1 > m else 0.0
            for f in (cos, sin):
                f[l, m] = (2 * l - 1) * z * f[l - 1, m] / div
                if l >= 2 and far:
                    f[l, m] = f[l, m] - far * rr * f[l - 2, m] / div
    out[:, :DEG] = cos
    out[:, DEG:] = sin[:, 1:]
    return out


def face_tensors():
    t = np.cos(np.pi * (np.arange(DEG) + 0.5) / DEG)
    fwd = np.cos(np.arange(DEG)[:, None] * np.arccos(t)[None, :]) * (2.0 / DEG)
    fwd[0] *= 0.5
    u, v = np.meshgrid(t / 2, t / 2, indexing="ij")
    half = np.full_like(u, 0.5)
    tensors = []
    for pts in ((half, u, v), (u, half, v), (u, v, half)):
        vals = solid_harmonics(*pts)
        tensors.append(np.einsum("pu,lfuv,qv->lfpq", fwd, vals, fwd))
    return np.stack(tensors)


def expansion_weights():
    w = np.zeros((DEG, 2 * DEG - 1))
    for l in range(DEG):
        for f in range(2 * DEG - 1):
            m = f if f < DEG else f - ORDER
            w[l, f] = (1.0 if m == 0 else 2.0) / (4.0 * math.pi * RADIUS * RATIO ** (l + 1))
    return w.astype(np.float32)


def split(x):
    hi = x.astype(jnp.bfloat16)
    return hi, (x - hi.astype(jnp.float32)).astype(jnp.bfloat16)


def dot(a, b):
    return jnp.dot(a, b, preferred_element_type=jnp.float32)


def left_mul(mat, x):
    hi, lo = split(x)
    return dot(mat[0], hi) + dot(mat[0], lo) + dot(mat[1], hi)


def right_mul(x, mat):
    hi, lo = split(x)
    return dot(hi, mat[0]) + dot(lo, mat[0]) + dot(hi, mat[1])


def dot_t(a, b):
    return lax.dot_general(a, b, (((1,), (1,)), ((), ())), preferred_element_type=jnp.float32)


def split_table(table):
    t = np.asarray(table, np.float32)
    hi = t.astype(BF16)
    return hi, (t - hi.astype(np.float32)).astype(BF16)


def turn(x, shift):
    width = x.shape[-1]
    shift %= width
    return pltpu.roll(x, shift, x.ndim - 1) if shift else x


class Plan:
    def __init__(self, ca, cb, n, gx, gy):
        self.ca, self.cb, self.n, self.gx, self.gy = ca, cb, n, gx, gy
        self.kb = n // gy
        self.h = 1.0 / (n + 1)
        self.norm = (2.0 * self.h) ** 2
        self.jb = n // gx
        self.width = LANES
        self.pack = LANES // self.kb
        self.sub = ca // self.pack
        self.step = max(1, self.sub // 8)
        self.pair = 2 if self.step % 2 == 0 else 1
        self.chunks = self.sub // self.step
        self.tile = min(n, 64)

    def lanes(self, rows):
        return lax.broadcasted_iota(jnp.int32, (rows, LANES), 1) // self.kb


def greet(p):
    ix, iy = lax.axis_index("gx"), lax.axis_index("gy")
    barrier = pltpu.get_barrier_semaphore()
    for d in range(1, p.gx):
        pl.semaphore_signal(barrier, inc=1, device_id={"gx": lax.rem(ix + d, p.gx)}, device_id_type=MESH)
    for d in range(1, p.gy):
        pl.semaphore_signal(barrier, inc=1, device_id={"gy": lax.rem(iy + d, p.gy)}, device_id_type=MESH)
    pl.semaphore_wait(barrier, p.gx + p.gy - 2)


def remote(src, dst, send, recv, where):
    return pltpu.make_async_remote_copy(
        src_ref=src, dst_ref=dst, send_sem=send, recv_sem=recv, device_id=where, device_id_type=MESH
    )


def mode_tables(p, epsj_ref, epsk_ref, tab_ref):
    iy = lax.axis_index("gy")
    sigma = epsj_ref[0] + epsk_ref[iy][0:1]
    s = 0.5 * jnp.sqrt(sigma)
    t = jnp.sqrt(1.0 + s * s)
    theta = 2.0 * jnp.log1p(s + s * s / (1.0 + t))
    lam = jnp.exp(-theta)
    tab_ref[0] = lam
    tab_ref[1] = p.h * p.h / (4.0 * s * t)
    tab_ref[2] = jnp.exp(-theta * float(p.sub))
    tab_ref[3] = jnp.exp(-theta * float(p.ca))
    tab_ref[4] = lam / (1.0 - jnp.exp(-theta * (2.0 * (p.n + 1))))
    tab_ref[5] = jnp.exp(-theta * float(p.n + 1))


def edge_sums(p, v_ref, tab_ref, left_ref, right_ref, edge_ref):
    for t in range(p.n // p.tile):
        rows = pl.ds(t * p.tile, p.tile)
        lam, lsub = tab_ref[0, rows], tab_ref[2, rows]
        left, right = v_ref[0, rows], v_ref[p.sub - 1, rows]
        for i in range(1, p.sub):
            left = left * lam + v_ref[i, rows]
            right = right * lam + v_ref[p.sub - 1 - i, rows]
        left_ref[rows] = left
        right_ref[rows] = right
        dev_l, dev_r = left, right
        for g in range(1, p.pack):
            dev_l = dev_l * lsub + turn(left, -g * p.kb)
            dev_r = dev_r * lsub + turn(right, g * p.kb)
        edge_ref[rows] = jnp.where(p.lanes(p.tile) == 0, dev_l, dev_r)


def line_exchange(p, tab_ref, edge_ref, got_ref, back_ref, ends_ref, sems, between):
    ix = lax.axis_index("gx")
    mine = pl.ds(ix * p.jb, p.jb)

    def copies(src, dst, base):
        out = []
        for d in range(1, p.gx):
            r = lax.rem(ix + d, p.gx)
            out.append(remote(src(r), dst, sems.at[base, d], sems.at[base + 1, d], {"gx": r}))
        return out

    first = copies(lambda r: edge_ref.at[pl.ds(r * p.jb, p.jb)], got_ref.at[ix], 0)
    for c in first:
        c.start()
    got_ref[ix] = edge_ref[mine]
    between(0)
    for c in first:
        c.wait_recv()
    lower = p.lanes(p.jb) == 0
    blk, det, lnp = tab_ref[3, mine], tab_ref[4, mine], tab_ref[5, mine]
    state = jnp.zeros((p.jb, LANES), jnp.float32)
    states = []
    for t in range(p.gx):
        states.append(state)
        state = state * blk + jnp.where(lower, got_ref[t], got_ref[p.gx - 1 - t])
    other = jnp.where(lower, turn(state, p.kb), turn(state, -p.kb))
    image = (other - state * lnp) * det
    for t in range(p.gx):
        states[t] = states[t] - image
        image = image * blk
    for t in range(p.gx):
        back_ref[t] = jnp.where(lower, states[t], states[p.gx - 1 - t])
    second = copies(lambda r: back_ref.at[r], ends_ref.at[mine], 2)
    for c in second:
        c.start()
    ends_ref[mine] = back_ref[ix]
    between(1)
    for c in second:
        c.wait_recv()
    for c in first + second:
        c.wait_send()


def carries(p, rows, tab_ref, left_ref, right_ref, ends_ref):
    lsub = tab_ref[2, rows]
    left, right = left_ref[rows], right_ref[rows]
    a = b = ends_ref[rows]
    place = p.lanes(p.tile)
    for g in range(p.pack - 1):
        a = jnp.where(place == g + 1, turn(a * lsub + left, p.kb), a)
        h = p.pack - 1 - g
        b = jnp.where(place == h - 1, turn(b * lsub + right, -p.kb), b)
    return a, b


def row_degrees():
    deg = np.full(ROWS, -1)
    deg[: (DEG + 1) // 2] = np.arange(0, DEG, 2)
    deg[EVEN : EVEN + DEG // 2] = np.arange(1, DEG, 2)
    return deg


def harmonic_tables(p):
    tens = face_tensors()
    deg = row_degrees()
    weights = expansion_weights() * (RADIUS ** -np.arange(DEG, dtype=np.float64))[:, None] * (p.norm / p.h)
    big = np.zeros((3, MI, ROWS, NBLK * LANES))
    sign = np.ones((3, ROWS, NBLK * LANES))
    gain = np.zeros((2, NBLK, 16, LANES))
    for l in range(DEG):
        for face in range(3):
            for i in range(ROWS):
                r = deg[i]
                if r < 0:
                    continue
                for q in range(DEG):
                    if face == 0:
                        odd, mpar = r % 2, (l - q) % 2
                    elif face == 1:
                        mpar = (l - q) % 2
                        odd = (r + mpar) % 2
                    else:
                        odd = q % 2
                        mpar = (r + odd) % 2
                    at = l * BLOCK + q
                    sign[face, i, at] = (-1.0) ** (mpar + odd, odd, l + mpar)[face]
                    for mi in range(MI):
                        m = mpar + 2 * mi
                        if m <= l and not (odd and m == 0):
                            big[face, mi, i, at] = tens[face, l, ORDER + m if odd else m][r, q]
        for c in range(2):
            for odd in range(2):
                for mi in range(MI):
                    m = (l - c) % 2 + 2 * mi
                    if m <= l:
                        at = (l % PER) * BLOCK + c
                        gain[odd, l // PER, mi, at : (l % PER + 1) * BLOCK : 2] = weights[l, m]
    return big.astype(np.float32), sign.astype(np.float32), gain.astype(np.float32)


def tables(p):
    n = p.n
    num = np.arange(n) + 1
    sine = np.sin(np.pi * ((num[:, None] * num[None, :]) % (2 * (n + 1))) / (n + 1))
    eps = 4.0 * np.sin(np.pi * num / (2.0 * (n + 1))) ** 2
    cheb = np.cos(np.arange(DEG)[None, :] * np.arccos((2.0 * np.arange(n) - (n - 1)) * p.h)[:, None])
    hat = sine @ cheb
    deg = row_degrees()
    used = deg >= 0
    jtab = np.stack([np.repeat(v[:, None], LANES, axis=1) for v in (eps, sine[0])])
    ktab = np.zeros((p.gy, 8, LANES))
    for r, v in enumerate((eps, sine[0], sine[n - 1])):
        ktab[:, r] = np.tile(v.reshape(p.gy, p.kb), (1, p.pack))
    wide = np.zeros((ROWS + 8, n))
    wide[:ROWS][used] = hat[:, deg[used]].T
    wide[ROWS], wide[ROWS + 1] = sine[0], sine[n - 1]
    lanes = np.zeros((n, LANES))
    for i in range(PER):
        lanes[:, i * BLOCK : i * BLOCK + DEG] = hat
    rows = np.zeros((n, BLOCK))
    rows[:, :ROWS][:, used] = cheb[:, deg[used]]
    rh, rl = split_table(rows)
    cols = np.zeros((BLOCK, n))
    cols[:DEG] = cheb.T
    ch, cl = split_table(cols)
    same = np.arange(LANES)
    same = (same[:, None] // BLOCK == same[None, :] // BLOCK) & ((same[:, None] - same[None, :]) % 2 == 0)
    big, sign, gain = harmonic_tables(p)
    f32 = np.float32
    return [
        np.stack(split_table(sine)),
        jtab.astype(f32),
        ktab.astype(f32),
        np.stack(split_table(wide)),
        lanes.astype(f32),
        np.concatenate([rh, rl, rh, np.zeros_like(rh)], axis=1),
        np.concatenate([ch, ch, cl, np.zeros_like(ch)], axis=0),
        big,
        sign,
        gain,
        same.astype(BF16),
    ]


def iota(shape, dim):
    return lax.broadcasted_iota(jnp.int32, shape, dim)


def face_prep(p, dmat_ref, r_ref):
    ix = lax.axis_index("gx")
    shape = (p.sub, LANES)
    cell = ix * p.ca + (iota(shape, 1) // p.kb) * p.sub + iota(shape, 0)
    t = (2 * cell - (p.n - 1)).astype(jnp.float32) * p.h
    prev, cur = jnp.ones(shape, jnp.float32), t
    dmat_ref[0] = prev
    for d in range(1, DEG):
        dmat_ref[d] = cur
        prev, cur = cur, 2.0 * t * cur - prev
    def inverse_radius(rows, start):
        u = (2 * (start + iota((rows, p.n), 0)) - (p.n - 1)).astype(jnp.float32) * (0.5 * p.h)
        v = (2 * iota((rows, p.n), 1) - (p.n - 1)).astype(jnp.float32) * (0.5 * p.h)
        return lax.rsqrt(0.25 + u * u + v * v)
    r_ref[0:p.n] = inverse_radius(p.n, 0)
    near = inverse_radius(p.ca, ix * p.ca)
    for k in range(4):
        r_ref[p.n + k * p.ca:p.n + (k + 1) * p.ca] = near


def moments(p, first_ref, rhs_ref, w_ref, v_ref, ktab_ref, dmat_ref, g_ref, y_ref):
    ix, iy = lax.axis_index("gx"), lax.axis_index("gy")
    pair = 2 if p.sub % 2 == 0 else 1
    energy = jnp.zeros((8, LANES), jnp.float32)
    for s in range(0, p.sub, pair):
        x = jnp.concatenate([first_ref[s + e] for e in range(pair)], axis=1)
        y = left_mul(w_ref, x)
        for e in range(pair):
            g_ref[s + e] = y[:, e * LANES:(e + 1) * LANES]
    for s in range(p.sub):
        prod = first_ref[s] * rhs_ref[s]
        for r in range(p.n // 8):
            energy = energy + prod[r * 8:(r + 1) * 8]
    y_ref[...] = jnp.zeros_like(y_ref)
    row_of = {d: i for i, d in enumerate(row_degrees()) if d >= 0}
    lane = iota((ROWS, LANES), 1)
    edge = [ktab_ref[iy][1:2], ktab_ref[iy][2:3]]
    mz = jnp.zeros((ROWS, LANES), jnp.float32)
    for d in range(DEG):
        acc = g_ref[0] * dmat_ref[d, 0:1]
        for s in range(1, p.sub):
            acc = acc + g_ref[s] * dmat_ref[d, s:s + 1]
        for f in range(2):
            at = f * ROWS + row_of[d]
            y_ref[at:at + 1] = acc[ROWS + f:ROWS + f + 1]
            total = jnp.sum(acc[:ROWS] * edge[f], axis=1, keepdims=True)
            mz = jnp.where(lane == f * BLOCK + d, total, mz)
    place = lane // p.kb
    lo = jnp.where((place == 0) & (ix == 0), g_ref[0][:ROWS], 0.0)
    hi = jnp.where((place == p.pack - 1) & (ix == p.gx - 1), g_ref[p.sub - 1][:ROWS], 0.0)
    x = jnp.concatenate([lo, hi, y_ref[...]], axis=0)
    table = v_ref[pl.ds(pl.multiple_of(iy * p.kb, 16), p.kb)]
    y = right_mul(x, split(jnp.concatenate([table] * p.pack, axis=0)))
    which = lane // BLOCK
    packed = y[0:ROWS]
    for i in range(1, 4):
        packed = jnp.where(which == i, y[i * ROWS:(i + 1) * ROWS], packed)
    return packed, mz, jnp.sum(energy, axis=1, keepdims=True)


def sum_slots(ref, count):
    total = ref[0]
    for i in range(1, count):
        total = total + ref[i]
    return total


def total_copies(p, src_ref, slots_ref, sems, axis, base):
    size = p.gx if axis == "gx" else p.gy
    me = lax.axis_index(axis)
    out = []
    for d in range(1, size):
        r = lax.rem(me + d, size)
        out.append(remote(src_ref, slots_ref.at[me], sems.at[base, d], sems.at[base + 1, d], {axis: r}))
    return out


def all_sum(p, pay_ref, xs_ref, sum_ref, ys_ref, sems):
    ix, iy = lax.axis_index("gx"), lax.axis_index("gy")
    a = total_copies(p, pay_ref, xs_ref, sems, "gx", 0)
    for c in a:
        c.start()
    xs_ref[ix] = pay_ref[...]
    for c in a:
        c.wait_recv()
    total = sum_slots(xs_ref, p.gx)
    sum_ref[...] = total
    b = total_copies(p, sum_ref, ys_ref, sems, "gy", 2)
    for c in b:
        c.start()
    ys_ref[iy] = total
    for c in b:
        c.wait_recv()
    for c in a + b:
        c.wait_send()
    return sum_slots(ys_ref, p.gy)


def trade(x):
    odd = iota(x.shape, 1) % 2 == 1
    return jnp.where(odd, turn(x, 1), turn(x, -1))


def project(p, packed, mz, energy, big_ref, sign_ref, gain_ref, same_ref, s_ref):
    which = iota((ROWS, LANES), 1) // BLOCK

    def spread(x, i):
        x = turn(jnp.where(which == i, x, 0.0), -i * BLOCK)
        x = x + turn(x, BLOCK)
        return x + turn(x, 2 * BLOCK)

    tall = (BLOCK, LANES)
    row, col = iota(tall, 0), iota(tall, 1)
    degree = jnp.where(row < EVEN, 2 * row, 2 * (row - EVEN) + 1)
    place = (col % BLOCK == degree).astype(jnp.float32).astype(BF16)
    mz = split(jnp.concatenate([mz, jnp.zeros((BLOCK - ROWS, LANES), jnp.float32)], axis=0))

    def flip(f):
        pick = (col == f * BLOCK + degree).astype(jnp.float32).astype(BF16)
        hi, lo = split(dot_t(pick, mz[0]) + dot_t(pick, mz[1]))
        return (dot(hi, place) + dot(lo, place))[:ROWS]

    pairs = [(spread(packed, 0), spread(packed, 1)), (spread(packed, 2), spread(packed, 3)), (flip(0), flip(1))]
    s_ref[...] = jnp.zeros_like(s_ref)
    for face in range(3):
        lo, hi = pairs[face]
        for blk in range(NBLK):
            cols = slice(blk * LANES, (blk + 1) * LANES)
            both = hi + sign_ref[face][:, cols] * lo
            for mi in range(MI):
                prod = big_ref[face, mi][:, cols] * both
                s_ref[face, 0, blk, mi:mi + 1] = jnp.sum(prod[:EVEN], axis=0, keepdims=True)
                s_ref[face, 1, blk, mi:mi + 1] = jnp.sum(prod[EVEN:], axis=0, keepdims=True)
    hi, lo = split(s_ref[...].reshape(6 * NBLK * 16, LANES))
    spread_sum = (dot(hi, same_ref[...]) + dot(lo, same_ref[...])).reshape(3, 2, NBLK, 16, LANES)
    lane = iota((16, LANES), 1)
    to = iota((8, LANES), 1)
    pay = jnp.zeros((8, LANES), jnp.float32)
    for blk in range(NBLK):
        l = blk * PER + lane // BLOCK
        right = lane % 2 == 1
        cross = (l - lane) % 2 == 1
        sx, sy, sz = spread_sum[0], spread_sum[1], spread_sum[2]
        lm = []
        for b in range(2):
            wide = [jnp.where((lane + b) % 2 == 0, sz[a, blk], trade(sz[a, blk])) for a in range(2)]
            other = jnp.where((l + lane + b) % 2 == 1, wide[1], wide[0])
            lm.append((sx[b, blk] + jnp.where(cross, sy[1 - b, blk], sy[b, blk]) + other) * gain_ref[b, blk])
        parts = [lm[0][:8], lm[1][:8], jnp.concatenate([lm[0][8:9], lm[1][8:9], jnp.zeros((6, LANES), jnp.float32)], axis=0)]
        for part, x in enumerate(parts):
            for i in range(PER):
                at = part * LOT + 2 * (blk * PER + i)
                pay = jnp.where((to >= at) & (to < at + 2), turn(x, at - i * BLOCK), pay)
    return jnp.where(to == LANES - 1, energy, pay)


def coefficients(p, total, big_ref, coef_ref):
    to = iota((8, LANES), 1)
    for blk in range(NBLK):
        wide = []
        for part in range(3):
            x = jnp.zeros((8, LANES), jnp.float32)
            for i in range(PER):
                at = part * LOT + 2 * (blk * PER + i)
                x = jnp.where((to >= i * BLOCK) & (to < i * BLOCK + 2), turn(total, i * BLOCK - at), x)
            for shift in (2, 4, 8, 16):
                x = x + turn(x, shift)
            wide.append(x)
        lm = [jnp.concatenate([wide[b], wide[2][b:b + 1], jnp.zeros((7, LANES), jnp.float32)], axis=0) for b in range(2)]
        l = blk * PER + iota((16, LANES), 1) // BLOCK
        lane = iota((16, LANES), 1)
        right = lane % 2 == 1
        cross = (l - lane) % 2 == 1
        rows = [lm, [jnp.where(cross, lm[1 - b], lm[b]) for b in range(2)],
                [jnp.where(right, *[jnp.where((l + a) % 2 == 1, trade(lm[b]), lm[b]) for b in (1, 0)]) for a in range(2)]]
        cols = slice(blk * LANES, (blk + 1) * LANES)
        for face in range(3):
            even = jnp.zeros((EVEN, LANES), jnp.float32)
            odd = jnp.zeros((ROWS - EVEN, LANES), jnp.float32)
            for mi in range(MI):
                t = big_ref[face, mi][:, cols]
                even = even + t[:EVEN] * rows[face][0][mi:mi + 1]
                odd = odd + t[EVEN:] * rows[face][1][mi:mi + 1]
            coef_ref[face, blk] = jnp.concatenate([even, odd], axis=0)


def face_coefs(p, coef_ref, sign_ref, c3_ref):
    ix = lax.axis_index("gx")
    which = iota((ROWS, LANES), 1) // BLOCK
    gap = jnp.zeros((BLOCK - ROWS, LANES), jnp.float32)
    rest = jnp.zeros((LANES - 3 * BLOCK, LANES), jnp.float32)
    for l in range(DEG):
        blk, i = divmod(l, PER)
        cols = slice(blk * LANES, (blk + 1) * LANES)
        for face in range(3):
            hi = coef_ref[face, blk]
            lo = hi * sign_ref[face][:, cols]
            for k, c in enumerate([jnp.where(ix == 0, lo, hi)] if face == 0 else [lo, hi]):
                c = turn(jnp.where(which == i, c, 0.0), -i * BLOCK)
                c = c + turn(c, BLOCK) + turn(c, 2 * BLOCK)
                top = c.astype(BF16).astype(jnp.float32)
                full = jnp.concatenate([top, gap, top, gap, c - top, gap, rest], axis=0)
                c3_ref[l, max(0, 2 * face - 1) + k] = full.astype(BF16)


def triple(e):
    top = e.astype(BF16).astype(jnp.float32)
    return jnp.where(iota(e.shape, 1) // BLOCK == 1, e - top, top).astype(BF16)


def faces(p, c3_ref, cu_ref, vt_ref, r_ref, e_ref, f_ref):
    near = pl.ds(pl.multiple_of(lax.axis_index("gx") * p.ca, 16), p.ca)
    rows = p.n + 4 * p.ca
    for l in range(DEG):
        e_ref[l, 0:p.n] = triple(dot(cu_ref[...], c3_ref[l, 0]))
        e = dot(cu_ref[near], jnp.concatenate([c3_ref[l, k] for k in range(1, 5)], axis=1))
        e = jnp.concatenate([e[:, k * LANES:(k + 1) * LANES] for k in range(4)], axis=0)
        e_ref[l, p.n:rows] = triple(e)
    tile = 64

    def step(t, carry):
        at = pl.ds(pl.multiple_of(t * tile, tile), tile)
        r = r_ref[at]
        acc = dot(e_ref[DEG - 1, at], vt_ref[...])
        for l in range(DEG - 2, -1, -1):
            acc = acc * r + dot(e_ref[l, at], vt_ref[...])
        f_ref[at] = acc
        return carry

    lax.fori_loop(0, rows // tile, step, 0)


def add_faces(p, rhs_ref, sine_ref, jtab_ref, ktab_ref, f_ref):
    ix, iy = lax.axis_index("gx"), lax.axis_index("gy")
    ca, n = p.ca, p.n
    chunk = pl.ds(pl.multiple_of(iy * p.kb, 16), p.kb)
    near = [jnp.concatenate([sine_ref[i, chunk]] * p.pack, axis=0) for i in range(2)]

    def to_lanes(x):
        hi, lo = split(x)
        return dot_t(hi, near[0]) + dot_t(lo, near[0]) + dot_t(hi, near[1])

    @pl.when((ix == 0) | (ix == p.gx - 1))
    def _():
        hat = left_mul(sine_ref, to_lanes(f_ref[0:n]))
        place = p.lanes(p.n)
        rhs_ref[0] += jnp.where((place == 0) & (ix == 0), hat, 0.0)
        rhs_ref[p.sub - 1] += jnp.where((place == p.pack - 1) & (ix == p.gx - 1), hat, 0.0)

    hy = to_lanes(f_ref[n:n + 2 * ca])
    place = p.lanes(p.sub)
    planes = []
    for f in range(2):
        acc = hy[f * ca:f * ca + p.sub]
        for g in range(1, p.pack):
            acc = jnp.where(place == g, hy[f * ca + g * p.sub:f * ca + (g + 1) * p.sub], acc)
        planes.append(acc)
    plus, minus = planes[0] + planes[1], planes[0] - planes[1]

    hi, lo = split(jnp.concatenate([f_ref[n + 2 * ca:n + 4 * ca]] * (LANES // (2 * ca)), axis=0))
    hz = dot_t(sine_ref[0], hi) + dot_t(sine_ref[1], hi) + dot_t(sine_ref[0], lo)
    top = hz.astype(BF16).astype(jnp.float32)
    both = jnp.where(iota(hz.shape, 1) // (2 * ca) == 1, hz - top, top).astype(BF16)
    top = top.astype(BF16)
    square = (LANES, LANES)
    row, col = iota(square, 0), iota(square, 1)
    edge = jnp.where(row % (2 * ca) < ca, ktab_ref[iy][1:2], ktab_ref[iy][2:3])
    head = edge.astype(BF16).astype(jnp.float32)
    fits = (row % ca) // p.sub == col // p.kb
    first = jnp.where(fits & (row // (2 * ca) < 2), head, 0.0)
    second = jnp.where(fits & (row < 2 * ca), edge - head, 0.0)
    pair = 2 if p.sub % 2 == 0 else 1
    even = iota((p.n, LANES), 0) % 2 == 0
    for s in range(0, p.sub, pair):
        pick = [row % p.sub == s + e for e in range(pair)]
        one = jnp.concatenate([jnp.where(k, first, 0.0).astype(BF16) for k in pick], axis=1)
        two = jnp.concatenate([jnp.where(k, second, 0.0).astype(BF16) for k in pick], axis=1)
        add = dot(both, one) + dot(top, two)
        for e in range(pair):
            at = s + e
            wave = jnp.where(even, plus[at:at + 1], minus[at:at + 1])
            rhs_ref[at] += add[:, e * LANES:(e + 1) * LANES] + jtab_ref[1] * wave


def kernel(p, rho_ref, *refs):
    names = ("sine", "jtab", "ktab", "wide", "lanes", "cu", "vt", "big", "sign", "gain", "same")
    hbm = refs[:len(names)]
    out_ref, energy_ref = refs[len(names):len(names) + 2]
    rest = refs[len(names) + 2:]
    local = rest[:len(names)]
    (x_ref, send_ref, spec_ref, rhs_ref, first_ref, tab_ref, left_ref, right_ref, edge_ref, carry_ref,
     got_ref, back_ref, ends_ref, got2_ref, back2_ref, ends2_ref,
     dmat_ref, r_ref, g_ref, y_ref, pay_ref, pxs_ref, psum_ref, pys_ref,
     s_ref, coef_ref, c3_ref, e_ref, f_ref,
     part_ref, xs_ref, sum_ref, ys_ref, u_ref, res_ref, fin_ref,
     table_sems, in_sems, out_sems, land_sems, back_out_sems, back_land_sems,
     line_sems, line2_sems, pay_sems, sum_sems, write_sems) = rest[len(names):]
    sine_ref, jtab_ref, ktab_ref, wide_ref, lanes_ref, cu_ref, vt_ref, big_ref, sign_ref, gain_ref, same_ref = local
    w_ref = spec_ref
    ix, iy = lax.axis_index("gx"), lax.axis_index("gy")
    order = list(range(p.gy // 2, p.gy)) + list(range(1, p.gy // 2))
    block = p.step * p.cb
    staged = [pltpu.make_async_copy(hbm[i], local[i], table_sems.at[i]) for i in range(len(names))]

    def load(c, g):
        rows = pl.ds(g * p.sub + c * p.step, p.step)
        return pltpu.make_async_copy(rho_ref.at[rows], x_ref.at[rows], in_sems.at[c, g])

    staged[0].start()
    for c in range(p.chunks):
        for g in range(p.pack):
            load(c, g).start()
    for copy in staged[1:]:
        copy.start()
    greet(p)
    staged[0].wait()

    def swap(c, d):
        q = lax.rem(iy + d, p.gy)
        planes = pl.ds(c * p.step, p.step)
        return remote(send_ref.at[q, planes], spec_ref.at[planes, pl.ds(iy * p.cb, p.cb)],
                      out_sems.at[c, d], land_sems.at[c, d], {"gy": q})

    def transform(c, carry):
        for g in range(p.pack):
            load(c, g).wait()
        x = jnp.concatenate(
            [x_ref[pl.ds(g * p.sub + c * p.step, p.step)].reshape(block, p.n) for g in range(p.pack)], axis=0
        )
        y = right_mul(x, sine_ref)
        place = p.lanes(block)
        planes = pl.ds(c * p.step, p.step)
        for q in range(p.gy):
            col, off = divmod(q * p.kb, LANES)
            piece = None
            for g in range(p.pack):
                part = turn(y[g * block:(g + 1) * block, col * LANES:(col + 1) * LANES], g * p.kb - off)
                piece = part if piece is None else jnp.where(place == g, part, piece)
            send_ref[q, planes] = piece.reshape(p.step, p.cb, LANES)

        @pl.when(c > 0)
        def _():
            for d in order:
                swap(c - 1, d).start()

        spec_ref[planes, pl.ds(iy * p.cb, p.cb)] = send_ref[iy, planes]
        return carry

    lax.fori_loop(0, p.chunks, transform, 0)
    staged[1].wait()
    staged[2].wait()
    mode_tables(p, jtab_ref, ktab_ref, tab_ref)
    for d in order:
        swap(p.chunks - 1, d).start()
    face_prep(p, dmat_ref, r_ref)

    def across(c, carry):
        for d in order:
            swap(c, d).wait_recv()
        for i in range(0, p.step, p.pair):
            s = c * p.step + i
            x = jnp.concatenate([spec_ref[s + e] for e in range(p.pair)], axis=1)
            y = left_mul(sine_ref, x)
            for e in range(p.pair):
                rhs_ref[s + e] = y[:, e * LANES:(e + 1) * LANES]
        return carry

    lax.fori_loop(0, p.chunks, across, 0)
    edge_sums(p, rhs_ref, tab_ref, left_ref, right_ref, edge_ref)
    line_exchange(p, tab_ref, edge_ref, got_ref, back_ref, ends_ref, line_sems, lambda stage: None)

    for t in range(p.n // p.tile):
        rows = pl.ds(t * p.tile, p.tile)
        lam, inv = tab_ref[0, rows], tab_ref[1, rows]
        a, b = carries(p, rows, tab_ref, left_ref, right_ref, ends_ref)
        for i in range(p.sub - 1, -1, -1):
            b = b * lam
            first_ref[i, rows] = b
            b = b + rhs_ref[i, rows]
        for i in range(p.sub):
            a = a * lam + rhs_ref[i, rows]
            first_ref[i, rows] = (a + first_ref[i, rows]) * inv

    def drain(c, carry):
        for d in order:
            swap(c, d).wait_send()
        return carry

    lax.fori_loop(0, p.chunks, drain, 0)
    for copy in staged[3:]:
        copy.wait()

    sums = moments(p, first_ref, rhs_ref, wide_ref, lanes_ref, ktab_ref, dmat_ref, g_ref, y_ref)
    pay_ref[...] = project(p, *sums, big_ref, sign_ref, gain_ref, same_ref, s_ref)
    total = all_sum(p, pay_ref, pxs_ref, psum_ref, pys_ref, pay_sems)
    energy_one = jnp.sum(jnp.where(iota(total.shape, 1) == LANES - 1, total, 0.0))
    coefficients(p, total, big_ref, coef_ref)
    face_coefs(p, coef_ref, sign_ref, c3_ref)
    faces(p, c3_ref, cu_ref, vt_ref, r_ref, e_ref, f_ref)
    add_faces(p, rhs_ref, sine_ref, jtab_ref, ktab_ref, f_ref)

    edge_sums(p, rhs_ref, tab_ref, left_ref, right_ref, edge_ref)
    ea = total_copies(p, part_ref, xs_ref, sum_sems, "gx", 0)
    eb = total_copies(p, sum_ref, ys_ref, sum_sems, "gy", 2)

    def between(stage):
        if stage == 0:
            energy = jnp.zeros((8, LANES), jnp.float32)
            for i in range(p.sub):
                prod = first_ref[i] * rhs_ref[i]
                for r in range(p.n // 8):
                    energy = energy + prod[r * 8:(r + 1) * 8]
            part_ref[...] = energy
            xs_ref[ix] = energy
            return
        for c in ea:
            c.start()

    line_exchange(p, tab_ref, edge_ref, got2_ref, back2_ref, ends2_ref, line2_sems, between)
    for t in range(p.n // p.tile):
        rows = pl.ds(t * p.tile, p.tile)
        lam = tab_ref[0, rows]
        a, b = carries(p, rows, tab_ref, left_ref, right_ref, ends2_ref)
        carry_ref[rows] = a
        for i in range(p.sub - 1, -1, -1):
            b = b * lam
            first_ref[i, rows] = b
            b = b + rhs_ref[i, rows]
    for c in ea:
        c.wait_recv()
    total = sum_slots(xs_ref, p.gx)
    sum_ref[...] = total
    ys_ref[iy] = total

    def swap_back(c, d):
        q = lax.rem(iy + d, p.gy)
        planes = pl.ds(c * p.step, p.step)
        return remote(u_ref.at[planes, pl.ds(q * p.cb, p.cb)], res_ref.at[iy, planes],
                      back_out_sems.at[c, d], back_land_sems.at[c, d], {"gy": q})

    def back_across(c, carry):
        for t in range(p.n // p.tile):
            rows = pl.ds(t * p.tile, p.tile)
            lam, inv = tab_ref[0, rows], tab_ref[1, rows] * p.norm
            a = carry_ref[rows]
            for i in range(p.step):
                s = c * p.step + i
                a = a * lam + rhs_ref[s, rows]
                first_ref[s, rows] = (a + first_ref[s, rows]) * inv
            carry_ref[rows] = a
        for i in range(0, p.step, p.pair):
            s = c * p.step + i
            x = jnp.concatenate([first_ref[s + e] for e in range(p.pair)], axis=1)
            y = left_mul(sine_ref, x)
            for e in range(p.pair):
                u_ref[s + e] = y[:, e * LANES:(e + 1) * LANES]
        planes = pl.ds(c * p.step, p.step)

        @pl.when(c > 0)
        def _():
            for d in order:
                swap_back(c - 1, d).start()

        res_ref[iy, planes] = u_ref[planes, pl.ds(iy * p.cb, p.cb)]
        return carry

    lax.fori_loop(0, p.chunks, back_across, 0)
    for c in eb:
        c.start()
    for d in order:
        swap_back(p.chunks - 1, d).start()

    def write(c, g):
        rows = pl.ds(g * p.sub + c * p.step, p.step)
        return pltpu.make_async_copy(fin_ref.at[rows], out_ref.at[rows], write_sems.at[c, g])

    def finish(c, carry):
        for d in order:
            swap_back(c, d).wait_recv()
        planes = pl.ds(c * p.step, p.step)
        place = p.lanes(block)
        parts = [res_ref[q, planes].reshape(block, LANES) for q in range(p.gy)]
        per = LANES // p.kb
        rows = []
        for g in range(p.pack):
            cols = []
            for col in range(p.n // LANES):
                acc = None
                for e in range(per):
                    part = turn(parts[col * per + e], (e - g) * p.kb)
                    acc = part if acc is None else jnp.where(place == e, part, acc)
                cols.append(acc)
            rows.append(jnp.concatenate(cols, axis=1))
        y = right_mul(jnp.concatenate(rows, axis=0), sine_ref)
        for g in range(p.pack):
            at = pl.ds(g * p.sub + c * p.step, p.step)
            fin_ref[at] = y[g * block:(g + 1) * block].reshape(p.step, p.cb, p.n)

        @pl.when(c > 0)
        def _():
            for g in range(p.pack):
                write(c - 1, g).start()

        return carry

    lax.fori_loop(0, p.chunks, finish, 0)
    for c in eb:
        c.wait_recv()
    energy_two = jnp.sum(sum_slots(ys_ref, p.gy))
    for g in range(p.pack):
        write(p.chunks - 1, g).start()
    scale = p.h**3 * p.norm
    energy_ref[...] = jnp.where(iota((8, LANES), 1) == 0, energy_one, energy_two) * scale
    for c in range(p.chunks):
        for g in range(p.pack):
            write(c, g).wait()
    for c in ea + eb:
        c.wait_send()

    def back_drain(c, carry):
        for d in order:
            swap_back(c, d).wait_send()
        return carry

    lax.fori_loop(0, p.chunks, back_drain, 0)


def shards(charge_density):
    ca, cb, n = charge_density.shape
    p = Plan(ca, cb, n, lax.axis_size("gx"), lax.axis_size("gy"))
    f32 = jnp.float32
    data = tables(p)
    cube = (p.sub, p.n, LANES)
    plane = (p.n, LANES)
    slots = (p.gx, p.jb, LANES)
    pay = (8, LANES)
    box = (p.gy, p.sub, p.cb, LANES)
    vmem = lambda shape, dtype=f32: pltpu.VMEM(shape, dtype)
    dma = pltpu.SemaphoreType.DMA
    anywhere = pl.BlockSpec(memory_space=pl.ANY)
    whole = (p.ca, p.cb, p.n)
    scratch = [vmem(t.shape, t.dtype) for t in data]
    scratch += [vmem(whole), vmem(box), vmem(cube), vmem(cube), vmem(cube), vmem((6,) + plane)]
    scratch += [vmem(plane)] * 4
    scratch += [vmem(slots), vmem(slots), vmem(plane)] * 2
    scratch += [vmem((DEG, p.sub, LANES)), vmem((p.n + 4 * p.ca, p.n)), vmem((p.sub, ROWS + 8, LANES)),
                vmem((2 * ROWS, LANES)), vmem(pay), vmem((p.gx,) + pay), vmem(pay), vmem((p.gy,) + pay)]
    scratch += [vmem((3, 2, NBLK, 16, LANES)), vmem((3, NBLK, ROWS, LANES)), vmem((DEG, 5, LANES, LANES), BF16),
                vmem((DEG, p.n + 4 * p.ca, LANES), BF16), vmem((p.n + 4 * p.ca, p.n))]
    scratch += [vmem((8, LANES)), vmem((p.gx, 8, LANES)), vmem((8, LANES)), vmem((p.gy, 8, LANES)),
                vmem(cube), vmem(box), vmem(whole)]
    most = max(p.gx, p.gy)
    scratch += [dma((len(data),)), dma((p.chunks, p.pack))] + [dma((p.chunks, p.gy))] * 4
    scratch += [dma((4, p.gx))] * 2 + [dma((4, most))] * 2 + [dma((p.chunks, p.pack))]
    potential, energies = pl.pallas_call(
        functools.partial(kernel, p),
        in_specs=[anywhere] * (1 + len(data)),
        out_specs=[anywhere, pl.BlockSpec(memory_space=pltpu.VMEM)],
        out_shape=[jax.ShapeDtypeStruct(whole, f32), jax.ShapeDtypeStruct((8, LANES), f32)],
        scratch_shapes=scratch,
        compiler_params=pltpu.CompilerParams(
            collective_id=0, has_side_effects=True, vmem_limit_bytes=56 * 2**20
        ),
        name="james",
    )(charge_density, *[jnp.asarray(t) for t in data])
    return potential, energies[0, :2]


def solution(mesh):
    return jax.shard_map(
        shards,
        mesh=mesh,
        in_specs=(P("gx", "gy", None),),
        out_specs=(P("gx", "gy", None), P()),
        check_vma=False,
    )
```

```python
import functools
import math

import jax
import jax.numpy as jnp
import numpy as np
from jax import lax
from jax.experimental import pallas as pl
from jax.experimental.pallas import tpu as pltpu
from jax.sharding import PartitionSpec as P

ORDER = 16
DEG = ORDER + 1
RATIO = 1.1
RADIUS = math.sqrt(3.0) / 2.0
LANES = 128
MESH = pl.DeviceIdType.MESH
BF16 = jnp.bfloat16
EVEN = -(-((DEG + 1) // 2) // 8) * 8
ROWS = EVEN + -(-(DEG // 2) // 8) * 8
BLOCK = 32
PER = LANES // BLOCK
NBLK = -(-DEG // PER)
MI = (DEG + 1) // 2
LOT = 2 * PER * NBLK


def solid_harmonics(x, y, z):
    rr = x * x + y * y + z * z
    out = np.zeros((DEG, 2 * DEG - 1) + x.shape)
    cos = np.zeros((DEG, DEG) + x.shape)
    sin = np.zeros((DEG, DEG) + x.shape)
    cos[0, 0] = 1.0
    for l in range(1, DEG):
        s = 1.0 if l == 1 else math.sqrt((2 * l - 1) / (2.0 * l))
        cos[l, l] = s * (x * cos[l - 1, l - 1] - y * sin[l - 1, l - 1])
        sin[l, l] = s * (x * sin[l - 1, l - 1] + y * cos[l - 1, l - 1])
        for m in range(l):
            div = math.sqrt(l * l - m * m)
            far = math.sqrt((l - 1) * (l - 1) - m * m) if l - 1 > m else 0.0
            for f in (cos, sin):
                f[l, m] = (2 * l - 1) * z * f[l - 1, m] / div
                if l >= 2 and far:
                    f[l, m] = f[l, m] - far * rr * f[l - 2, m] / div
    out[:, :DEG] = cos
    out[:, DEG:] = sin[:, 1:]
    return out


def face_tensors():
    t = np.cos(np.pi * (np.arange(DEG) + 0.5) / DEG)
    fwd = np.cos(np.arange(DEG)[:, None] * np.arccos(t)[None, :]) * (2.0 / DEG)
    fwd[0] *= 0.5
    u, v = np.meshgrid(t / 2, t / 2, indexing="ij")
    half = np.full_like(u, 0.5)
    tensors = []
    for pts in ((half, u, v), (u, half, v), (u, v, half)):
        vals = solid_harmonics(*pts)
        tensors.append(np.einsum("pu,lfuv,qv->lfpq", fwd, vals, fwd))
    return np.stack(tensors)


def expansion_weights():
    w = np.zeros((DEG, 2 * DEG - 1))
    for l in range(DEG):
        for f in range(2 * DEG - 1):
            m = f if f < DEG else f - ORDER
            w[l, f] = (1.0 if m == 0 else 2.0) / (4.0 * math.pi * RADIUS * RATIO ** (l + 1))
    return w.astype(np.float32)


def split(x):
    hi = x.astype(jnp.bfloat16)
    return hi, (x - hi.astype(jnp.float32)).astype(jnp.bfloat16)


def dot(a, b):
    return jnp.dot(a, b, preferred_element_type=jnp.float32)


def left_mul(mat, x):
    hi, lo = split(x)
    return dot(mat[0], hi) + dot(mat[0], lo) + dot(mat[1], hi)


def right_mul(x, mat):
    hi, lo = split(x)
    return dot(hi, mat[0]) + dot(lo, mat[0]) + dot(hi, mat[1])


def dot_t(a, b):
    return lax.dot_general(a, b, (((1,), (1,)), ((), ())), preferred_element_type=jnp.float32)


def split_table(table):
    t = np.asarray(table, np.float32)
    hi = t.astype(BF16)
    return hi, (t - hi.astype(np.float32)).astype(BF16)


def turn(x, shift):
    width = x.shape[-1]
    shift %= width
    return pltpu.roll(x, shift, x.ndim - 1) if shift else x


class Plan:
    def __init__(self, ca, cb, n, gx, gy):
        self.ca, self.cb, self.n, self.gx, self.gy = ca, cb, n, gx, gy
        self.kb = n // gy
        self.h = 1.0 / (n + 1)
        self.norm = (2.0 * self.h) ** 2
        self.jb = n // gx
        self.width = LANES
        self.pack = LANES // self.kb
        self.sub = ca // self.pack
        self.step = max(1, self.sub // 8)
        self.pair = 2 if self.step % 2 == 0 else 1
        self.chunks = self.sub // self.step
        self.tile = min(n, 64)

    def lanes(self, rows):
        return lax.broadcasted_iota(jnp.int32, (rows, LANES), 1) // self.kb


def greet(p):
    ix, iy = lax.axis_index("gx"), lax.axis_index("gy")
    barrier = pltpu.get_barrier_semaphore()
    for d in range(1, p.gx):
        pl.semaphore_signal(barrier, inc=1, device_id={"gx": lax.rem(ix + d, p.gx)}, device_id_type=MESH)
    for d in range(1, p.gy):
        pl.semaphore_signal(barrier, inc=1, device_id={"gy": lax.rem(iy + d, p.gy)}, device_id_type=MESH)
    pl.semaphore_wait(barrier, p.gx + p.gy - 2)


def remote(src, dst, send, recv, where):
    return pltpu.make_async_remote_copy(
        src_ref=src, dst_ref=dst, send_sem=send, recv_sem=recv, device_id=where, device_id_type=MESH
    )


def mode_tables(p, epsj_ref, epsk_ref, tab_ref):
    iy = lax.axis_index("gy")
    sigma = epsj_ref[0] + epsk_ref[iy][0:1]
    s = 0.5 * jnp.sqrt(sigma)
    t = jnp.sqrt(1.0 + s * s)
    theta = 2.0 * jnp.log1p(s + s * s / (1.0 + t))
    lam = jnp.exp(-theta)
    tab_ref[0] = lam
    tab_ref[1] = p.h * p.h / (4.0 * s * t)
    tab_ref[2] = jnp.exp(-theta * float(p.sub))
    tab_ref[3] = jnp.exp(-theta * float(p.ca))
    tab_ref[4] = lam / (1.0 - jnp.exp(-theta * (2.0 * (p.n + 1))))
    tab_ref[5] = jnp.exp(-theta * float(p.n + 1))


def edge_sums(p, v_ref, tab_ref, left_ref, right_ref, edge_ref):
    for t in range(p.n // p.tile):
        rows = pl.ds(t * p.tile, p.tile)
        lam, lsub = tab_ref[0, rows], tab_ref[2, rows]
        left, right = v_ref[0, rows], v_ref[p.sub - 1, rows]
        for i in range(1, p.sub):
            left = left * lam + v_ref[i, rows]
            right = right * lam + v_ref[p.sub - 1 - i, rows]
        left_ref[rows] = left
        right_ref[rows] = right
        dev_l, dev_r = left, right
        for g in range(1, p.pack):
            dev_l = dev_l * lsub + turn(left, -g * p.kb)
            dev_r = dev_r * lsub + turn(right, g * p.kb)
        edge_ref[rows] = jnp.where(p.lanes(p.tile) == 0, dev_l, dev_r)


def line_exchange(p, tab_ref, edge_ref, got_ref, back_ref, ends_ref, sems, between):
    ix = lax.axis_index("gx")
    mine = pl.ds(ix * p.jb, p.jb)

    def copies(src, dst, base):
        out = []
        for d in range(1, p.gx):
            r = lax.rem(ix + d, p.gx)
            out.append(remote(src(r), dst, sems.at[base, d], sems.at[base + 1, d], {"gx": r}))
        return out

    first = copies(lambda r: edge_ref.at[pl.ds(r * p.jb, p.jb)], got_ref.at[ix], 0)
    for c in first:
        c.start()
    got_ref[ix] = edge_ref[mine]
    between(0)
    for c in first:
        c.wait_recv()
    lower = p.lanes(p.jb) == 0
    blk, det, lnp = tab_ref[3, mine], tab_ref[4, mine], tab_ref[5, mine]
    state = jnp.zeros((p.jb, LANES), jnp.float32)
    states = []
    for t in range(p.gx):
        states.append(state)
        state = state * blk + jnp.where(lower, got_ref[t], got_ref[p.gx - 1 - t])
    other = jnp.where(lower, turn(state, p.kb), turn(state, -p.kb))
    image = (other - state * lnp) * det
    for t in range(p.gx):
        states[t] = states[t] - image
        image = image * blk
    for t in range(p.gx):
        back_ref[t] = jnp.where(lower, states[t], states[p.gx - 1 - t])
    second = copies(lambda r: back_ref.at[r], ends_ref.at[mine], 2)
    for c in second:
        c.start()
    ends_ref[mine] = back_ref[ix]
    between(1)
    for c in second:
        c.wait_recv()
    for c in first + second:
        c.wait_send()


def carries(p, rows, tab_ref, left_ref, right_ref, ends_ref):
    lsub = tab_ref[2, rows]
    left, right = left_ref[rows], right_ref[rows]
    a = b = ends_ref[rows]
    place = p.lanes(p.tile)
    for g in range(p.pack - 1):
        a = jnp.where(place == g + 1, turn(a * lsub + left, p.kb), a)
        h = p.pack - 1 - g
        b = jnp.where(place == h - 1, turn(b * lsub + right, -p.kb), b)
    return a, b


def row_degrees():
    deg = np.full(ROWS, -1)
    deg[: (DEG + 1) // 2] = np.arange(0, DEG, 2)
    deg[EVEN : EVEN + DEG // 2] = np.arange(1, DEG, 2)
    return deg


def harmonic_tables(p):
    tens = face_tensors()
    deg = row_degrees()
    weights = expansion_weights() * (RADIUS ** -np.arange(DEG, dtype=np.float64))[:, None] * (p.norm / p.h)
    big = np.zeros((3, MI, ROWS, NBLK * LANES))
    gain = np.zeros((2, NBLK, 16, LANES))
    for l in range(DEG):
        for face in range(3):
            for i in range(ROWS):
                r = deg[i]
                if r < 0:
                    continue
                for q in range(DEG):
                    if face == 0:
                        odd, mpar = r % 2, (l - q) % 2
                    elif face == 1:
                        mpar = (l - q) % 2
                        odd = (r + mpar) % 2
                    else:
                        odd = q % 2
                        mpar = (r + odd) % 2
                    at = l * BLOCK + q
                    for mi in range(MI):
                        m = mpar + 2 * mi
                        if m <= l and not (odd and m == 0):
                            big[face, mi, i, at] = tens[face, l, ORDER + m if odd else m][r, q]
        for c in range(2):
            for odd in range(2):
                for mi in range(MI):
                    m = (l - c) % 2 + 2 * mi
                    if m <= l:
                        at = (l % PER) * BLOCK + c
                        gain[odd, l // PER, mi, at : (l % PER + 1) * BLOCK : 2] = weights[l, m]
    return big.astype(np.float32), gain.astype(np.float32)


def tables(p):
    n = p.n
    num = np.arange(n) + 1
    sine = np.sin(np.pi * ((num[:, None] * num[None, :]) % (2 * (n + 1))) / (n + 1))
    eps = 4.0 * np.sin(np.pi * num / (2.0 * (n + 1))) ** 2
    cheb = np.cos(np.arange(DEG)[None, :] * np.arccos((2.0 * np.arange(n) - (n - 1)) * p.h)[:, None])
    hat = sine @ cheb
    deg = row_degrees()
    used = deg >= 0
    jtab = np.stack([np.repeat(v[:, None], LANES, axis=1) for v in (eps, sine[0])])
    ktab = np.zeros((p.gy, 8, LANES))
    for r, v in enumerate((eps, sine[0], sine[n - 1])):
        ktab[:, r] = np.tile(v.reshape(p.gy, p.kb), (1, p.pack))
    wide = np.zeros((ROWS + 8, n))
    wide[:ROWS][used] = hat[:, deg[used]].T
    wide[ROWS], wide[ROWS + 1] = sine[0], sine[n - 1]
    lanes = np.zeros((n, LANES))
    for i in range(PER):
        lanes[:, i * BLOCK : i * BLOCK + DEG] = hat
    rows = np.zeros((n, BLOCK))
    rows[:, :ROWS][:, used] = cheb[:, deg[used]]
    rh, rl = split_table(rows)
    cols = np.zeros((BLOCK, n))
    cols[:DEG] = cheb.T
    ch, cl = split_table(cols)
    same = np.arange(LANES)
    same = (same[:, None] // BLOCK == same[None, :] // BLOCK) & ((same[:, None] - same[None, :]) % 2 == 0)
    big, gain = harmonic_tables(p)
    f32 = np.float32
    own = np.arange(p.cb) + 1
    small = np.sin(np.pi * ((own[:, None] * own[None, :]) % (2 * (p.cb + 1))) / (p.cb + 1))
    small_eps = 4.0 * np.sin(np.pi * own / (2.0 * (p.cb + 1))) ** 2
    ltab = np.stack([np.repeat(v[:, None], LANES, axis=1) for v in (small_eps, small[0])])
    rtab = np.zeros((8, n))
    rtab[0], rtab[1] = eps, sine[0]
    pick = np.zeros((max(16, 2 * p.gy), n))
    for q in range(p.gy):
        if q > 0:
            pick[2 * q] = sine[q * p.cb - 1]
        if q < p.gy - 1:
            pick[2 * q + 1] = sine[(q + 1) * p.cb]
    return [
        np.stack(split_table(sine)),
        jtab.astype(f32),
        ktab.astype(f32),
        np.stack(split_table(wide)),
        lanes.astype(f32),
        np.concatenate([rh, rl, rh, np.zeros_like(rh)], axis=1),
        np.concatenate([ch, ch, cl, np.zeros_like(ch)], axis=0),
        big,
        gain,
        same.astype(BF16),
        np.stack(split_table(np.tile(small, (1, n // p.cb)))),
        ltab.astype(f32),
        rtab.astype(f32),
        np.stack(split_table(pick)),
    ]


def iota(shape, dim):
    return lax.broadcasted_iota(jnp.int32, shape, dim)


def face_prep(p, dmat_ref, r_ref):
    ix = lax.axis_index("gx")
    shape = (p.sub, LANES)
    cell = ix * p.ca + (iota(shape, 1) // p.kb) * p.sub + iota(shape, 0)
    t = (2 * cell - (p.n - 1)).astype(jnp.float32) * p.h
    prev, cur = jnp.ones(shape, jnp.float32), t
    dmat_ref[0] = prev
    for d in range(1, DEG):
        dmat_ref[d] = cur
        prev, cur = cur, 2.0 * t * cur - prev
    def inverse_radius(rows, start):
        u = (2 * (start + iota((rows, p.n), 0)) - (p.n - 1)).astype(jnp.float32) * (0.5 * p.h)
        v = (2 * iota((rows, p.n), 1) - (p.n - 1)).astype(jnp.float32) * (0.5 * p.h)
        return lax.rsqrt(0.25 + u * u + v * v)
    r_ref[0:p.n] = inverse_radius(p.n, 0)
    near = inverse_radius(p.ca, ix * p.ca)
    for k in range(4):
        r_ref[p.n + k * p.ca:p.n + (k + 1) * p.ca] = near


def moments(p, first_ref, rhs_ref, w_ref, v_ref, ktab_ref, dmat_ref, g_ref, y_ref):
    ix, iy = lax.axis_index("gx"), lax.axis_index("gy")
    pair = 2 if p.sub % 2 == 0 else 1
    energy = jnp.zeros((8, LANES), jnp.float32)
    for s in range(0, p.sub, pair):
        x = jnp.concatenate([first_ref[s + e] for e in range(pair)], axis=1)
        y = left_mul(w_ref, x)
        for e in range(pair):
            g_ref[s + e] = y[:, e * LANES:(e + 1) * LANES]
    for s in range(p.sub):
        prod = first_ref[s] * rhs_ref[s]
        for r in range(p.n // 8):
            energy = energy + prod[r * 8:(r + 1) * 8]
    y_ref[...] = jnp.zeros_like(y_ref)
    row_of = {d: i for i, d in enumerate(row_degrees()) if d >= 0}
    lane = iota((ROWS, LANES), 1)
    edge = [ktab_ref[iy][1:2], ktab_ref[iy][2:3]]
    mz = jnp.zeros((ROWS, LANES), jnp.float32)
    for d in range(DEG):
        acc = g_ref[0] * dmat_ref[d, 0:1]
        for s in range(1, p.sub):
            acc = acc + g_ref[s] * dmat_ref[d, s:s + 1]
        for f in range(2):
            at = f * ROWS + row_of[d]
            y_ref[at:at + 1] = acc[ROWS + f:ROWS + f + 1]
            total = jnp.sum(acc[:ROWS] * edge[f], axis=1, keepdims=True)
            mz = jnp.where(lane == f * BLOCK + d, total, mz)
    place = lane // p.kb
    lo = jnp.where((place == 0) & (ix == 0), g_ref[0][:ROWS], 0.0)
    hi = jnp.where((place == p.pack - 1) & (ix == p.gx - 1), g_ref[p.sub - 1][:ROWS], 0.0)
    x = jnp.concatenate([lo, hi, y_ref[...]], axis=0)
    table = v_ref[pl.ds(pl.multiple_of(iy * p.kb, 16), p.kb)]
    y = right_mul(x, split(jnp.concatenate([table] * p.pack, axis=0)))
    which = lane // BLOCK
    packed = y[0:ROWS]
    for i in range(1, 4):
        packed = jnp.where(which == i, y[i * ROWS:(i + 1) * ROWS], packed)
    return packed, mz, jnp.sum(energy, axis=1, keepdims=True)


def sum_slots(ref, count):
    total = ref[0]
    for i in range(1, count):
        total = total + ref[i]
    return total


def total_copies(p, src_ref, slots_ref, sems, axis, base):
    size = p.gx if axis == "gx" else p.gy
    me = lax.axis_index(axis)
    out = []
    for d in range(1, size):
        r = lax.rem(me + d, size)
        out.append(remote(src_ref, slots_ref.at[me], sems.at[base, d], sems.at[base + 1, d], {axis: r}))
    return out


def all_sum(p, pay_ref, xs_ref, sum_ref, ys_ref, sems):
    ix, iy = lax.axis_index("gx"), lax.axis_index("gy")
    a = total_copies(p, pay_ref, xs_ref, sems, "gx", 0)
    for c in a:
        c.start()
    xs_ref[ix] = pay_ref[...]
    for c in a:
        c.wait_recv()
    total = sum_slots(xs_ref, p.gx)
    sum_ref[...] = total
    b = total_copies(p, sum_ref, ys_ref, sems, "gy", 2)
    for c in b:
        c.start()
    ys_ref[iy] = total
    for c in b:
        c.wait_recv()
    for c in a + b:
        c.wait_send()
    return sum_slots(ys_ref, p.gy)


def mirror(blk):
    shape = (ROWS, LANES)
    lane = iota(shape, 1)
    total = blk * PER + lane // BLOCK + lane + (iota(shape, 0) >= EVEN).astype(jnp.int32)
    return jnp.where(total % 2 == 0, 1.0, -1.0)


def trade(x):
    odd = iota(x.shape, 1) % 2 == 1
    return jnp.where(odd, turn(x, 1), turn(x, -1))


def project(p, packed, mz, energy, big_ref, gain_ref, same_ref, s_ref):
    which = iota((ROWS, LANES), 1) // BLOCK

    def spread(x, i):
        x = turn(jnp.where(which == i, x, 0.0), -i * BLOCK)
        x = x + turn(x, BLOCK)
        return x + turn(x, 2 * BLOCK)

    tall = (BLOCK, LANES)
    row, col = iota(tall, 0), iota(tall, 1)
    degree = jnp.where(row < EVEN, 2 * row, 2 * (row - EVEN) + 1)
    place = (col % BLOCK == degree).astype(jnp.float32).astype(BF16)
    mz = split(jnp.concatenate([mz, jnp.zeros((BLOCK - ROWS, LANES), jnp.float32)], axis=0))

    def flip(f):
        pick = (col == f * BLOCK + degree).astype(jnp.float32).astype(BF16)
        hi, lo = split(dot_t(pick, mz[0]) + dot_t(pick, mz[1]))
        return (dot(hi, place) + dot(lo, place))[:ROWS]

    pairs = [(spread(packed, 0), spread(packed, 1)), (spread(packed, 2), spread(packed, 3)), (flip(0), flip(1))]
    s_ref[...] = jnp.zeros_like(s_ref)
    for face in range(3):
        lo, hi = pairs[face]
        for blk in range(NBLK):
            cols = slice(blk * LANES, (blk + 1) * LANES)
            both = hi + mirror(blk) * lo
            for mi in range(MI):
                prod = big_ref[face, mi][:, cols] * both
                s_ref[face, 0, blk, mi:mi + 1] = jnp.sum(prod[:EVEN], axis=0, keepdims=True)
                s_ref[face, 1, blk, mi:mi + 1] = jnp.sum(prod[EVEN:], axis=0, keepdims=True)
    hi, lo = split(s_ref[...].reshape(6 * NBLK * 16, LANES))
    spread_sum = (dot(hi, same_ref[...]) + dot(lo, same_ref[...])).reshape(3, 2, NBLK, 16, LANES)
    lane = iota((16, LANES), 1)
    to = iota((8, LANES), 1)
    pay = jnp.zeros((8, LANES), jnp.float32)
    for blk in range(NBLK):
        l = blk * PER + lane // BLOCK
        right = lane % 2 == 1
        cross = (l - lane) % 2 == 1
        sx, sy, sz = spread_sum[0], spread_sum[1], spread_sum[2]
        lm = []
        for b in range(2):
            wide = [jnp.where((lane + b) % 2 == 0, sz[a, blk], trade(sz[a, blk])) for a in range(2)]
            other = jnp.where((l + lane + b) % 2 == 1, wide[1], wide[0])
            lm.append((sx[b, blk] + jnp.where(cross, sy[1 - b, blk], sy[b, blk]) + other) * gain_ref[b, blk])
        parts = [lm[0][:8], lm[1][:8], jnp.concatenate([lm[0][8:9], lm[1][8:9], jnp.zeros((6, LANES), jnp.float32)], axis=0)]
        for part, x in enumerate(parts):
            for i in range(PER):
                at = part * LOT + 2 * (blk * PER + i)
                pay = jnp.where((to >= at) & (to < at + 2), turn(x, at - i * BLOCK), pay)
    return jnp.where(to == LANES - 1, energy, pay)


def coefficients(p, total, big_ref, coef_ref):
    to = iota((8, LANES), 1)
    for blk in range(NBLK):
        wide = []
        for part in range(3):
            x = jnp.zeros((8, LANES), jnp.float32)
            for i in range(PER):
                at = part * LOT + 2 * (blk * PER + i)
                x = jnp.where((to >= i * BLOCK) & (to < i * BLOCK + 2), turn(total, i * BLOCK - at), x)
            for shift in (2, 4, 8, 16):
                x = x + turn(x, shift)
            wide.append(x)
        lm = [jnp.concatenate([wide[b], wide[2][b:b + 1], jnp.zeros((7, LANES), jnp.float32)], axis=0) for b in range(2)]
        l = blk * PER + iota((16, LANES), 1) // BLOCK
        lane = iota((16, LANES), 1)
        right = lane % 2 == 1
        cross = (l - lane) % 2 == 1
        rows = [lm, [jnp.where(cross, lm[1 - b], lm[b]) for b in range(2)],
                [jnp.where(right, *[jnp.where((l + a) % 2 == 1, trade(lm[b]), lm[b]) for b in (1, 0)]) for a in range(2)]]
        cols = slice(blk * LANES, (blk + 1) * LANES)
        for face in range(3):
            even = jnp.zeros((EVEN, LANES), jnp.float32)
            odd = jnp.zeros((ROWS - EVEN, LANES), jnp.float32)
            for mi in range(MI):
                t = big_ref[face, mi][:, cols]
                even = even + t[:EVEN] * rows[face][0][mi:mi + 1]
                odd = odd + t[EVEN:] * rows[face][1][mi:mi + 1]
            coef_ref[face, blk] = jnp.concatenate([even, odd], axis=0)


def face_coefs(p, coef_ref, c3_ref):
    ix = lax.axis_index("gx")
    which = iota((ROWS, LANES), 1) // BLOCK
    gap = jnp.zeros((BLOCK - ROWS, LANES), jnp.float32)
    rest = jnp.zeros((LANES - 3 * BLOCK, LANES), jnp.float32)
    for l in range(DEG):
        blk, i = divmod(l, PER)
        for face in range(3):
            hi = coef_ref[face, blk]
            lo = hi * mirror(blk)
            for k, c in enumerate([jnp.where(ix == 0, lo, hi)] if face == 0 else [lo, hi]):
                c = turn(jnp.where(which == i, c, 0.0), -i * BLOCK)
                c = c + turn(c, BLOCK) + turn(c, 2 * BLOCK)
                top = c.astype(BF16).astype(jnp.float32)
                full = jnp.concatenate([top, gap, top, gap, c - top, gap, rest], axis=0)
                c3_ref[l, max(0, 2 * face - 1) + k] = full.astype(BF16)


def triple(e):
    top = e.astype(BF16).astype(jnp.float32)
    return jnp.where(iota(e.shape, 1) // BLOCK == 1, e - top, top).astype(BF16)


def faces(p, c3_ref, cu_ref, vt_ref, r_ref, e_ref, f_ref):
    near = pl.ds(pl.multiple_of(lax.axis_index("gx") * p.ca, 16), p.ca)
    rows = p.n + 4 * p.ca
    for l in range(DEG):
        e_ref[l, 0:p.n] = triple(dot(cu_ref[...], c3_ref[l, 0]))
        e = dot(cu_ref[near], jnp.concatenate([c3_ref[l, k] for k in range(1, 5)], axis=1))
        e = jnp.concatenate([e[:, k * LANES:(k + 1) * LANES] for k in range(4)], axis=0)
        e_ref[l, p.n:rows] = triple(e)
    tile = 64

    def step(t, carry):
        at = pl.ds(pl.multiple_of(t * tile, tile), tile)
        r = r_ref[at]
        acc = dot(e_ref[DEG - 1, at], vt_ref[...])
        for l in range(DEG - 2, -1, -1):
            acc = acc * r + dot(e_ref[l, at], vt_ref[...])
        f_ref[at] = acc
        return carry

    lax.fori_loop(0, rows // tile, step, 0)


def add_faces(p, rhs_ref, sine_ref, jtab_ref, ktab_ref, f_ref):
    ix, iy = lax.axis_index("gx"), lax.axis_index("gy")
    ca, n = p.ca, p.n
    chunk = pl.ds(pl.multiple_of(iy * p.kb, 16), p.kb)
    near = [jnp.concatenate([sine_ref[i, chunk]] * p.pack, axis=0) for i in range(2)]

    def to_lanes(x):
        hi, lo = split(x)
        return dot_t(hi, near[0]) + dot_t(lo, near[0]) + dot_t(hi, near[1])

    @pl.when((ix == 0) | (ix == p.gx - 1))
    def _():
        hat = left_mul(sine_ref, to_lanes(f_ref[0:n]))
        place = p.lanes(p.n)
        rhs_ref[0] += jnp.where((place == 0) & (ix == 0), hat, 0.0)
        rhs_ref[p.sub - 1] += jnp.where((place == p.pack - 1) & (ix == p.gx - 1), hat, 0.0)

    hy = to_lanes(f_ref[n:n + 2 * ca])
    place = p.lanes(p.sub)
    planes = []
    for f in range(2):
        acc = hy[f * ca:f * ca + p.sub]
        for g in range(1, p.pack):
            acc = jnp.where(place == g, hy[f * ca + g * p.sub:f * ca + (g + 1) * p.sub], acc)
        planes.append(acc)
    plus, minus = planes[0] + planes[1], planes[0] - planes[1]

    hi, lo = split(jnp.concatenate([f_ref[n + 2 * ca:n + 4 * ca]] * (LANES // (2 * ca)), axis=0))
    hz = dot_t(sine_ref[0], hi) + dot_t(sine_ref[1], hi) + dot_t(sine_ref[0], lo)
    top = hz.astype(BF16).astype(jnp.float32)
    both = jnp.where(iota(hz.shape, 1) // (2 * ca) == 1, hz - top, top).astype(BF16)
    top = top.astype(BF16)
    square = (LANES, LANES)
    row, col = iota(square, 0), iota(square, 1)
    edge = jnp.where(row % (2 * ca) < ca, ktab_ref[iy][1:2], ktab_ref[iy][2:3])
    head = edge.astype(BF16).astype(jnp.float32)
    fits = (row % ca) // p.sub == col // p.kb
    first = jnp.where(fits & (row // (2 * ca) < 2), head, 0.0)
    second = jnp.where(fits & (row < 2 * ca), edge - head, 0.0)
    pair = 2 if p.sub % 2 == 0 else 1
    even = iota((p.n, LANES), 0) % 2 == 0
    for s in range(0, p.sub, pair):
        pick = [row % p.sub == s + e for e in range(pair)]
        one = jnp.concatenate([jnp.where(k, first, 0.0).astype(BF16) for k in pick], axis=1)
        two = jnp.concatenate([jnp.where(k, second, 0.0).astype(BF16) for k in pick], axis=1)
        add = dot(both, one) + dot(top, two)
        for e in range(pair):
            at = s + e
            wave = jnp.where(even, plus[at:at + 1], minus[at:at + 1])
            rhs_ref[at] += add[:, e * LANES:(e + 1) * LANES] + jtab_ref[1] * wave


def wide(p, x):
    return jnp.concatenate([x] * (p.n // LANES), axis=1)


def local_prep(p, loc_ref, ltab_ref, rtab_ref, z_ref, kron_ref, lmode_ref, t_ref):
    sigma = wide(p, ltab_ref[0]) + rtab_ref[0:1]
    s = 0.5 * jnp.sqrt(sigma)
    t = jnp.sqrt(1.0 + s * s)
    theta = 2.0 * jnp.log1p(s + s * s / (1.0 + t))
    lam = jnp.exp(-theta)
    last = float(p.ca + 1)
    lmode_ref[0] = lam
    lmode_ref[1] = (4.0 * p.h**3 / (p.cb + 1)) / (4.0 * s * t)
    lmode_ref[2] = jnp.exp(-theta * last)
    lmode_ref[3] = lam / (1.0 - jnp.exp(-theta * (2.0 * last)))
    block = iota((p.cb, p.n), 1) // p.cb
    for i in range(2):
        tile = loc_ref[i].astype(jnp.float32)
        for b in range(p.n // p.cb):
            kron_ref[i, b * p.cb:(b + 1) * p.cb] = jnp.where(block == b, tile, 0.0).astype(BF16)

    def step(c, carry):
        rows = pl.ds(c * p.gy, p.gy)
        t_ref[rows] = left_mul(kron_ref, z_ref[rows].reshape(p.n, p.n)).reshape(p.gy, p.cb, p.n)
        return carry

    lax.fori_loop(0, p.ca // p.gy, step, 0)


def local_sources(p, f_ref, sine_ref, kron_ref, rtab_ref, t_ref, yb_ref, xb_ref):
    ix, iy = lax.axis_index("gx"), lax.axis_index("gy")
    ca, n = p.ca, p.n
    own = pl.ds(pl.multiple_of(iy * p.cb, 16), p.cb)
    hi, lo = split(jnp.concatenate([f_ref[n + 2 * ca:n + 4 * ca]] * (LANES // (2 * ca)), axis=0))
    hz = dot_t(kron_ref[0, own], hi) + dot_t(kron_ref[1, own], hi) + dot_t(kron_ref[0, own], lo)
    other = turn(hz, -ca)
    plus, minus = hz + other, hz - other
    even = iota((p.cb, n), 1) % 2 == 0
    for x in range(ca):
        t_ref[x] += rtab_ref[1:2] * jnp.where(even, plus[:, x:x + 1], minus[:, x:x + 1])
    hat = right_mul(f_ref[n:n + 2 * ca], sine_ref)
    yb_ref[0] = jnp.where(iy == 0, hat[:ca], 0.0)
    yb_ref[1] = jnp.where(iy == p.gy - 1, hat[ca:], 0.0)
    hat = right_mul(f_ref[own], sine_ref)
    xb_ref[0] = jnp.where(ix == 0, hat, 0.0)
    xb_ref[1] = jnp.where(ix == p.gx - 1, hat, 0.0)


def gather_lanes(p, parts, g):
    place = p.lanes(parts[0].shape[0])
    per = LANES // p.kb
    cols = []
    for col in range(p.n // LANES):
        acc = None
        for e in range(per):
            part = turn(parts[col * per + e], (e - g) * p.kb)
            acc = part if acc is None else jnp.where(place == e, part, acc)
        cols.append(acc)
    return jnp.concatenate(cols, axis=1)


def local_solve(p, xgot_ref, ygot_ref, xb_ref, yb_ref, ltab_ref, lmode_ref, kron_ref, wave_ref, t_ref, z_ref):
    ca, cb, n = p.ca, p.cb, p.n
    sides = [gather_lanes(p, [xgot_ref[q] for q in range(p.gy)], g) + xb_ref[e] for e, g in ((0, 0), (1, p.pack - 1))]
    if n > 2 * cb:
        sides.append(jnp.zeros((n - 2 * cb, n), jnp.float32))
    hat = left_mul(kron_ref, jnp.concatenate(sides, axis=0))
    t_ref[0] += hat[:cb]
    t_ref[ca - 1] += hat[cb:2 * cb]
    rows = []
    for e in range(2):
        got = [gather_lanes(p, [ygot_ref[q, e] for q in range(p.gy)], g) for g in range(p.pack)]
        rows.append(jnp.concatenate(got, axis=0) + yb_ref[e])
    wave_ref[0] = rows[0] + rows[1]
    wave_ref[1] = rows[0] - rows[1]
    tile = 16

    def strip(j, carry):
        at = pl.ds(pl.multiple_of(j * tile, tile), tile)
        lam, inv = lmode_ref[0, at], lmode_ref[1, at]
        column = wide(p, ltab_ref[1, at])
        even = iota((tile, n), 0) % 2 == 0
        left = jnp.zeros((tile, n), jnp.float32)
        for i in range(ca):
            v = t_ref[i, at] + column * jnp.where(even, wave_ref[0, i:i + 1], wave_ref[1, i:i + 1])
            t_ref[i, at] = v
            left = left * lam + v
        right = t_ref[ca - 1, at]
        for i in range(ca - 2, -1, -1):
            right = right * lam + t_ref[i, at]
        f0, f1 = right * lmode_ref[3, at], left * lmode_ref[3, at]
        a = f1 * lmode_ref[2, at] - f0
        b = f0 * lmode_ref[2, at] - f1
        for i in range(ca - 1, -1, -1):
            b = b * lam
            z_ref[i, at] = b
            b = b + t_ref[i, at]
        for i in range(ca):
            a = a * lam + t_ref[i, at]
            z_ref[i, at] = (a + z_ref[i, at]) * inv
        return carry

    lax.fori_loop(0, cb // tile, strip, 0)


def kernel(p, rho_ref, *refs):
    names = ("sine", "jtab", "ktab", "wide", "lanes", "cu", "vt", "big", "gain", "same", "loc", "ltab", "rtab", "pick")
    hbm = refs[:len(names)]
    out_ref, energy_ref = refs[len(names):len(names) + 2]
    rest = refs[len(names) + 2:]
    local = rest[:len(names)]
    (x_ref, send_ref, spec_ref, rhs_ref, first_ref, tab_ref, left_ref, right_ref, edge_ref, wall_ref,
     got_ref, back_ref, ends_ref, got2_ref, back2_ref, ends2_ref,
     dmat_ref, r_ref, g_ref, y_ref, pay_ref, pxs_ref, psum_ref, pys_ref,
     s_ref, coef_ref, c3_ref, e_ref, f_ref,
     part_ref, xs_ref, sum_ref, ys_ref, fin_ref, z_ref, t_ref, kron_ref, lmode_ref,
     xg_ref, xgot_ref, yg_ref, ygot_ref, yb_ref, xb_ref, wave_ref,
     table_sems, in_sems, out_sems, land_sems, ghost_out_sems, ghost_land_sems,
     line_sems, line2_sems, pay_sems, sum_sems, write_sems) = rest[len(names):]
    sine_ref, jtab_ref, ktab_ref, wide_ref, lanes_ref, cu_ref, vt_ref, big_ref, gain_ref, same_ref, loc_ref, ltab_ref, rtab_ref, pick_ref = local
    ix, iy = lax.axis_index("gx"), lax.axis_index("gy")
    order = list(range(p.gy // 2, p.gy)) + list(range(1, p.gy // 2))
    block = p.step * p.cb
    staged = [pltpu.make_async_copy(hbm[i], local[i], table_sems.at[i]) for i in range(len(names))]

    def load(c, g):
        rows = pl.ds(g * p.sub + c * p.step, p.step)
        return pltpu.make_async_copy(rho_ref.at[rows], x_ref.at[rows], in_sems.at[c, g])

    staged[0].start()
    for c in range(p.chunks):
        for g in range(p.pack):
            load(c, g).start()
    for copy in staged[1:]:
        copy.start()
    greet(p)
    staged[0].wait()

    def swap(c, d):
        q = lax.rem(iy + d, p.gy)
        planes = pl.ds(c * p.step, p.step)
        return remote(send_ref.at[q, planes], spec_ref.at[planes, pl.ds(iy * p.cb, p.cb)],
                      out_sems.at[c, d], land_sems.at[c, d], {"gy": q})

    def transform(c, carry):
        for g in range(p.pack):
            load(c, g).wait()
        x = jnp.concatenate(
            [x_ref[pl.ds(g * p.sub + c * p.step, p.step)].reshape(block, p.n) for g in range(p.pack)], axis=0
        )
        y = right_mul(x, sine_ref)
        for g in range(p.pack):
            z_ref[pl.ds(g * p.sub + c * p.step, p.step)] = y[g * block:(g + 1) * block].reshape(p.step, p.cb, p.n)
        place = p.lanes(block)
        planes = pl.ds(c * p.step, p.step)
        for q in range(p.gy):
            col, off = divmod(q * p.kb, LANES)
            piece = None
            for g in range(p.pack):
                part = turn(y[g * block:(g + 1) * block, col * LANES:(col + 1) * LANES], g * p.kb - off)
                piece = part if piece is None else jnp.where(place == g, part, piece)
            send_ref[q, planes] = piece.reshape(p.step, p.cb, LANES)

        @pl.when(c > 0)
        def _():
            for d in order:
                swap(c - 1, d).start()

        spec_ref[planes, pl.ds(iy * p.cb, p.cb)] = send_ref[iy, planes]
        return carry

    lax.fori_loop(0, p.chunks, transform, 0)
    staged[1].wait()
    staged[2].wait()
    mode_tables(p, jtab_ref, ktab_ref, tab_ref)
    for d in order:
        swap(p.chunks - 1, d).start()
    face_prep(p, dmat_ref, r_ref)
    for copy in staged[3:]:
        copy.wait()
    local_prep(p, loc_ref, ltab_ref, rtab_ref, z_ref, kron_ref, lmode_ref, t_ref)

    def across(c, carry):
        for d in order:
            swap(c, d).wait_recv()
        for i in range(0, p.step, p.pair):
            s = c * p.step + i
            x = jnp.concatenate([spec_ref[s + e] for e in range(p.pair)], axis=1)
            y = left_mul(sine_ref, x)
            for e in range(p.pair):
                rhs_ref[s + e] = y[:, e * LANES:(e + 1) * LANES]
        return carry

    lax.fori_loop(0, p.chunks, across, 0)
    edge_sums(p, rhs_ref, tab_ref, left_ref, right_ref, edge_ref)
    line_exchange(p, tab_ref, edge_ref, got_ref, back_ref, ends_ref, line_sems, lambda stage: None)

    for t in range(p.n // p.tile):
        rows = pl.ds(t * p.tile, p.tile)
        lam, inv = tab_ref[0, rows], tab_ref[1, rows]
        a, b = carries(p, rows, tab_ref, left_ref, right_ref, ends_ref)
        for i in range(p.sub - 1, -1, -1):
            b = b * lam
            first_ref[i, rows] = b
            b = b + rhs_ref[i, rows]
        for i in range(p.sub):
            a = a * lam + rhs_ref[i, rows]
            first_ref[i, rows] = (a + first_ref[i, rows]) * inv

    def drain(c, carry):
        for d in order:
            swap(c, d).wait_send()
        return carry

    lax.fori_loop(0, p.chunks, drain, 0)
    sums = moments(p, first_ref, rhs_ref, wide_ref, lanes_ref, ktab_ref, dmat_ref, g_ref, y_ref)
    pay_ref[...] = project(p, *sums, big_ref, gain_ref, same_ref, s_ref)
    total = all_sum(p, pay_ref, pxs_ref, psum_ref, pys_ref, pay_sems)
    energy_one = jnp.sum(jnp.where(iota(total.shape, 1) == LANES - 1, total, 0.0))
    coefficients(p, total, big_ref, coef_ref)
    face_coefs(p, coef_ref, c3_ref)
    faces(p, c3_ref, cu_ref, vt_ref, r_ref, e_ref, f_ref)
    add_faces(p, rhs_ref, sine_ref, jtab_ref, ktab_ref, f_ref)

    edge_sums(p, rhs_ref, tab_ref, left_ref, right_ref, edge_ref)
    ea = total_copies(p, part_ref, xs_ref, sum_sems, "gx", 0)
    eb = total_copies(p, sum_ref, ys_ref, sum_sems, "gy", 2)

    def between(stage):
        if stage == 0:
            energy = jnp.zeros((8, LANES), jnp.float32)
            for i in range(p.sub):
                prod = first_ref[i] * rhs_ref[i]
                for r in range(p.n // 8):
                    energy = energy + prod[r * 8:(r + 1) * 8]
            part_ref[...] = energy
            xs_ref[ix] = energy
            local_sources(p, f_ref, sine_ref, kron_ref, rtab_ref, t_ref, yb_ref, xb_ref)
            return
        for c in ea:
            c.start()

    line_exchange(p, tab_ref, edge_ref, got2_ref, back2_ref, ends2_ref, line2_sems, between)
    for t in range(p.n // p.tile):
        rows = pl.ds(t * p.tile, p.tile)
        lam, inv = tab_ref[0, rows], tab_ref[1, rows] * (2.0 / p.h)
        a, b = carries(p, rows, tab_ref, left_ref, right_ref, ends2_ref)
        low, high = a, b
        for i in range(p.sub - 1, -1, -1):
            b = b * lam
            first_ref[i, rows] = b
            b = b + rhs_ref[i, rows]
        low = low + b * lam
        for i in range(p.sub):
            a = a * lam + rhs_ref[i, rows]
            first_ref[i, rows] = (a + first_ref[i, rows]) * inv
        high = high + a * lam
        wall_ref[rows] = jnp.where(p.lanes(p.tile) == 0, low, high) * inv
    xg_ref[...] = left_mul(sine_ref, wall_ref[...])

    def ghost(k, d):
        q = lax.rem(iy + d, p.gy)
        src = yg_ref.at[q] if k else xg_ref.at[pl.ds(q * p.cb, p.cb)]
        dst = ygot_ref if k else xgot_ref
        return remote(src, dst.at[iy], ghost_out_sems.at[k, d], ghost_land_sems.at[k, d], {"gy": q})

    pair = 2 if p.sub % 2 == 0 else 1
    for s in range(0, p.sub, pair):
        y = left_mul(pick_ref, jnp.concatenate([first_ref[s + e] for e in range(pair)], axis=1))
        if s == 0:
            for d in order:
                ghost(0, d).start()
        for e in range(pair):
            for q in range(p.gy):
                for f in range(2):
                    yg_ref[q, f, s + e:s + e + 1] = y[2 * q + f:2 * q + f + 1, e * LANES:(e + 1) * LANES]
    xgot_ref[iy] = xg_ref[pl.ds(pl.multiple_of(iy * p.cb, 16), p.cb)]
    ygot_ref[iy] = yg_ref[iy]
    for d in order:
        ghost(1, d).start()
    for c in ea:
        c.wait_recv()
    total = sum_slots(xs_ref, p.gx)
    sum_ref[...] = total
    ys_ref[iy] = total

    for c in eb:
        c.start()
    for d in order:
        for k in range(2):
            ghost(k, d).wait_recv()
    local_solve(p, xgot_ref, ygot_ref, xb_ref, yb_ref, ltab_ref, lmode_ref, kron_ref, wave_ref, t_ref, z_ref)

    def write(c):
        rows = pl.ds(c * p.gy, p.gy)
        return pltpu.make_async_copy(fin_ref.at[rows], out_ref.at[rows], write_sems.at[c])

    def finish(c, carry):
        rows = pl.ds(c * p.gy, p.gy)
        y = right_mul(left_mul(kron_ref, z_ref[rows].reshape(p.n, p.n)), sine_ref)
        fin_ref[rows] = y.reshape(p.gy, p.cb, p.n)

        @pl.when(c > 0)
        def _():
            write(c - 1).start()

        return carry

    groups = p.ca // p.gy
    lax.fori_loop(0, groups, finish, 0)
    for c in eb:
        c.wait_recv()
    energy_two = jnp.sum(sum_slots(ys_ref, p.gy))
    write(groups - 1).start()
    scale = p.h**3 * p.norm
    energy_ref[...] = jnp.where(iota((8, LANES), 1) == 0, energy_one, energy_two) * scale
    for c in range(groups):
        write(c).wait()
    for c in ea + eb:
        c.wait_send()
    for d in order:
        for k in range(2):
            ghost(k, d).wait_send()


def shards(charge_density):
    ca, cb, n = charge_density.shape
    p = Plan(ca, cb, n, lax.axis_size("gx"), lax.axis_size("gy"))
    f32 = jnp.float32
    data = tables(p)
    cube = (p.sub, p.n, LANES)
    plane = (p.n, LANES)
    slots = (p.gx, p.jb, LANES)
    pay = (8, LANES)
    box = (p.gy, p.sub, p.cb, LANES)
    vmem = lambda shape, dtype=f32: pltpu.VMEM(shape, dtype)
    dma = pltpu.SemaphoreType.DMA
    anywhere = pl.BlockSpec(memory_space=pl.ANY)
    whole = (p.ca, p.cb, p.n)
    scratch = [vmem(t.shape, t.dtype) for t in data]
    scratch += [vmem(whole), vmem(box), vmem(cube), vmem(cube), vmem(cube), vmem((6,) + plane)]
    scratch += [vmem(plane)] * 4
    scratch += [vmem(slots), vmem(slots), vmem(plane)] * 2
    scratch += [vmem((DEG, p.sub, LANES)), vmem((p.n + 4 * p.ca, p.n)), vmem((p.sub, ROWS + 8, LANES)),
                vmem((2 * ROWS, LANES)), vmem(pay), vmem((p.gx,) + pay), vmem(pay), vmem((p.gy,) + pay)]
    scratch += [vmem((3, 2, NBLK, 16, LANES)), vmem((3, NBLK, ROWS, LANES)), vmem((DEG, 5, LANES, LANES), BF16),
                vmem((DEG, p.n + 4 * p.ca, LANES), BF16), vmem((p.n + 4 * p.ca, p.n))]
    scratch += [vmem((8, LANES)), vmem((p.gx, 8, LANES)), vmem((8, LANES)), vmem((p.gy, 8, LANES)),
                vmem(whole), vmem(whole), vmem(whole), vmem((2, n, n), BF16), vmem((4, cb, n)),
                vmem(plane), vmem((p.gy, cb, LANES)), vmem((p.gy, 2, p.sub, LANES)), vmem((p.gy, 2, p.sub, LANES)),
                vmem((2, ca, n)), vmem((2, cb, n)), vmem((2, ca, n))]
    most = max(p.gx, p.gy)
    scratch += [dma((len(data),)), dma((p.chunks, p.pack))] + [dma((p.chunks, p.gy))] * 2 + [dma((2, p.gy))] * 2
    scratch += [dma((4, p.gx))] * 2 + [dma((4, most))] * 2 + [dma((p.ca // p.gy,))]
    potential, energies = pl.pallas_call(
        functools.partial(kernel, p),
        in_specs=[anywhere] * (1 + len(data)),
        out_specs=[anywhere, pl.BlockSpec(memory_space=pltpu.VMEM)],
        out_shape=[jax.ShapeDtypeStruct(whole, f32), jax.ShapeDtypeStruct((8, LANES), f32)],
        scratch_shapes=scratch,
        compiler_params=pltpu.CompilerParams(
            collective_id=0, has_side_effects=True, vmem_limit_bytes=56 * 2**20
        ),
        name="james",
    )(charge_density, *[jnp.asarray(t) for t in data])
    return potential, energies[0, :2]


def solution(mesh):
    return jax.shard_map(
        shards,
        mesh=mesh,
        in_specs=(P("gx", "gy", None),),
        out_specs=(P("gx", "gy", None), P()),
        check_vma=False,
    )
```

```python
import functools
import math

import jax
import jax.numpy as jnp
import numpy as np
from jax import lax
from jax.experimental import pallas as pl
from jax.experimental.pallas import tpu as pltpu
from jax.sharding import PartitionSpec as P

ORDER = 16
DEG = ORDER + 1
RATIO = 1.1
RADIUS = math.sqrt(3.0) / 2.0
LANES = 128
MESH = pl.DeviceIdType.MESH
BF16 = jnp.bfloat16
EVEN = -(-((DEG + 1) // 2) // 8) * 8
ROWS = EVEN + -(-(DEG // 2) // 8) * 8
BLOCK = 32
PER = LANES // BLOCK
NBLK = -(-DEG // PER)
MI = (DEG + 1) // 2
LOT = 2 * PER * NBLK


def solid_harmonics(x, y, z):
    rr = x * x + y * y + z * z
    out = np.zeros((DEG, 2 * DEG - 1) + x.shape)
    cos = np.zeros((DEG, DEG) + x.shape)
    sin = np.zeros((DEG, DEG) + x.shape)
    cos[0, 0] = 1.0
    for l in range(1, DEG):
        s = 1.0 if l == 1 else math.sqrt((2 * l - 1) / (2.0 * l))
        cos[l, l] = s * (x * cos[l - 1, l - 1] - y * sin[l - 1, l - 1])
        sin[l, l] = s * (x * sin[l - 1, l - 1] + y * cos[l - 1, l - 1])
        for m in range(l):
            div = math.sqrt(l * l - m * m)
            far = math.sqrt((l - 1) * (l - 1) - m * m) if l - 1 > m else 0.0
            for f in (cos, sin):
                f[l, m] = (2 * l - 1) * z * f[l - 1, m] / div
                if l >= 2 and far:
                    f[l, m] = f[l, m] - far * rr * f[l - 2, m] / div
    out[:, :DEG] = cos
    out[:, DEG:] = sin[:, 1:]
    return out


def face_tensors():
    t = np.cos(np.pi * (np.arange(DEG) + 0.5) / DEG)
    fwd = np.cos(np.arange(DEG)[:, None] * np.arccos(t)[None, :]) * (2.0 / DEG)
    fwd[0] *= 0.5
    u, v = np.meshgrid(t / 2, t / 2, indexing="ij")
    half = np.full_like(u, 0.5)
    tensors = []
    for pts in ((half, u, v), (u, half, v), (u, v, half)):
        vals = solid_harmonics(*pts)
        tensors.append(np.einsum("pu,lfuv,qv->lfpq", fwd, vals, fwd))
    return np.stack(tensors)


def expansion_weights():
    w = np.zeros((DEG, 2 * DEG - 1))
    for l in range(DEG):
        for f in range(2 * DEG - 1):
            m = f if f < DEG else f - ORDER
            w[l, f] = (1.0 if m == 0 else 2.0) / (4.0 * math.pi * RADIUS * RATIO ** (l + 1))
    return w.astype(np.float32)


def split(x):
    hi = x.astype(jnp.bfloat16)
    return hi, (x - hi.astype(jnp.float32)).astype(jnp.bfloat16)


def dot(a, b):
    return jnp.dot(a, b, preferred_element_type=jnp.float32)


def left_mul(mat, x):
    hi, lo = split(x)
    return dot(mat[0], hi) + dot(mat[0], lo) + dot(mat[1], hi)


def right_mul(x, mat):
    hi, lo = split(x)
    return dot(hi, mat[0]) + dot(lo, mat[0]) + dot(hi, mat[1])


def dot_t(a, b):
    return lax.dot_general(a, b, (((1,), (1,)), ((), ())), preferred_element_type=jnp.float32)


def split_table(table):
    t = np.asarray(table, np.float32)
    hi = t.astype(BF16)
    return hi, (t - hi.astype(np.float32)).astype(BF16)


def turn(x, shift):
    width = x.shape[-1]
    shift %= width
    return pltpu.roll(x, shift, x.ndim - 1) if shift else x


class Plan:
    def __init__(self, ca, cb, n, gx, gy):
        self.ca, self.cb, self.n, self.gx, self.gy = ca, cb, n, gx, gy
        self.kb = n // gy
        self.h = 1.0 / (n + 1)
        self.norm = (2.0 * self.h) ** 2
        self.jb = n // gx
        self.width = LANES
        self.pack = LANES // self.kb
        self.sub = ca // self.pack
        self.step = max(1, self.sub // 8)
        self.pair = 2 if self.step % 2 == 0 else 1
        self.chunks = self.sub // self.step
        self.tile = min(n, 64)

    def lanes(self, rows):
        return lax.broadcasted_iota(jnp.int32, (rows, LANES), 1) // self.kb


def greet(p):
    ix, iy = lax.axis_index("gx"), lax.axis_index("gy")
    barrier = pltpu.get_barrier_semaphore()
    for d in range(1, p.gx):
        pl.semaphore_signal(barrier, inc=1, device_id={"gx": lax.rem(ix + d, p.gx)}, device_id_type=MESH)
    for d in range(1, p.gy):
        pl.semaphore_signal(barrier, inc=1, device_id={"gy": lax.rem(iy + d, p.gy)}, device_id_type=MESH)
    return barrier


def remote(src, dst, send, recv, where):
    return pltpu.make_async_remote_copy(
        src_ref=src, dst_ref=dst, send_sem=send, recv_sem=recv, device_id=where, device_id_type=MESH
    )


def mode_tables(p, epsj_ref, epsk_ref, tab_ref):
    iy = lax.axis_index("gy")
    sigma = epsj_ref[0] + epsk_ref[iy][0:1]
    s = 0.5 * jnp.sqrt(sigma)
    t = jnp.sqrt(1.0 + s * s)
    theta = 2.0 * jnp.log1p(s + s * s / (1.0 + t))
    lam = jnp.exp(-theta)
    tab_ref[0] = lam
    tab_ref[1] = p.h * p.h / (4.0 * s * t)
    tab_ref[2] = jnp.exp(-theta * float(p.sub))
    tab_ref[3] = jnp.exp(-theta * float(p.ca))
    tab_ref[4] = lam / (1.0 - jnp.exp(-theta * (2.0 * (p.n + 1))))
    tab_ref[5] = jnp.exp(-theta * float(p.n + 1))


def edge_sums(p, v_ref, tab_ref, left_ref, right_ref, edge_ref):
    def strip(t, carry):
        rows = pl.ds(pl.multiple_of(t * p.tile, p.tile), p.tile)
        lam, lsub = tab_ref[0, rows], tab_ref[2, rows]
        left, right = v_ref[0, rows], v_ref[p.sub - 1, rows]
        for i in range(1, p.sub):
            left = left * lam + v_ref[i, rows]
            right = right * lam + v_ref[p.sub - 1 - i, rows]
        left_ref[rows] = left
        right_ref[rows] = right
        dev_l, dev_r = left, right
        for g in range(1, p.pack):
            dev_l = dev_l * lsub + turn(left, -g * p.kb)
            dev_r = dev_r * lsub + turn(right, g * p.kb)
        edge_ref[rows] = jnp.where(p.lanes(p.tile) == 0, dev_l, dev_r)
        return carry

    lax.fori_loop(0, p.n // p.tile, strip, 0)


def line_exchange(p, tab_ref, edge_ref, got_ref, back_ref, ends_ref, sems, between):
    ix = lax.axis_index("gx")
    mine = pl.ds(ix * p.jb, p.jb)

    def copies(src, dst, base):
        out = []
        for d in range(1, p.gx):
            r = lax.rem(ix + d, p.gx)
            out.append(remote(src(r), dst, sems.at[base, d], sems.at[base + 1, d], {"gx": r}))
        return out

    first = copies(lambda r: edge_ref.at[pl.ds(r * p.jb, p.jb)], got_ref.at[ix], 0)
    for c in first:
        c.start()
    got_ref[ix] = edge_ref[mine]
    between(0)
    for c in first:
        c.wait_recv()
    lower = p.lanes(p.jb) == 0
    blk, det, lnp = tab_ref[3, mine], tab_ref[4, mine], tab_ref[5, mine]
    state = jnp.zeros((p.jb, LANES), jnp.float32)
    states = []
    for t in range(p.gx):
        states.append(state)
        state = state * blk + jnp.where(lower, got_ref[t], got_ref[p.gx - 1 - t])
    other = jnp.where(lower, turn(state, p.kb), turn(state, -p.kb))
    image = (other - state * lnp) * det
    for t in range(p.gx):
        states[t] = states[t] - image
        image = image * blk
    for t in range(p.gx):
        back_ref[t] = jnp.where(lower, states[t], states[p.gx - 1 - t])
    second = copies(lambda r: back_ref.at[r], ends_ref.at[mine], 2)
    for c in second:
        c.start()
    ends_ref[mine] = back_ref[ix]
    between(1)
    for c in second:
        c.wait_recv()
    for c in first + second:
        c.wait_send()


def carries(p, rows, tab_ref, left_ref, right_ref, ends_ref):
    lsub = tab_ref[2, rows]
    left, right = left_ref[rows], right_ref[rows]
    a = b = ends_ref[rows]
    place = p.lanes(p.tile)
    for g in range(p.pack - 1):
        a = jnp.where(place == g + 1, turn(a * lsub + left, p.kb), a)
        h = p.pack - 1 - g
        b = jnp.where(place == h - 1, turn(b * lsub + right, -p.kb), b)
    return a, b


def row_degrees():
    deg = np.full(ROWS, -1)
    deg[: (DEG + 1) // 2] = np.arange(0, DEG, 2)
    deg[EVEN : EVEN + DEG // 2] = np.arange(1, DEG, 2)
    return deg


def harmonic_tables(p):
    tens = face_tensors()
    deg = row_degrees()
    weights = expansion_weights() * (RADIUS ** -np.arange(DEG, dtype=np.float64))[:, None] * (p.norm / p.h)
    big = np.zeros((3, MI, ROWS, NBLK * LANES))
    gain = np.zeros((2, NBLK, 16, LANES))
    for l in range(DEG):
        for face in range(3):
            for i in range(ROWS):
                r = deg[i]
                if r < 0:
                    continue
                for q in range(DEG):
                    if face == 0:
                        odd, mpar = r % 2, (l - q) % 2
                    elif face == 1:
                        mpar = (l - q) % 2
                        odd = (r + mpar) % 2
                    else:
                        odd = q % 2
                        mpar = (r + odd) % 2
                    at = l * BLOCK + q
                    for mi in range(MI):
                        m = mpar + 2 * mi
                        if m <= l and not (odd and m == 0):
                            big[face, mi, i, at] = tens[face, l, ORDER + m if odd else m][r, q]
        for c in range(2):
            for odd in range(2):
                for mi in range(MI):
                    m = (l - c) % 2 + 2 * mi
                    if m <= l:
                        at = (l % PER) * BLOCK + c
                        gain[odd, l // PER, mi, at : (l % PER + 1) * BLOCK : 2] = weights[l, m]
    return big.astype(np.float32), gain.astype(np.float32)


def tables(p):
    n = p.n
    num = np.arange(n) + 1
    sine = np.sin(np.pi * ((num[:, None] * num[None, :]) % (2 * (n + 1))) / (n + 1))
    eps = 4.0 * np.sin(np.pi * num / (2.0 * (n + 1))) ** 2
    cheb = np.cos(np.arange(DEG)[None, :] * np.arccos((2.0 * np.arange(n) - (n - 1)) * p.h)[:, None])
    hat = sine @ cheb
    deg = row_degrees()
    used = deg >= 0
    jtab = np.stack([np.repeat(v[:, None], LANES, axis=1) for v in (eps, sine[0])])
    ktab = np.zeros((p.gy, 8, LANES))
    for r, v in enumerate((eps, sine[0], sine[n - 1])):
        ktab[:, r] = np.tile(v.reshape(p.gy, p.kb), (1, p.pack))
    wide = np.zeros((ROWS + 8, n))
    wide[:ROWS][used] = hat[:, deg[used]].T
    wide[ROWS], wide[ROWS + 1] = sine[0], sine[n - 1]
    lanes = np.zeros((n, LANES))
    for i in range(PER):
        lanes[:, i * BLOCK : i * BLOCK + DEG] = hat
    rows = np.zeros((n, BLOCK))
    rows[:, :ROWS][:, used] = cheb[:, deg[used]]
    rh, rl = split_table(rows)
    cols = np.zeros((BLOCK, n))
    cols[:DEG] = cheb.T
    ch, cl = split_table(cols)
    same = np.arange(LANES)
    same = (same[:, None] // BLOCK == same[None, :] // BLOCK) & ((same[:, None] - same[None, :]) % 2 == 0)
    big, gain = harmonic_tables(p)
    f32 = np.float32
    own = np.arange(p.cb) + 1
    small = np.sin(np.pi * ((own[:, None] * own[None, :]) % (2 * (p.cb + 1))) / (p.cb + 1))
    small_eps = 4.0 * np.sin(np.pi * own / (2.0 * (p.cb + 1))) ** 2
    ltab = np.stack([np.repeat(v[:, None], LANES, axis=1) for v in (small_eps, small[0])])
    rtab = np.zeros((8, n))
    rtab[0], rtab[1] = eps, sine[0]
    pick = np.zeros((max(16, 2 * p.gy), n))
    for q in range(p.gy):
        if q > 0:
            pick[2 * q] = sine[q * p.cb - 1]
        if q < p.gy - 1:
            pick[2 * q + 1] = sine[(q + 1) * p.cb]
    return [
        np.stack(split_table(sine)),
        jtab.astype(f32),
        ktab.astype(f32),
        np.stack(split_table(wide)),
        lanes.astype(f32),
        np.concatenate([rh, rl, rh, np.zeros_like(rh)], axis=1),
        np.concatenate([ch, ch, cl, np.zeros_like(ch)], axis=0),
        big,
        gain,
        same.astype(BF16),
        np.stack(split_table(np.tile(small, (1, n // p.cb)))),
        ltab.astype(f32),
        rtab.astype(f32),
        np.stack(split_table(pick)),
    ]


def iota(shape, dim):
    return lax.broadcasted_iota(jnp.int32, shape, dim)


def face_prep(p, dmat_ref, r_ref):
    ix = lax.axis_index("gx")
    shape = (p.sub, LANES)
    cell = ix * p.ca + (iota(shape, 1) // p.kb) * p.sub + iota(shape, 0)
    t = (2 * cell - (p.n - 1)).astype(jnp.float32) * p.h
    prev, cur = jnp.ones(shape, jnp.float32), t
    dmat_ref[0] = prev
    for d in range(1, DEG):
        dmat_ref[d] = cur
        prev, cur = cur, 2.0 * t * cur - prev
    def inverse_radius(rows, start):
        u = (2 * (start + iota((rows, p.n), 0)) - (p.n - 1)).astype(jnp.float32) * (0.5 * p.h)
        v = (2 * iota((rows, p.n), 1) - (p.n - 1)).astype(jnp.float32) * (0.5 * p.h)
        return lax.rsqrt(0.25 + u * u + v * v)
    r_ref[0:p.n] = inverse_radius(p.n, 0)
    near = inverse_radius(p.ca, ix * p.ca)
    for k in range(4):
        r_ref[p.n + k * p.ca:p.n + (k + 1) * p.ca] = near


def moments(p, first_ref, rhs_ref, w_ref, v_ref, ktab_ref, dmat_ref, g_ref, y_ref):
    ix, iy = lax.axis_index("gx"), lax.axis_index("gy")
    pair = 2 if p.sub % 2 == 0 else 1
    energy = jnp.zeros((8, LANES), jnp.float32)
    for s in range(0, p.sub, pair):
        x = jnp.concatenate([first_ref[s + e] for e in range(pair)], axis=1)
        y = left_mul(w_ref, x)
        for e in range(pair):
            g_ref[s + e] = y[:, e * LANES:(e + 1) * LANES]
    for s in range(p.sub):
        prod = first_ref[s] * rhs_ref[s]
        for r in range(p.n // 8):
            energy = energy + prod[r * 8:(r + 1) * 8]
    y_ref[...] = jnp.zeros_like(y_ref)
    row_of = {d: i for i, d in enumerate(row_degrees()) if d >= 0}
    lane = iota((ROWS, LANES), 1)
    edge = [ktab_ref[iy][1:2], ktab_ref[iy][2:3]]
    mz = jnp.zeros((ROWS, LANES), jnp.float32)
    for d in range(DEG):
        acc = g_ref[0] * dmat_ref[d, 0:1]
        for s in range(1, p.sub):
            acc = acc + g_ref[s] * dmat_ref[d, s:s + 1]
        for f in range(2):
            at = f * ROWS + row_of[d]
            y_ref[at:at + 1] = acc[ROWS + f:ROWS + f + 1]
            total = jnp.sum(acc[:ROWS] * edge[f], axis=1, keepdims=True)
            mz = jnp.where(lane == f * BLOCK + d, total, mz)
    place = lane // p.kb
    lo = jnp.where((place == 0) & (ix == 0), g_ref[0][:ROWS], 0.0)
    hi = jnp.where((place == p.pack - 1) & (ix == p.gx - 1), g_ref[p.sub - 1][:ROWS], 0.0)
    x = jnp.concatenate([lo, hi, y_ref[...]], axis=0)
    table = v_ref[pl.ds(pl.multiple_of(iy * p.kb, 16), p.kb)]
    y = right_mul(x, split(jnp.concatenate([table] * p.pack, axis=0)))
    which = lane // BLOCK
    packed = y[0:ROWS]
    for i in range(1, 4):
        packed = jnp.where(which == i, y[i * ROWS:(i + 1) * ROWS], packed)
    return packed, mz, jnp.sum(energy, axis=1, keepdims=True)


def sum_slots(ref, count):
    total = ref[0]
    for i in range(1, count):
        total = total + ref[i]
    return total


def total_copies(p, src_ref, slots_ref, sems, axis, base):
    size = p.gx if axis == "gx" else p.gy
    me = lax.axis_index(axis)
    out = []
    for d in range(1, size):
        r = lax.rem(me + d, size)
        out.append(remote(src_ref, slots_ref.at[me], sems.at[base, d], sems.at[base + 1, d], {axis: r}))
    return out


def all_sum(p, pay_ref, xs_ref, sum_ref, ys_ref, sems):
    ix, iy = lax.axis_index("gx"), lax.axis_index("gy")
    a = total_copies(p, pay_ref, xs_ref, sems, "gx", 0)
    for c in a:
        c.start()
    xs_ref[ix] = pay_ref[...]
    for c in a:
        c.wait_recv()
    total = sum_slots(xs_ref, p.gx)
    sum_ref[...] = total
    b = total_copies(p, sum_ref, ys_ref, sems, "gy", 2)
    for c in b:
        c.start()
    ys_ref[iy] = total
    for c in b:
        c.wait_recv()
    for c in a + b:
        c.wait_send()
    return sum_slots(ys_ref, p.gy)


def mirror(blk):
    shape = (ROWS, LANES)
    lane = iota(shape, 1)
    total = blk * PER + lane // BLOCK + lane + (iota(shape, 0) >= EVEN).astype(jnp.int32)
    return jnp.where(total % 2 == 0, 1.0, -1.0)


def trade(x):
    odd = iota(x.shape, 1) % 2 == 1
    return jnp.where(odd, turn(x, 1), turn(x, -1))


def project(p, packed, mz, energy, big_ref, gain_ref, same_ref, s_ref):
    which = iota((ROWS, LANES), 1) // BLOCK

    def spread(x, i):
        x = turn(jnp.where(which == i, x, 0.0), -i * BLOCK)
        x = x + turn(x, BLOCK)
        return x + turn(x, 2 * BLOCK)

    tall = (BLOCK, LANES)
    row, col = iota(tall, 0), iota(tall, 1)
    degree = jnp.where(row < EVEN, 2 * row, 2 * (row - EVEN) + 1)
    place = (col % BLOCK == degree).astype(jnp.float32).astype(BF16)
    mz = split(jnp.concatenate([mz, jnp.zeros((BLOCK - ROWS, LANES), jnp.float32)], axis=0))

    def flip(f):
        pick = (col == f * BLOCK + degree).astype(jnp.float32).astype(BF16)
        hi, lo = split(dot_t(pick, mz[0]) + dot_t(pick, mz[1]))
        return (dot(hi, place) + dot(lo, place))[:ROWS]

    pairs = [(spread(packed, 0), spread(packed, 1)), (spread(packed, 2), spread(packed, 3)), (flip(0), flip(1))]
    s_ref[...] = jnp.zeros_like(s_ref)
    for face in range(3):
        lo, hi = pairs[face]
        for blk in range(NBLK):
            cols = slice(blk * LANES, (blk + 1) * LANES)
            both = hi + mirror(blk) * lo
            for mi in range(MI):
                prod = big_ref[face, mi][:, cols] * both
                s_ref[face, 0, blk, mi:mi + 1] = jnp.sum(prod[:EVEN], axis=0, keepdims=True)
                s_ref[face, 1, blk, mi:mi + 1] = jnp.sum(prod[EVEN:], axis=0, keepdims=True)
    hi, lo = split(s_ref[...].reshape(6 * NBLK * 16, LANES))
    spread_sum = (dot(hi, same_ref[...]) + dot(lo, same_ref[...])).reshape(3, 2, NBLK, 16, LANES)
    lane = iota((16, LANES), 1)
    to = iota((8, LANES), 1)
    pay = jnp.zeros((8, LANES), jnp.float32)
    for blk in range(NBLK):
        l = blk * PER + lane // BLOCK
        right = lane % 2 == 1
        cross = (l - lane) % 2 == 1
        sx, sy, sz = spread_sum[0], spread_sum[1], spread_sum[2]
        lm = []
        for b in range(2):
            wide = [jnp.where((lane + b) % 2 == 0, sz[a, blk], trade(sz[a, blk])) for a in range(2)]
            other = jnp.where((l + lane + b) % 2 == 1, wide[1], wide[0])
            lm.append((sx[b, blk] + jnp.where(cross, sy[1 - b, blk], sy[b, blk]) + other) * gain_ref[b, blk])
        parts = [lm[0][:8], lm[1][:8], jnp.concatenate([lm[0][8:9], lm[1][8:9], jnp.zeros((6, LANES), jnp.float32)], axis=0)]
        for part, x in enumerate(parts):
            for i in range(PER):
                at = part * LOT + 2 * (blk * PER + i)
                pay = jnp.where((to >= at) & (to < at + 2), turn(x, at - i * BLOCK), pay)
    return jnp.where(to == LANES - 1, energy, pay)


def coefficients(p, total, big_ref, coef_ref):
    to = iota((8, LANES), 1)
    for blk in range(NBLK):
        wide = []
        for part in range(3):
            x = jnp.zeros((8, LANES), jnp.float32)
            for i in range(PER):
                at = part * LOT + 2 * (blk * PER + i)
                x = jnp.where((to >= i * BLOCK) & (to < i * BLOCK + 2), turn(total, i * BLOCK - at), x)
            for shift in (2, 4, 8, 16):
                x = x + turn(x, shift)
            wide.append(x)
        lm = [jnp.concatenate([wide[b], wide[2][b:b + 1], jnp.zeros((7, LANES), jnp.float32)], axis=0) for b in range(2)]
        l = blk * PER + iota((16, LANES), 1) // BLOCK
        lane = iota((16, LANES), 1)
        right = lane % 2 == 1
        cross = (l - lane) % 2 == 1
        rows = [lm, [jnp.where(cross, lm[1 - b], lm[b]) for b in range(2)],
                [jnp.where(right, *[jnp.where((l + a) % 2 == 1, trade(lm[b]), lm[b]) for b in (1, 0)]) for a in range(2)]]
        cols = slice(blk * LANES, (blk + 1) * LANES)
        for face in range(3):
            even = jnp.zeros((EVEN, LANES), jnp.float32)
            odd = jnp.zeros((ROWS - EVEN, LANES), jnp.float32)
            for mi in range(MI):
                t = big_ref[face, mi][:, cols]
                even = even + t[:EVEN] * rows[face][0][mi:mi + 1]
                odd = odd + t[EVEN:] * rows[face][1][mi:mi + 1]
            coef_ref[face, blk] = jnp.concatenate([even, odd], axis=0)


def face_coefs(p, coef_ref, c3_ref):
    ix = lax.axis_index("gx")
    which = iota((ROWS, LANES), 1) // BLOCK
    gap = jnp.zeros((BLOCK - ROWS, LANES), jnp.float32)
    rest = jnp.zeros((LANES - 3 * BLOCK, LANES), jnp.float32)
    for l in range(DEG):
        blk, i = divmod(l, PER)
        for face in range(3):
            hi = coef_ref[face, blk]
            lo = hi * mirror(blk)
            for k, c in enumerate([jnp.where(ix == 0, lo, hi)] if face == 0 else [lo, hi]):
                c = turn(jnp.where(which == i, c, 0.0), -i * BLOCK)
                c = c + turn(c, BLOCK) + turn(c, 2 * BLOCK)
                top = c.astype(BF16).astype(jnp.float32)
                full = jnp.concatenate([top, gap, top, gap, c - top, gap, rest], axis=0)
                c3_ref[l, max(0, 2 * face - 1) + k] = full.astype(BF16)


def triple(e):
    top = e.astype(BF16).astype(jnp.float32)
    return jnp.where(iota(e.shape, 1) // BLOCK == 1, e - top, top).astype(BF16)


def faces(p, c3_ref, cu_ref, vt_ref, r_ref, e_ref, f_ref):
    near = pl.ds(pl.multiple_of(lax.axis_index("gx") * p.ca, 16), p.ca)
    rows = p.n + 4 * p.ca
    for l in range(DEG):
        e_ref[l, 0:p.n] = triple(dot(cu_ref[...], c3_ref[l, 0]))
        e = dot(cu_ref[near], jnp.concatenate([c3_ref[l, k] for k in range(1, 5)], axis=1))
        e = jnp.concatenate([e[:, k * LANES:(k + 1) * LANES] for k in range(4)], axis=0)
        e_ref[l, p.n:rows] = triple(e)
    tile = 64

    def step(t, carry):
        at = pl.ds(pl.multiple_of(t * tile, tile), tile)
        r = r_ref[at]
        acc = dot(e_ref[DEG - 1, at], vt_ref[...])
        for l in range(DEG - 2, -1, -1):
            acc = acc * r + dot(e_ref[l, at], vt_ref[...])
        f_ref[at] = acc
        return carry

    lax.fori_loop(0, rows // tile, step, 0)


def add_faces(p, rhs_ref, sine_ref, jtab_ref, ktab_ref, f_ref):
    ix, iy = lax.axis_index("gx"), lax.axis_index("gy")
    ca, n = p.ca, p.n
    chunk = pl.ds(pl.multiple_of(iy * p.kb, 16), p.kb)
    near = [jnp.concatenate([sine_ref[i, chunk]] * p.pack, axis=0) for i in range(2)]

    def to_lanes(x):
        hi, lo = split(x)
        return dot_t(hi, near[0]) + dot_t(lo, near[0]) + dot_t(hi, near[1])

    @pl.when((ix == 0) | (ix == p.gx - 1))
    def _():
        hat = left_mul(sine_ref, to_lanes(f_ref[0:n]))
        place = p.lanes(p.n)
        rhs_ref[0] += jnp.where((place == 0) & (ix == 0), hat, 0.0)
        rhs_ref[p.sub - 1] += jnp.where((place == p.pack - 1) & (ix == p.gx - 1), hat, 0.0)

    hy = to_lanes(f_ref[n:n + 2 * ca])
    place = p.lanes(p.sub)
    planes = []
    for f in range(2):
        acc = hy[f * ca:f * ca + p.sub]
        for g in range(1, p.pack):
            acc = jnp.where(place == g, hy[f * ca + g * p.sub:f * ca + (g + 1) * p.sub], acc)
        planes.append(acc)
    plus, minus = planes[0] + planes[1], planes[0] - planes[1]

    hi, lo = split(jnp.concatenate([f_ref[n + 2 * ca:n + 4 * ca]] * (LANES // (2 * ca)), axis=0))
    hz = dot_t(sine_ref[0], hi) + dot_t(sine_ref[1], hi) + dot_t(sine_ref[0], lo)
    top = hz.astype(BF16).astype(jnp.float32)
    both = jnp.where(iota(hz.shape, 1) // (2 * ca) == 1, hz - top, top).astype(BF16)
    top = top.astype(BF16)
    square = (LANES, LANES)
    row, col = iota(square, 0), iota(square, 1)
    edge = jnp.where(row % (2 * ca) < ca, ktab_ref[iy][1:2], ktab_ref[iy][2:3])
    head = edge.astype(BF16).astype(jnp.float32)
    fits = (row % ca) // p.sub == col // p.kb
    first = jnp.where(fits & (row // (2 * ca) < 2), head, 0.0)
    second = jnp.where(fits & (row < 2 * ca), edge - head, 0.0)
    pair = 2 if p.sub % 2 == 0 else 1
    even = iota((p.n, LANES), 0) % 2 == 0
    for s in range(0, p.sub, pair):
        pick = [row % p.sub == s + e for e in range(pair)]
        one = jnp.concatenate([jnp.where(k, first, 0.0).astype(BF16) for k in pick], axis=1)
        two = jnp.concatenate([jnp.where(k, second, 0.0).astype(BF16) for k in pick], axis=1)
        add = dot(both, one) + dot(top, two)
        for e in range(pair):
            at = s + e
            wave = jnp.where(even, plus[at:at + 1], minus[at:at + 1])
            rhs_ref[at] += add[:, e * LANES:(e + 1) * LANES] + jtab_ref[1] * wave


def wide(p, x):
    return jnp.concatenate([x] * (p.n // LANES), axis=1)


def local_prep(p, loc_ref, ltab_ref, rtab_ref, z_ref, kron_ref, lmode_ref, t_ref):
    sigma = wide(p, ltab_ref[0]) + rtab_ref[0:1]
    s = 0.5 * jnp.sqrt(sigma)
    t = jnp.sqrt(1.0 + s * s)
    theta = 2.0 * jnp.log1p(s + s * s / (1.0 + t))
    lam = jnp.exp(-theta)
    last = float(p.ca + 1)
    lmode_ref[0] = lam
    lmode_ref[1] = (4.0 * p.h**3 / (p.cb + 1)) / (4.0 * s * t)
    lmode_ref[2] = jnp.exp(-theta * last)
    lmode_ref[3] = lam / (1.0 - jnp.exp(-theta * (2.0 * last)))
    block = iota((p.cb, p.n), 1) // p.cb
    for i in range(2):
        tile = loc_ref[i].astype(jnp.float32)
        for b in range(p.n // p.cb):
            kron_ref[i, b * p.cb:(b + 1) * p.cb] = jnp.where(block == b, tile, 0.0).astype(BF16)

    def step(c, carry):
        rows = pl.ds(c * p.gy, p.gy)
        t_ref[rows] = left_mul(kron_ref, z_ref[rows].reshape(p.n, p.n)).reshape(p.gy, p.cb, p.n)
        return carry

    lax.fori_loop(0, p.ca // p.gy, step, 0)


def local_sources(p, f_ref, sine_ref, kron_ref, rtab_ref, t_ref, yb_ref, xb_ref):
    ix, iy = lax.axis_index("gx"), lax.axis_index("gy")
    ca, n = p.ca, p.n
    own = pl.ds(pl.multiple_of(iy * p.cb, 16), p.cb)
    hi, lo = split(jnp.concatenate([f_ref[n + 2 * ca:n + 4 * ca]] * (LANES // (2 * ca)), axis=0))
    hz = dot_t(kron_ref[0, own], hi) + dot_t(kron_ref[1, own], hi) + dot_t(kron_ref[0, own], lo)
    other = turn(hz, -ca)
    plus, minus = hz + other, hz - other
    even = iota((p.cb, n), 1) % 2 == 0
    for x in range(ca):
        t_ref[x] += rtab_ref[1:2] * jnp.where(even, plus[:, x:x + 1], minus[:, x:x + 1])
    hat = right_mul(f_ref[n:n + 2 * ca], sine_ref)
    yb_ref[0] = jnp.where(iy == 0, hat[:ca], 0.0)
    yb_ref[1] = jnp.where(iy == p.gy - 1, hat[ca:], 0.0)
    hat = right_mul(f_ref[own], sine_ref)
    xb_ref[0] = jnp.where(ix == 0, hat, 0.0)
    xb_ref[1] = jnp.where(ix == p.gx - 1, hat, 0.0)


def gather_lanes(p, parts, g):
    place = p.lanes(parts[0].shape[0])
    per = LANES // p.kb
    cols = []
    for col in range(p.n // LANES):
        acc = None
        for e in range(per):
            part = turn(parts[col * per + e], (e - g) * p.kb)
            acc = part if acc is None else jnp.where(place == e, part, acc)
        cols.append(acc)
    return jnp.concatenate(cols, axis=1)


def local_solve(p, xgot_ref, ygot_ref, xb_ref, yb_ref, ltab_ref, lmode_ref, kron_ref, wave_ref, t_ref, z_ref):
    ca, cb, n = p.ca, p.cb, p.n
    sides = [gather_lanes(p, [xgot_ref[q] for q in range(p.gy)], g) + xb_ref[e] for e, g in ((0, 0), (1, p.pack - 1))]
    if n > 2 * cb:
        sides.append(jnp.zeros((n - 2 * cb, n), jnp.float32))
    hat = left_mul(kron_ref, jnp.concatenate(sides, axis=0))
    t_ref[0] += hat[:cb]
    t_ref[ca - 1] += hat[cb:2 * cb]
    rows = []
    for e in range(2):
        got = [gather_lanes(p, [ygot_ref[q, e] for q in range(p.gy)], g) for g in range(p.pack)]
        rows.append(jnp.concatenate(got, axis=0) + yb_ref[e])
    wave_ref[0] = rows[0] + rows[1]
    wave_ref[1] = rows[0] - rows[1]
    tile = 16

    def strip(j, carry):
        at = pl.ds(pl.multiple_of(j * tile, tile), tile)
        lam, inv = lmode_ref[0, at], lmode_ref[1, at]
        column = wide(p, ltab_ref[1, at])
        even = iota((tile, n), 0) % 2 == 0
        left = jnp.zeros((tile, n), jnp.float32)
        for i in range(ca):
            v = t_ref[i, at] + column * jnp.where(even, wave_ref[0, i:i + 1], wave_ref[1, i:i + 1])
            t_ref[i, at] = v
            left = left * lam + v
        right = t_ref[ca - 1, at]
        for i in range(ca - 2, -1, -1):
            right = right * lam + t_ref[i, at]
        f0, f1 = right * lmode_ref[3, at], left * lmode_ref[3, at]
        a = f1 * lmode_ref[2, at] - f0
        b = f0 * lmode_ref[2, at] - f1
        for i in range(ca - 1, -1, -1):
            b = b * lam
            z_ref[i, at] = b
            b = b + t_ref[i, at]
        for i in range(ca):
            a = a * lam + t_ref[i, at]
            z_ref[i, at] = (a + z_ref[i, at]) * inv
        return carry

    lax.fori_loop(0, cb // tile, strip, 0)


def kernel(p, rho_ref, *refs):
    names = ("sine", "jtab", "ktab", "wide", "lanes", "cu", "vt", "big", "gain", "same", "loc", "ltab", "rtab", "pick")
    hbm = refs[:len(names)]
    out_ref, energy_ref = refs[len(names):len(names) + 2]
    rest = refs[len(names) + 2:]
    local = rest[:len(names)]
    (x_ref, send_ref, spec_ref, rhs_ref, first_ref, tab_ref, left_ref, right_ref, edge_ref, wall_ref,
     got_ref, back_ref, ends_ref, got2_ref, back2_ref, ends2_ref,
     dmat_ref, r_ref, g_ref, y_ref, pay_ref, pxs_ref, psum_ref, pys_ref,
     s_ref, coef_ref, c3_ref, e_ref, f_ref,
     part_ref, xs_ref, sum_ref, ys_ref, z_ref, t_ref, kron_ref, lmode_ref,
     xg_ref, xgot_ref, yg_ref, ygot_ref, yb_ref, xb_ref, wave_ref,
     table_sems, in_sems, out_sems, land_sems, ghost_out_sems, ghost_land_sems,
     line_sems, line2_sems, pay_sems, sum_sems) = rest[len(names):]
    sine_ref, jtab_ref, ktab_ref, wide_ref, lanes_ref, cu_ref, vt_ref, big_ref, gain_ref, same_ref, loc_ref, ltab_ref, rtab_ref, pick_ref = local
    ix, iy = lax.axis_index("gx"), lax.axis_index("gy")
    order = list(range(p.gy // 2, p.gy)) + list(range(1, p.gy // 2))
    block = p.step * p.cb
    staged = [pltpu.make_async_copy(hbm[i], local[i], table_sems.at[i]) for i in range(len(names))]

    def load(c, g):
        rows = pl.ds(g * p.sub + c * p.step, p.step)
        return pltpu.make_async_copy(rho_ref.at[rows], x_ref.at[rows], in_sems.at[c, g])

    staged[0].start()
    for c in range(p.chunks):
        for g in range(p.pack):
            load(c, g).start()
    for copy in staged[1:]:
        copy.start()
    barrier = greet(p)
    staged[0].wait()

    def swap(c, d):
        q = lax.rem(iy + d, p.gy)
        planes = pl.ds(c * p.step, p.step)
        return remote(send_ref.at[q, planes], spec_ref.at[planes, pl.ds(iy * p.cb, p.cb)],
                      out_sems.at[c, d], land_sems.at[c, d], {"gy": q})

    def transform(c, carry):
        for g in range(p.pack):
            load(c, g).wait()
        x = jnp.concatenate(
            [x_ref[pl.ds(g * p.sub + c * p.step, p.step)].reshape(block, p.n) for g in range(p.pack)], axis=0
        )
        y = right_mul(x, sine_ref)
        for g in range(p.pack):
            z_ref[pl.ds(g * p.sub + c * p.step, p.step)] = y[g * block:(g + 1) * block].reshape(p.step, p.cb, p.n)
        place = p.lanes(block)
        planes = pl.ds(c * p.step, p.step)
        for q in range(p.gy):
            col, off = divmod(q * p.kb, LANES)
            piece = None
            for g in range(p.pack):
                part = turn(y[g * block:(g + 1) * block, col * LANES:(col + 1) * LANES], g * p.kb - off)
                piece = part if piece is None else jnp.where(place == g, part, piece)
            send_ref[q, planes] = piece.reshape(p.step, p.cb, LANES)
        if not isinstance(c, int):
            for d in order:
                swap(c - 1, d).start()
        spec_ref[planes, pl.ds(iy * p.cb, p.cb)] = send_ref[iy, planes]
        return carry

    transform(0, 0)
    pl.semaphore_wait(barrier, p.gx + p.gy - 2)
    lax.fori_loop(1, p.chunks, transform, 0)
    staged[1].wait()
    staged[2].wait()
    mode_tables(p, jtab_ref, ktab_ref, tab_ref)
    for d in order:
        swap(p.chunks - 1, d).start()
    face_prep(p, dmat_ref, r_ref)
    for copy in staged[3:]:
        copy.wait()
    local_prep(p, loc_ref, ltab_ref, rtab_ref, z_ref, kron_ref, lmode_ref, t_ref)

    def across(c, carry):
        for d in order:
            swap(c, d).wait_recv()
        for i in range(0, p.step, p.pair):
            s = c * p.step + i
            x = jnp.concatenate([spec_ref[s + e] for e in range(p.pair)], axis=1)
            y = left_mul(sine_ref, x)
            for e in range(p.pair):
                rhs_ref[s + e] = y[:, e * LANES:(e + 1) * LANES]
        return carry

    lax.fori_loop(0, p.chunks, across, 0)
    edge_sums(p, rhs_ref, tab_ref, left_ref, right_ref, edge_ref)
    line_exchange(p, tab_ref, edge_ref, got_ref, back_ref, ends_ref, line_sems, lambda stage: None)

    for t in range(p.n // p.tile):
        rows = pl.ds(t * p.tile, p.tile)
        lam, inv = tab_ref[0, rows], tab_ref[1, rows]
        a, b = carries(p, rows, tab_ref, left_ref, right_ref, ends_ref)
        for i in range(p.sub - 1, -1, -1):
            b = b * lam
            first_ref[i, rows] = b
            b = b + rhs_ref[i, rows]
        for i in range(p.sub):
            a = a * lam + rhs_ref[i, rows]
            first_ref[i, rows] = (a + first_ref[i, rows]) * inv

    def drain(c, carry):
        for d in order:
            swap(c, d).wait_send()
        return carry

    lax.fori_loop(0, p.chunks, drain, 0)
    sums = moments(p, first_ref, rhs_ref, wide_ref, lanes_ref, ktab_ref, dmat_ref, g_ref, y_ref)
    pay_ref[...] = project(p, *sums, big_ref, gain_ref, same_ref, s_ref)
    total = all_sum(p, pay_ref, pxs_ref, psum_ref, pys_ref, pay_sems)
    energy_one = jnp.sum(jnp.where(iota(total.shape, 1) == LANES - 1, total, 0.0))
    coefficients(p, total, big_ref, coef_ref)
    face_coefs(p, coef_ref, c3_ref)
    faces(p, c3_ref, cu_ref, vt_ref, r_ref, e_ref, f_ref)
    add_faces(p, rhs_ref, sine_ref, jtab_ref, ktab_ref, f_ref)

    edge_sums(p, rhs_ref, tab_ref, left_ref, right_ref, edge_ref)
    ea = total_copies(p, part_ref, xs_ref, sum_sems, "gx", 0)
    eb = total_copies(p, sum_ref, ys_ref, sum_sems, "gy", 2)

    def between(stage):
        if stage == 0:
            energy = jnp.zeros((8, LANES), jnp.float32)
            for i in range(p.sub):
                prod = first_ref[i] * rhs_ref[i]
                for r in range(p.n // 8):
                    energy = energy + prod[r * 8:(r + 1) * 8]
            part_ref[...] = energy
            xs_ref[ix] = energy
            local_sources(p, f_ref, sine_ref, kron_ref, rtab_ref, t_ref, yb_ref, xb_ref)
            return
        for c in ea:
            c.start()

    line_exchange(p, tab_ref, edge_ref, got2_ref, back2_ref, ends2_ref, line2_sems, between)
    for t in range(p.n // p.tile):
        rows = pl.ds(t * p.tile, p.tile)
        lam, inv = tab_ref[0, rows], tab_ref[1, rows] * (2.0 / p.h)
        a, b = carries(p, rows, tab_ref, left_ref, right_ref, ends2_ref)
        low, high = a, b
        for i in range(p.sub - 1, -1, -1):
            b = b * lam
            first_ref[i, rows] = b
            b = b + rhs_ref[i, rows]
        low = low + b * lam
        for i in range(p.sub):
            a = a * lam + rhs_ref[i, rows]
            first_ref[i, rows] = (a + first_ref[i, rows]) * inv
        high = high + a * lam
        wall_ref[rows] = jnp.where(p.lanes(p.tile) == 0, low, high) * inv
    xg_ref[...] = left_mul(sine_ref, wall_ref[...])

    def ghost(k, d):
        q = lax.rem(iy + d, p.gy)
        src = yg_ref.at[q] if k else xg_ref.at[pl.ds(q * p.cb, p.cb)]
        dst = ygot_ref if k else xgot_ref
        return remote(src, dst.at[iy], ghost_out_sems.at[k, d], ghost_land_sems.at[k, d], {"gy": q})

    pair = 2 if p.sub % 2 == 0 else 1
    for s in range(0, p.sub, pair):
        y = left_mul(pick_ref, jnp.concatenate([first_ref[s + e] for e in range(pair)], axis=1))
        if s == 0:
            for d in order:
                ghost(0, d).start()
        for e in range(pair):
            for q in range(p.gy):
                for f in range(2):
                    yg_ref[q, f, s + e:s + e + 1] = y[2 * q + f:2 * q + f + 1, e * LANES:(e + 1) * LANES]
    xgot_ref[iy] = xg_ref[pl.ds(pl.multiple_of(iy * p.cb, 16), p.cb)]
    ygot_ref[iy] = yg_ref[iy]
    for d in order:
        ghost(1, d).start()
    for c in ea:
        c.wait_recv()
    total = sum_slots(xs_ref, p.gx)
    sum_ref[...] = total
    ys_ref[iy] = total

    for c in eb:
        c.start()
    for d in order:
        for k in range(2):
            ghost(k, d).wait_recv()
    local_solve(p, xgot_ref, ygot_ref, xb_ref, yb_ref, ltab_ref, lmode_ref, kron_ref, wave_ref, t_ref, z_ref)

    def finish(c, carry):
        rows = pl.ds(c * p.gy, p.gy)
        y = right_mul(left_mul(kron_ref, z_ref[rows].reshape(p.n, p.n)), sine_ref)
        out_ref[rows] = y.reshape(p.gy, p.cb, p.n)
        return carry

    groups = p.ca // p.gy
    lax.fori_loop(0, groups, finish, 0, unroll=2 if groups % 2 == 0 else 1)
    for c in eb:
        c.wait_recv()
    energy_two = jnp.sum(sum_slots(ys_ref, p.gy))
    scale = p.h**3 * p.norm
    energy_ref[...] = jnp.where(iota((8, LANES), 1) == 0, energy_one, energy_two) * scale
    for c in ea + eb:
        c.wait_send()
    for d in order:
        for k in range(2):
            ghost(k, d).wait_send()


def shards(charge_density):
    ca, cb, n = charge_density.shape
    p = Plan(ca, cb, n, lax.axis_size("gx"), lax.axis_size("gy"))
    f32 = jnp.float32
    data = tables(p)
    cube = (p.sub, p.n, LANES)
    plane = (p.n, LANES)
    slots = (p.gx, p.jb, LANES)
    pay = (8, LANES)
    box = (p.gy, p.sub, p.cb, LANES)
    vmem = lambda shape, dtype=f32: pltpu.VMEM(shape, dtype)
    dma = pltpu.SemaphoreType.DMA
    whole = (p.ca, p.cb, p.n)
    scratch = [vmem(t.shape, t.dtype) for t in data]
    scratch += [vmem(whole), vmem(box), vmem(cube), vmem(cube), vmem(cube), vmem((6,) + plane)]
    scratch += [vmem(plane)] * 4
    scratch += [vmem(slots), vmem(slots), vmem(plane)] * 2
    scratch += [vmem((DEG, p.sub, LANES)), vmem((p.n + 4 * p.ca, p.n)), vmem((p.sub, ROWS + 8, LANES)),
                vmem((2 * ROWS, LANES)), vmem(pay), vmem((p.gx,) + pay), vmem(pay), vmem((p.gy,) + pay)]
    scratch += [vmem((3, 2, NBLK, 16, LANES)), vmem((3, NBLK, ROWS, LANES)), vmem((DEG, 5, LANES, LANES), BF16),
                vmem((DEG, p.n + 4 * p.ca, LANES), BF16), vmem((p.n + 4 * p.ca, p.n))]
    scratch += [vmem((8, LANES)), vmem((p.gx, 8, LANES)), vmem((8, LANES)), vmem((p.gy, 8, LANES)),
                vmem(whole), vmem(whole), vmem((2, n, n), BF16), vmem((4, cb, n)),
                vmem(plane), vmem((p.gy, cb, LANES)), vmem((p.gy, 2, p.sub, LANES)), vmem((p.gy, 2, p.sub, LANES)),
                vmem((2, ca, n)), vmem((2, cb, n)), vmem((2, ca, n))]
    most = max(p.gx, p.gy)
    scratch += [dma((len(data),)), dma((p.chunks, p.pack))] + [dma((p.chunks, p.gy))] * 2 + [dma((2, p.gy))] * 2
    scratch += [dma((4, p.gx))] * 2 + [dma((4, most))] * 2
    potential, energies = pl.pallas_call(
        functools.partial(kernel, p),
        in_specs=[pl.BlockSpec(memory_space=pltpu.HBM)] * (1 + len(data)),
        out_specs=[pl.BlockSpec(memory_space=pltpu.VMEM)] * 2,
        out_shape=[jax.ShapeDtypeStruct(whole, f32), jax.ShapeDtypeStruct((8, LANES), f32)],
        scratch_shapes=scratch,
        compiler_params=pltpu.CompilerParams(
            collective_id=0, has_side_effects=True, vmem_limit_bytes=31 * 2**20
        ),
        name="james",
    )(*[pltpu.with_memory_space_constraint(t, pltpu.HBM) for t in (charge_density, *map(jnp.asarray, data))])
    return potential, energies[0, :2]


def solution(mesh):
    return jax.shard_map(
        shards,
        mesh=mesh,
        in_specs=(P("gx", "gy", None),),
        out_specs=(P("gx", "gy", None), P()),
        check_vma=False,
    )
```
